32 devices in a mesh: dp: 8 (over z, x), fsdp: 4 (over y, core).
Axes of the slice: x: 2, y: 2, z: 4, core: 2. Of those that a mesh axis runs over, the one named last changes fastest.
Arguments:
- hidden: bfloat16 [16, 256, 5120], P('dp', None, 'fsdp'), may hold values from -8 to 8
- gain: bfloat16 [5120], P('fsdp'), may hold values from 0.25 to 1.75
- head: bfloat16 [2048, 5120], P('fsdp'), may hold values from -1 to 1
- targets: int32 [16, 256], P('dp'), may hold values from 0 to 2047, as said below
- lengths: int32 [16], P('dp'), may hold values from 1 to 256, 2048 in all
- old_logp: float32 [16, 256], P('dp'), may hold values from -64 to 0
- rewards: float32 [16], P('dp'), may hold values from -6 to 6
- group_slot: int32 [16], P('dp'), may hold values from 0 to 15, each once
Outputs:
- loss: float32 [], replicated
- grad_hidden: bfloat16 [16, 256, 5120], P('dp', None, 'fsdp')
- grad_gain: float32 [5120], P('fsdp')
- grad_head_t: float32 [5120, 2048], P('dp', 'fsdp')
The draws below stay inside these ranges and needn't reach their ends.
Inputs may be any that keep to these rules, and one draw needn't show every extreme that they name: `lengths`: they sum to 2048 and one of them equals 256. `group_slot`: each value once; responses with equal group_slot // 8 answer one prompt. At position 0, different responses have different targets.
All inputs are finite; a program needn't handle non-finite values. No bound on the sum of `lengths` on one device may be relied on, other than what follows from the above.
Results may differ from the reference program's by a relative error of at most 0.018.
Values may be sent and summed in bfloat16 or wider, within the bound.
A program may use at most 64 MiB of HBM per device.

```python
import math
import jax
import jax.numpy as jnp
import numpy as np
from jax import lax

D = 5120
VOC_DEV = 512
LEN = 256
GROUP = 8
RESP_DEV = 2
RESPONSES = 16
VOCAB = 2048
NGROUPS = 2
TOKENS = 4096
N_DP = 8
N_FSDP = 4


def drawn_entries(key):
    amount = RESPONSES
    order = jax.random.permutation(jax.random.fold_in(key, 7001), VOCAB).astype(jnp.int32)
    return order[:amount]


def draw_targets(key, part):
    upper_ids = drawn_entries(key)
    base = jax.random.randint(jax.random.fold_in(key, 7101), (RESPONSES, LEN), 0, VOCAB, jnp.int32)
    return base.at[:, 0].set(upper_ids)


def draw_hidden(key, part):
    base = jax.random.normal(jax.random.fold_in(key, 7201), (RESPONSES, LEN, D), jnp.float32)
    base = jnp.clip(base, -6.0, 6.0)
    return base.astype(jnp.bfloat16)


def draw_gain(key, part):
    base = jax.random.normal(jax.random.fold_in(key, 7501), (D,), jnp.float32)
    return (1.0 + 0.15 * jnp.clip(base, -5.0, 5.0)).astype(jnp.bfloat16)


def draw_head(key, part):
    spread = math.sqrt(9.0 / D)
    base = jax.random.normal(jax.random.fold_in(key, 7301), (VOCAB, D), jnp.float32) * spread
    base = jnp.clip(base, -6.0 * spread, 6.0 * spread)
    return base.astype(jnp.bfloat16)


def draw_old_logp(key, part):
    states = draw_hidden(key, part)
    gain_f = draw_gain(key, part).astype(jnp.float32)
    weights = draw_head(key, part)
    picks = draw_targets(key, part)

    def response_logp(item):
        rows_here, chosen_ids = item
        values = rows_here.astype(jnp.float32)
        inv = lax.rsqrt(jnp.mean(values * values, axis=1, keepdims=True) + 1e-06)
        normed = (values * inv * gain_f).astype(jnp.bfloat16)
        logits = lax.dot_general(normed, weights, (((1,), (1,)), ((), ())), preferred_element_type=jnp.float32)
        top = jnp.max(logits, axis=1)
        lse = top + jnp.log(jnp.sum(jnp.exp(logits - top[:, None]), axis=1))
        hits = jnp.arange(VOCAB, dtype=jnp.int32)[None, :] == chosen_ids[:, None]
        return jnp.sum(jnp.where(hits, logits, 0.0), axis=1) - lse
    logp = lax.map(response_logp, (states, picks))
    band = jax.random.randint(jax.random.fold_in(key, 7402), (RESPONSES, LEN), 0, 4, jnp.int32)
    lows = jnp.log(jnp.array([0.5, 0.88, 1.4, 3.6], jnp.float32))
    highs = jnp.log(jnp.array([0.7, 1.12, 2.5, 6.0], jnp.float32))
    lower_edge = jnp.take(lows, band)
    upper_edge = jnp.take(highs, band)
    level = jax.random.uniform(jax.random.fold_in(key, 7403), (RESPONSES, LEN), jnp.float32, 0.0, 1.0)
    logratio = lower_edge + level * (upper_edge - lower_edge)
    older = logp - logratio
    older = jnp.where(older > 0.0, logp - math.log(2.0), older)
    return jnp.clip(older, -64.0, 0.0)


def block_scale(key, dims, split, smallest, high):
    level = 1.0
    for axis_at, shards_of in split:
        heights = jax.random.uniform(jax.random.fold_in(jax.random.fold_in(key, 6), axis_at), (shards_of,), jnp.float32, smallest / len(split), high / len(split))
        level = level * jnp.repeat(jnp.exp(heights), dims[axis_at] // shards_of).reshape((-1,) + (1,) * (len(dims) - 1 - axis_at))
    return level


def length_profile(number_of, total, limit, lean):
    loads = [(1 << 20) // math.isqrt(standing ** lean) + 1 for standing in range(2, number_of + 1)]
    surplus, counts = total - limit - (number_of - 1), [1] * (number_of - 1)
    while surplus > 0:
        candidates = [i for i in range(number_of - 1) if counts[i] < limit]
        pool, budget = sum([loads[i] for i in candidates]), surplus
        for i in candidates:
            more = min(limit - counts[i], max(1, budget * loads[i] // pool), surplus)
            counts[i] = counts[i] + more
            surplus = surplus - more
    return np.array([limit] + counts)


def uneven(own_key, count, total, limit, skew):
    if count == 2:
        one = jax.random.randint(own_key, (), max(1, total - limit), min(limit, total - 1) + 1)
        return jnp.stack([one, total - one])
    sizes = jnp.asarray(length_profile(count, total, limit, skew), jnp.int32)
    couples = (count - 1) // 2
    source_of, taker = sizes[1:1 + 2 * couples:2], sizes[2:2 + 2 * couples:2]
    slack = jnp.minimum(source_of - 1, limit - taker)
    shifted = jax.random.randint(jax.random.fold_in(own_key, 1), (couples,), 0, 1 << 20) % (slack + 1)
    sizes = sizes.at[1:1 + 2 * couples:2].set(source_of - shifted).at[2:2 + 2 * couples:2].set(taker + shifted)
    return sizes[jax.random.permutation(jax.random.fold_in(own_key, 2), count)]


def normal_values(own_key, shape, scale, reach, split=(), kind=jnp.bfloat16):
    result = scale * jax.random.normal(own_key, shape, jnp.float32)
    if split:
        result = result * block_scale(own_key, shape, split, -0.22, 0.18)
    return jnp.clip(result, -reach, reach).astype(kind)


def setup_inputs(seed: int = 0) -> dict:
    key_list = jax.random.split(jax.random.key(seed), 9)
    hidden = draw_hidden(jax.random.fold_in(key_list[8], 71), 0)
    gain = draw_gain(jax.random.fold_in(key_list[8], 71), 0)
    head = draw_head(jax.random.fold_in(key_list[8], 71), 0)
    targets = draw_targets(jax.random.fold_in(key_list[8], 71), 0)
    lengths = uneven(key_list[4], RESPONSES, RESPONSES * LEN // 2, LEN, 2).astype(jnp.int32)
    old_logp = draw_old_logp(jax.random.fold_in(key_list[8], 71), 0)
    rewards = normal_values(key_list[6], (RESPONSES,), 1.0, 6.0, ((0, 8),), jnp.float32)
    group_slot = jax.random.permutation(key_list[7], RESPONSES).astype(jnp.int32)
    return {"hidden": hidden, "gain": gain, "head": head, "targets": targets, "lengths": lengths, "old_logp": old_logp, "rewards": rewards, "group_slot": group_slot}


eps_norm = 1e-06
clip_low = 0.8
clip_high = 1.2
dual_bound = 3.0

def reference(hidden, gain, head, targets, lengths, old_logp, rewards, group_slot):
    rows = RESPONSES * LEN
    h = hidden.reshape(rows, D).astype(jnp.float32)
    inv = lax.rsqrt(lax.optimization_barrier(jnp.mean(h * h, axis=1, keepdims=True)) + eps_norm)
    gain_f = gain.astype(jnp.float32)
    normed = (h * inv * gain_f).astype(jnp.bfloat16)
    logits = lax.dot_general(normed.astype(jnp.float32), head.astype(jnp.float32), (((1,), (1,)), ((), ())), preferred_element_type=jnp.float32)
    top = lax.optimization_barrier(jnp.max(logits, axis=1, keepdims=True))
    lse = top[:, 0] + jnp.log(lax.optimization_barrier(jnp.sum(jnp.exp(logits - top), axis=1)))
    flat_targets = targets.reshape(rows).astype(jnp.int32)
    hits = jnp.arange(VOCAB, dtype=jnp.int32)[None, :] == flat_targets[:, None]
    chosen = lax.optimization_barrier(jnp.sum(jnp.where(hits, logits, 0.0), axis=1))
    logp = chosen - lse
    group = group_slot // GROUP
    member = (group[:, None] == jnp.arange(NGROUPS, dtype=jnp.int32)[None, :]).astype(jnp.float32)
    group_sums = lax.optimization_barrier(jnp.sum(member * rewards[:, None], axis=0))
    adv_resp = rewards - lax.optimization_barrier(jnp.sum(member * group_sums[None, :], axis=1)) / GROUP
    adv = jnp.repeat(adv_resp, LEN)
    mask = (jnp.arange(LEN, dtype=jnp.int32)[None, :] < lengths[:, None]).astype(jnp.float32).reshape(rows)
    count = jnp.sum(lengths).astype(jnp.float32)
    ratio = jnp.exp(logp - old_logp.reshape(rows))
    first = ratio * adv
    second = jnp.clip(ratio, clip_low, clip_high) * adv
    policy = -jnp.minimum(first, second)
    policy = jnp.where(adv < 0, jnp.minimum(policy, -dual_bound * adv), policy)
    loss = jnp.sum(mask * policy) / count
    active = (first <= second) & jnp.logical_not((adv < 0) & (first < dual_bound * adv))
    grad_logp = TOKENS / count * mask * jnp.where(active, -ratio * adv, 0.0)
    probs = jnp.exp(logits - lse[:, None])
    dlogits = (grad_logp[:, None] * (hits.astype(jnp.float32) - probs)).astype(jnp.bfloat16)

    def add_block(total, index):
        piece = lax.dynamic_slice_in_dim(dlogits, index * VOC_DEV, VOC_DEV, 1)
        rows_w = lax.dynamic_slice_in_dim(head, index * VOC_DEV, VOC_DEV, 0)
        term = jnp.dot(piece.astype(jnp.float32), rows_w.astype(jnp.float32), preferred_element_type=jnp.float32)
        return (total + term.astype(jnp.bfloat16).astype(jnp.float32), None)
    dnormed, _ = lax.scan(add_block, jnp.zeros((rows, D), jnp.float32), jnp.arange(N_FSDP, dtype=jnp.int32))
    dy = dnormed * gain_f
    dots = lax.optimization_barrier(jnp.sum(h * dy, axis=1, keepdims=True))
    grad_h = inv * dy - h * inv * inv * inv * dots / D
    grad_hidden = grad_h.astype(jnp.bfloat16).reshape(RESPONSES, LEN, D)
    grad_gain = lax.optimization_barrier(jnp.sum(dnormed * h * inv, axis=0))
    per_group = RESP_DEV * LEN

    def add_group(total, index):
        left = lax.dynamic_slice_in_dim(normed, index * per_group, per_group, 0)
        right = lax.dynamic_slice_in_dim(dlogits, index * per_group, per_group, 0)
        term = lax.dot_general(left.astype(jnp.float32), right.astype(jnp.float32), (((0,), (0,)), ((), ())), preferred_element_type=jnp.float32)
        return (total + term.astype(jnp.bfloat16).astype(jnp.float32), None)
    grad_head_t, _ = lax.scan(add_group, jnp.zeros((D, VOCAB), jnp.float32), jnp.arange(N_DP, dtype=jnp.int32))
    return (loss, grad_hidden, grad_gain, grad_head_t)
```

```python
import functools
import jax
import jax.numpy as jnp
from jax import lax
from jax.experimental import pallas as pl
from jax.experimental.pallas import tpu as pltpu
from jax.sharding import PartitionSpec as P

GROUP = 8
LANES = 128


eps_norm = 1e-06
clip_low = 0.8
clip_high = 1.2
dual_bound = 3.0


MESH = pl.DeviceIdType.MESH


def whole_kernel(
    n_dp,
    n_fsdp,
    length_max,
    small_ref,
    hidden_ref,
    head_hbm,
    gh_ref,
    gw_ref,
    gg_ref,
    head,
    hs,
    hz,
    nm,
    lg,
    inv_s,
    rowv,
    cnt,
    loss_s,
    gain_in,
    meta_out,
    meta_in,
    st_out,
    st_in,
    dls,
    dlz,
    c_out,
    c_in,
    y_out,
    y_in,
    acc,
    d_out,
    d_in,
    x_out,
    x_in,
    z_out,
    z_in,
    fin,
    g_out,
    g_in,
    own_sem,
    head_sem,
    ysem,
    nsem,
    fsem,
    zsem,
    wsem,
    ssem,
    msem,
    tsem,
    lsem,
    csem,
    rsem,
    dsem,
    xsem,
    hsem,
    gsem,
):
    dp = lax.axis_index("dp")
    fs = lax.axis_index("fsdp")
    zh, zl, x = dp // 4, (dp // 2) % 2, dp % 2
    y, c = fs // 2, fs % 2
    rows, cols = hidden_ref.shape
    voc = head_hbm.shape[0]
    nch = rows // LANES
    half = LANES // 2
    feats = gw_ref.shape[0]
    groups_all = rows // length_max * n_dp // GROUP
    f32, bf = jnp.float32, jnp.bfloat16
    pick = (c + 1 - zl) % 2

    def span(i):
        return pl.ds(pl.multiple_of(i * LANES, LANES), LANES)

    def shard(j):
        return pl.ds(pl.multiple_of((fs ^ j) * cols, LANES), cols)

    def remote(src, dst, sems, at, to):
        return pltpu.make_async_remote_copy(
            src_ref=src,
            dst_ref=dst,
            send_sem=sems.at[(0, *at)],
            recv_sem=sems.at[(1, *at)],
            device_id=to,
            device_id_type=MESH,
        )

    core, across = (dp, fs ^ 1), (dp, fs ^ 2)
    near, side, far = (dp ^ 2, fs), (dp ^ 1, fs), (dp ^ 4, fs)

    def own_copy(i):
        return pltpu.make_async_copy(hidden_ref.at[span(i)], hs.at[0, span(i)], own_sem.at[i])

    head_copy = pltpu.make_async_copy(head_hbm, head, head_sem.at[0])

    def y_copy(i):
        return remote(hs.at[0, span(i)], hs.at[2, span(i)], ysem, (i,), across)

    def n_copy(i):
        return remote(hs.at[0, span(i)], hs.at[1, span(i)], nsem, (i,), core)

    def f_copy(i):
        return remote(hs.at[2, span(i)], hs.at[3, span(i)], fsem, (i,), core)

    def z_copy(k, i):
        part = pl.ds(pl.multiple_of(i * LANES + c * half, half), half)
        return remote(hs.at[2 * k + pick, part], hz.at[k, part], zsem, (k, i), near)

    def w_copy(k, i):
        part = pl.ds(pl.multiple_of(i * LANES + c * half, half), half)
        return remote(hz.at[k, part], hz.at[k, part], wsem, (k, i), core)

    def s_copy(j):
        return remote(small_ref, gain_in.at[j], ssem, (j,), (dp, fs ^ j))

    def m_copy(k):
        return remote(meta_out, meta_in.at[k], msem, (k,), (dp ^ k, fs))

    def t_copy(j, i):
        return remote(st_out.at[i], st_in.at[j, i], tsem, (j, i), (dp, fs ^ j))

    def l_copy(i):
        return remote(dls.at[i], dlz.at[i], lsem, (i,), near)

    def c_copy(k, i):
        return remote(c_out.at[k, span(i)], c_in.at[k, span(i)], csem, (k, i), core)

    def r_copy(i):
        return remote(y_out.at[span(i)], y_in.at[span(i)], rsem, (i,), across)

    def d_copy(j, i):
        return remote(d_out.at[i], d_in.at[j, i], dsem, (j, i), (dp, fs ^ j))

    def x_copy(k, p):
        return remote(x_out.at[k, span(p)], x_in.at[k, span(p)], xsem, (k, p), side)

    def h_copy(p):
        return remote(z_out.at[span(p)], z_in.at[span(p)], hsem, (p,), far)

    def g_copy(k):
        return remote(g_out, g_in.at[k], gsem, (k,), (dp ^ k, fs))

    for i in range(nch):
        own_copy(i).start()
    head_copy.start()

    barrier = pltpu.get_barrier_semaphore()
    for k in range(1, n_dp):
        pl.semaphore_signal(barrier, inc=1, device_id=(dp ^ k, fs), device_id_type=MESH)
    for k in range(1, n_fsdp):
        pl.semaphore_signal(barrier, inc=1, device_id=(dp, fs ^ k), device_id_type=MESH)
    pl.semaphore_wait(barrier, n_dp + n_fsdp - 2)

    @pl.loop(0, nch)
    def _(i):
        own_copy(i).wait()
        y_copy(i).start()
        n_copy(i).start()

    for j in range(1, n_fsdp):
        s_copy(j).start()

    reward = small_ref[4:5, :rows]
    group = small_ref[5:6, :rows]
    lens = small_ref[3:4, :rows]
    place = lax.broadcasted_iota(jnp.int32, (1, rows), 1) % length_max
    first_here = place == 0
    lane = lax.broadcasted_iota(jnp.int32, (8, LANES), 1)
    tile = jnp.where(
        lane == groups_all, jnp.sum(jnp.where(first_here, lens, 0.0), axis=1, keepdims=True), 0.0
    )
    for g in range(groups_all):
        mine = jnp.where(first_here & (group == float(g)), reward, 0.0)
        tile = jnp.where(lane == g, jnp.sum(mine, axis=1, keepdims=True), tile)
    meta_out[...] = tile
    for k in range(1, n_dp):
        m_copy(k).start()

    loss_s[...] = jnp.zeros_like(loss_s)
    g_out[...] = jnp.zeros_like(g_out)
    head_copy.wait()

    @pl.loop(0, nch)
    def _(i):
        n_copy(i).wait_recv()
        z_copy(0, i).start()

    gain_in[0] = small_ref[...]
    for j in range(1, n_fsdp):
        s_copy(j).wait_recv()
    total = meta_out[...]
    for k in range(1, n_dp):
        m_copy(k).wait_recv()
        total += meta_in[k]

    def entry(g):
        return jnp.sum(jnp.where(lane == g, total, 0.0), axis=1, keepdims=True)[:1]

    mean = jnp.zeros((1, rows), f32)
    for g in range(groups_all):
        mean = jnp.where(group == float(g), entry(g) / GROUP, mean)
    rowv[0:1] = reward - mean
    rowv[1:2] = jnp.where(place.astype(f32) < lens, 1.0, 0.0)
    cnt[...] = jnp.broadcast_to(entry(groups_all), cnt.shape)
    slots_all = rows * n_dp

    def hits_of(i):
        at = lax.broadcasted_iota(jnp.int32, (voc, LANES), 0) + fs * voc
        return at.astype(f32) == small_ref[1:2, span(i)]

    def forward(i):
        y_copy(i).wait_recv()
        f_copy(i).start()
        z_copy(0, i).wait_recv()
        w_copy(0, i).start()
        square = jnp.zeros((LANES, 1), f32)
        for j in range(3):
            h = hs[j, span(i)].astype(f32)
            square += jnp.sum(h * h, axis=1, keepdims=True)
        f_copy(i).wait_recv()
        z_copy(1, i).start()
        h = hs[3, span(i)].astype(f32)
        square += jnp.sum(h * h, axis=1, keepdims=True)
        inv = lax.rsqrt(square / (cols * n_fsdp) + eps_norm)
        inv_s[span(i)] = inv
        for j in range(n_fsdp):
            nm[j] = (hs[j, span(i)].astype(f32) * inv * gain_in[j, 0:1, :cols]).astype(bf)
        lg[i] = jnp.zeros((voc, LANES), f32)

        @pl.loop(0, n_fsdp)
        def _(j):
            lg[i] += lax.dot_general(
                head[:, shard(j)], nm[j], (((1,), (1,)), ((), ())), preferred_element_type=f32
            )

        logits = lg[i]
        top = jnp.max(logits, axis=0, keepdims=True)
        st_out[i, 0:1] = top
        st_out[i, 1:2] = jnp.sum(jnp.exp(logits - top), axis=0, keepdims=True)
        st_out[i, 2:3] = jnp.sum(jnp.where(hits_of(i), logits, 0.0), axis=0, keepdims=True)
        st_out[i, 3:8] = jnp.zeros((5, LANES), f32)
        for j in range(1, n_fsdp):
            t_copy(j, i).start()

    def backward(i):
        for j in range(1, n_fsdp):
            t_copy(j, i).wait_recv()
        stats = [st_out[i]] + [st_in[j, i] for j in range(1, n_fsdp)]
        top = stats[0][0:1]
        for s in stats[1:]:
            top = jnp.maximum(top, s[0:1])
        total = jnp.zeros_like(top)
        chosen = jnp.zeros_like(top)
        for s in stats:
            total += s[1:2] * jnp.exp(s[0:1] - top)
            chosen += s[2:3]
        lse = top + jnp.log(total)
        adv, mask = rowv[0:1, span(i)], rowv[1:2, span(i)]
        ratio = jnp.exp(chosen - lse - small_ref[2:3, span(i)])
        first = ratio * adv
        second = jnp.clip(ratio, clip_low, clip_high) * adv
        policy = -jnp.minimum(first, second)
        policy = jnp.where(adv < 0, jnp.minimum(policy, -dual_bound * adv), policy)
        loss_s[0:1] += mask * policy
        active = (first <= second) & jnp.logical_not((adv < 0) & (first < dual_bound * adv))
        slope = slots_all / cnt[0:1] * mask * jnp.where(active, -ratio * adv, 0.0)
        grad = slope * (hits_of(i).astype(f32) - jnp.exp(lg[i] - lse))
        inv_row = jnp.transpose(jnp.broadcast_to(inv_s[span(i)], (LANES, LANES)))[:1]
        dls[i] = (grad * inv_row).astype(bf)
        l_copy(i).start()
        left = jnp.transpose(grad).astype(bf)

        def dn(j):
            return jnp.dot(left, head[:, shard(j)], preferred_element_type=f32)

        c_out[1, span(i)] = dn(3).astype(bf)
        c_copy(1, i).start()
        c_out[0, span(i)] = dn(1).astype(bf)
        c_copy(0, i).start()
        z_copy(1, i).wait_recv()
        w_copy(1, i).start()
        acc[span(i)] = dn(2)
        c_copy(1, i).wait_recv()
        y_out[span(i)] = (acc[span(i)] + c_in[1, span(i)].astype(f32)).astype(bf)
        r_copy(i).start()
        acc[span(i)] = dn(0)
        c_copy(0, i).wait_recv()
        acc[span(i)] += c_in[0, span(i)].astype(f32)

    @pl.loop(0, nch + 1)
    def _(i):
        @pl.when(i < nch)
        def _():
            forward(i)

        @pl.when(i > 0)
        def _():
            backward(i - 1)

    def dots(i):
        r_copy(i).wait_recv()
        grad = acc[span(i)] + y_in[span(i)].astype(f32)
        acc[span(i)] = grad
        h = hs[0, span(i)].astype(f32)
        prod = grad * h
        g_out[:, :cols] += jnp.sum((prod * inv_s[span(i)]).reshape(LANES // 8, 8, cols), axis=0)
        part = jnp.sum(prod * gain_in[0, 0:1, :cols], axis=1, keepdims=True)
        d_out[i] = jnp.transpose(jnp.broadcast_to(part, (LANES, LANES)))[:8]
        for j in range(1, n_fsdp):
            d_copy(j, i).start()

    def finish(i):
        whole = d_out[i]
        for j in range(1, n_fsdp):
            d_copy(j, i).wait_recv()
            whole += d_in[j, i]
        column = jnp.transpose(jnp.broadcast_to(whole[:1], (LANES, LANES)))[:, :1]
        inv = inv_s[span(i)]
        scale = inv * inv * inv * column / (cols * n_fsdp)
        gh_ref[span(i)] = (
            inv * (acc[span(i)] * gain_in[0, 0:1, :cols])
            - hs[0, span(i)].astype(f32) * scale
        ).astype(bf)

    def dw(p, zb, xb):
        at = pl.ds(pl.multiple_of(xb * feats, LANES), feats)
        left = jnp.concatenate([dls[i, span(p)] for i in range(nch)], axis=1)
        other = jnp.concatenate([dlz[i, span(p)] for i in range(nch)], axis=1)
        return jnp.dot(
            left, hs[fs ^ (2 * zb + zl), :, at], preferred_element_type=f32
        ) + jnp.dot(other, hz[y ^ zb, :, at], preferred_element_type=f32)

    for i in range(nch):
        l_copy(i).wait_recv()
        w_copy(0, i).wait_recv()
        w_copy(1, i).wait_recv()

    @pl.loop(0, nch)
    def _(p):
        x_out[0, span(p)] = dw(p, 1 - zh, 1 - x).astype(bf)
        x_copy(0, p).start()

    @pl.loop(0, nch)
    def _(p):
        x_out[1, span(p)] = dw(p, zh, 1 - x).astype(bf)
        x_copy(1, p).start()
        dots(p)
        fin[span(p)] = dw(p, 1 - zh, x)
        x_copy(0, p).wait_recv()
        z_out[span(p)] = (fin[span(p)] + x_in[0, span(p)].astype(f32)).astype(bf)
        h_copy(p).start()
        finish(p)

    g_out[:, cols:] = loss_s[...]

    @pl.loop(1, n_dp)
    def _(k):
        g_copy(k).start()

    @pl.loop(0, nch)
    def _(p):
        fin[span(p)] = dw(p, zh, x)
        x_copy(1, p).wait_recv()
        fin[span(p)] += x_in[1, span(p)].astype(f32)

    gg_ref[...] = g_out[...]

    @pl.loop(1, n_dp)
    def _(k):
        g_copy(k).wait_recv()
        gg_ref[...] += g_in[k]

    gg_ref[:, cols:] = jnp.broadcast_to(
        jnp.sum(gg_ref[0:1, cols:], axis=1, keepdims=True) / cnt[0:1], (8, LANES)
    )
    gg_ref[0:1, :cols] = jnp.sum(gg_ref[:, :cols], axis=0, keepdims=True)

    mine = gain_in[fs ^ (2 * zh + zl), 0:1, pl.ds(pl.multiple_of(x * feats, LANES), feats)]
    for p in range(nch):
        h_copy(p).wait_recv()
        piece = (fin[span(p)] + z_in[span(p)].astype(f32)) * mine
        gw_ref[:, span(p)] = jnp.transpose(piece)

    @pl.loop(0, nch)
    def _(i):
        y_copy(i).wait_send()
        n_copy(i).wait_send()
        f_copy(i).wait_send()
        l_copy(i).wait_send()
        r_copy(i).wait_send()
        h_copy(i).wait_send()
        for k in range(2):
            z_copy(k, i).wait_send()
            w_copy(k, i).wait_send()
            c_copy(k, i).wait_send()
            x_copy(k, i).wait_send()
        for j in range(1, n_fsdp):
            t_copy(j, i).wait_send()
            d_copy(j, i).wait_send()

    for j in range(1, n_fsdp):
        s_copy(j).wait_send()

    @pl.loop(1, n_dp)
    def _(k):
        m_copy(k).wait_send()
        g_copy(k).wait_send()


def whole(small, hidden, head, length_max):
    n_dp, n_fsdp = lax.axis_size("dp"), lax.axis_size("fsdp")
    rows, cols = hidden.shape
    voc, width = head.shape
    feats = width // n_dp
    nch = rows // LANES
    wide = cols + LANES
    bf, f32 = jnp.bfloat16, jnp.float32
    vm = pl.BlockSpec(memory_space=pltpu.VMEM)
    anywhere = pl.BlockSpec(memory_space=pl.ANY)
    dma = pltpu.SemaphoreType.DMA
    return pl.pallas_call(
        functools.partial(whole_kernel, n_dp, n_fsdp, length_max),
        out_shape=(
            jax.ShapeDtypeStruct((rows, cols), bf),
            jax.ShapeDtypeStruct((feats, voc), f32),
            jax.ShapeDtypeStruct((8, wide), f32),
        ),
        in_specs=[vm, anywhere, anywhere],
        out_specs=(vm, vm, vm),
        scratch_shapes=[
            pltpu.VMEM((voc, width), bf),
            pltpu.VMEM((n_fsdp, rows, cols), bf),
            pltpu.VMEM((2, rows, cols), bf),
            pltpu.VMEM((n_fsdp, LANES, cols), bf),
            pltpu.VMEM((nch, voc, LANES), f32),
            pltpu.VMEM((rows, 1), f32),
            pltpu.VMEM((8, rows), f32),
            pltpu.VMEM((8, LANES), f32),
            pltpu.VMEM((8, LANES), f32),
            pltpu.VMEM((n_fsdp, *small.shape), f32),
            pltpu.VMEM((8, LANES), f32),
            pltpu.VMEM((n_dp, 8, LANES), f32),
            pltpu.VMEM((nch, 8, LANES), f32),
            pltpu.VMEM((n_fsdp, nch, 8, LANES), f32),
            pltpu.VMEM((nch, voc, LANES), bf),
            pltpu.VMEM((nch, voc, LANES), bf),
            pltpu.VMEM((2, rows, cols), bf),
            pltpu.VMEM((2, rows, cols), bf),
            pltpu.VMEM((rows, cols), bf),
            pltpu.VMEM((rows, cols), bf),
            pltpu.VMEM((rows, cols), f32),
            pltpu.VMEM((nch, 8, LANES), f32),
            pltpu.VMEM((n_fsdp, nch, 8, LANES), f32),
            pltpu.VMEM((2, voc, feats), bf),
            pltpu.VMEM((2, voc, feats), bf),
            pltpu.VMEM((voc, feats), bf),
            pltpu.VMEM((voc, feats), bf),
            pltpu.VMEM((voc, feats), f32),
            pltpu.VMEM((8, wide), f32),
            pltpu.VMEM((n_dp, 8, wide), f32),
            dma((nch,)),
            dma((1,)),
            dma((2, nch)),
            dma((2, nch)),
            dma((2, nch)),
            dma((2, 2, nch)),
            dma((2, 2, nch)),
            dma((2, n_fsdp)),
            dma((2, n_dp)),
            dma((2, n_fsdp, nch)),
            dma((2, nch)),
            dma((2, 2, nch)),
            dma((2, nch)),
            dma((2, n_fsdp, nch)),
            dma((2, 2, nch)),
            dma((2, nch)),
            dma((2, n_dp)),
        ],
        compiler_params=pltpu.CompilerParams(
            collective_id=1, has_side_effects=True, vmem_limit_bytes=60 * 1024 * 1024
        ),
    )(small, hidden, head)


def fits(hidden, head):
    n_dp, n_fsdp = lax.axis_size("dp"), lax.axis_size("fsdp")
    rows = hidden.shape[0] * hidden.shape[1]
    voc, width = head.shape
    return (
        n_dp == 2 * n_fsdp
        and n_fsdp == 2 * 2
        and (width // n_dp) % LANES == 0
        and rows % LANES == 0
        and rows == voc
        and rows <= hidden.shape[2]
    )


def body(hidden, gain, head, targets, lengths, old_logp, rewards, group_slot):
    if not fits(hidden, head):
        return general(hidden, gain, head, targets, lengths, old_logp, rewards, group_slot)
    resp_here, length_max, cols = hidden.shape
    rows = resp_here * length_max

    def row(values):
        flat = values.astype(jnp.float32).reshape(-1)
        return jnp.pad(flat, (0, cols - flat.shape[0]))

    def per_position(values):
        return row(jnp.broadcast_to(values[:, None], (resp_here, length_max)))

    small = jnp.stack(
        [
            row(gain),
            row(targets),
            row(old_logp),
            per_position(lengths),
            per_position(rewards),
            per_position(group_slot // GROUP),
            jnp.zeros((cols,), jnp.float32),
            jnp.zeros((cols,), jnp.float32),
        ]
    )
    grad_h, grad_head_t, sums = whole(small, hidden.reshape(rows, cols), head, length_max)
    loss = sums[0, cols]
    grad_gain = sums[0, :cols]
    return (loss, grad_h.reshape(resp_here, length_max, cols), grad_gain, grad_head_t)


def tail_kernel(
    n_dp,
    n_fsdp,
    feats,
    normed_ref,
    dlogits_ref,
    head_ref,
    hidden_ref,
    gain_ref,
    inv_ref,
    loss_ref,
    gh_ref,
    gw_ref,
    gg_ref,
    x_out,
    x_in,
    n_out,
    n_in,
    z_out,
    z_in,
    c_out,
    c_in,
    y_out,
    y_in,
    acc,
    d_out,
    d_in,
    g_out,
    g_in,
    xs,
    xr,
    ns,
    nr,
    zs,
    zr,
    cs,
    cr,
    ys,
    yr,
    ds_,
    dr,
    gs,
    gr,
):
    dp = lax.axis_index("dp")
    fs = lax.axis_index("fsdp")
    z, x = dp // 2, dp % 2
    y, c = fs // 2, fs % 2
    outer_dp, outer_fs, quads = n_dp // 2, n_fsdp // 2, n_dp // 4
    cols = hidden_ref.shape[1]

    barrier = pltpu.get_barrier_semaphore()
    for k in range(1, n_dp):
        pl.semaphore_signal(barrier, inc=1, device_id=(dp ^ k, fs), device_id_type=MESH)
    for k in range(1, n_fsdp):
        pl.semaphore_signal(barrier, inc=1, device_id=(dp, fs ^ k), device_id_type=MESH)
    pl.semaphore_wait(barrier, n_dp + n_fsdp - 2)

    def remote(out, into, send, recv, k, dst):
        return pltpu.make_async_remote_copy(
            src_ref=out,
            dst_ref=into.at[k],
            send_sem=send.at[k],
            recv_sem=recv.at[k],
            device_id=dst,
            device_id_type=MESH,
        )

    def x_copy(k):
        return remote(x_out.at[k], x_in, xs, xr, k, (dp ^ 1, fs))

    def z_copy(k):
        return remote(z_out.at[k], z_in, zs, zr, k, (dp ^ (4 * k), fs))

    def n_copy(k):
        return remote(n_out.at[k], n_in, ns, nr, k, (dp ^ 2, fs))

    def c_copy(j):
        return remote(c_out.at[j], c_in, cs, cr, j, (dp, fs ^ 1))

    def y_copy(j):
        return remote(y_out.at[j], y_in, ys, yr, j, (dp, (y ^ j) * 2 + c))

    def d_copy(j):
        return remote(d_out, d_in, ds_, dr, j, (dp, fs ^ j))

    def g_copy(k):
        return remote(g_out, g_in, gs, gr, k, (dp ^ k, fs))

    def dw(block):
        if feats % 128 == 0:
            left = normed_ref[:, pl.ds(pl.multiple_of(block * feats, 128), feats)]
        else:
            left = normed_ref[block]
        return lax.dot_general(
            left, dlogits_ref[...], (((0,), (0,)), ((), ())), preferred_element_type=jnp.float32
        )

    def dn(block):
        right = head_ref[:, pl.ds(pl.multiple_of(block * cols, 128), cols)]
        return jnp.dot(dlogits_ref[...], right, preferred_element_type=jnp.float32)

    @pl.loop(0, outer_dp)
    def _(i):
        k = outer_dp - 1 - i
        x_out[k] = dw((z ^ k) * 2 + (1 - x)).astype(jnp.bfloat16)
        x_copy(k).start()

    @pl.loop(0, outer_fs)
    def _(i):
        j = outer_fs - 1 - i
        c_out[j] = dn((y ^ j) * 2 + (1 - c)).astype(jnp.bfloat16)
        c_copy(j).start()

    @pl.loop(0, outer_fs - 1)
    def _(i):
        j = outer_fs - 1 - i
        mine = dn((y ^ j) * 2 + c)
        c_copy(j).wait_recv()
        y_out[j] = (mine + c_in[j].astype(jnp.float32)).astype(jnp.bfloat16)
        y_copy(j).start()

    acc[...] = dn(fs)
    c_copy(0).wait_recv()
    acc[...] += c_in[0].astype(jnp.float32)

    def pair_sum(k):
        mine = dw((z ^ k) * 2 + x)
        x_copy(k).wait_recv()
        return mine + x_in[k].astype(jnp.float32)

    def to_near(q):
        n_out[q] = pair_sum(2 * q + 1).astype(jnp.bfloat16)
        n_copy(q).start()

    @pl.loop(0, quads - 1)
    def _(i):
        q = quads - 1 - i
        to_near(q)
        mine = pair_sum(2 * q)
        n_copy(q).wait_recv()
        z_out[q] = (mine + n_in[q].astype(jnp.float32)).astype(jnp.bfloat16)
        z_copy(q).start()

    to_near(0)

    @pl.loop(1, outer_fs)
    def _(j):
        y_copy(j).wait_recv()
        acc[...] += y_in[j].astype(jnp.float32)

    h = hidden_ref[...].astype(jnp.float32)
    inv = inv_ref[...]
    g_out[:, :cols] = jnp.broadcast_to(
        jnp.sum(acc[...] * h * inv, axis=0, keepdims=True), (8, cols)
    )
    g_out[:, cols:] = loss_ref[...]

    @pl.loop(1, n_dp)
    def _(k):
        g_copy(k).start()

    dy = acc[...] * gain_ref[...]
    part = jnp.sum(h * dy, axis=1, keepdims=True)
    rows = part.shape[0]
    d_out[...] = jnp.transpose(jnp.broadcast_to(part, (rows, 128)))[:8]
    for j in range(1, n_fsdp):
        d_copy(j).start()
    dots = d_out[...]
    for j in range(1, n_fsdp):
        d_copy(j).wait_recv()
        dots += d_in[j]
    column = jnp.transpose(jnp.broadcast_to(dots[:1], (128, rows)))[:, :1]
    scale = inv * inv * inv * column / (cols * n_fsdp)
    gh_ref[...] = (
        inv * (acc[...] * gain_ref[...]) - hidden_ref[...].astype(jnp.float32) * scale
    ).astype(jnp.bfloat16)

    gg_ref[...] = g_out[...]

    @pl.loop(1, n_dp)
    def _(k):
        g_copy(k).wait_recv()
        gg_ref[...] += g_in[k]

    gw_ref[...] = pair_sum(0)
    n_copy(0).wait_recv()
    gw_ref[...] += n_in[0].astype(jnp.float32)

    @pl.loop(1, quads)
    def _(k):
        z_copy(k).wait_recv()
        gw_ref[...] += z_in[k].astype(jnp.float32)

    @pl.loop(0, outer_dp)
    def _(k):
        x_copy(k).wait_send()

    @pl.loop(0, quads)
    def _(k):
        n_copy(k).wait_send()

    @pl.loop(1, quads)
    def _(k):
        z_copy(k).wait_send()

    @pl.loop(0, outer_fs)
    def _(j):
        c_copy(j).wait_send()

    @pl.loop(1, outer_fs)
    def _(j):
        y_copy(j).wait_send()

    for j in range(1, n_fsdp):
        d_copy(j).wait_send()

    @pl.loop(1, n_dp)
    def _(k):
        g_copy(k).wait_send()


def tail(normed, dlogits, head, hidden, gain_row, inv, loss_tile):
    n_dp, n_fsdp = lax.axis_size("dp"), lax.axis_size("fsdp")
    rows, width = normed.shape
    vocab_here = head.shape[0]
    cols = hidden.shape[1]
    feats = width // n_dp
    zd, qd, yd = n_dp // 2, n_dp // 4, n_fsdp // 2
    if feats % 128:
        normed = normed.reshape(rows, n_dp, feats).transpose(1, 0, 2)
    wide = cols + 128
    bf, f32 = jnp.bfloat16, jnp.float32
    vm = pl.BlockSpec(memory_space=pltpu.VMEM)
    dma = pltpu.SemaphoreType.DMA
    return pl.pallas_call(
        functools.partial(tail_kernel, n_dp, n_fsdp, feats),
        out_shape=(
            jax.ShapeDtypeStruct((rows, cols), bf),
            jax.ShapeDtypeStruct((feats, vocab_here), f32),
            jax.ShapeDtypeStruct((8, wide), f32),
        ),
        in_specs=[vm] * 7,
        out_specs=(vm, vm, vm),
        scratch_shapes=[
            pltpu.VMEM((zd, feats, vocab_here), bf),
            pltpu.VMEM((zd, feats, vocab_here), bf),
            pltpu.VMEM((qd, feats, vocab_here), bf),
            pltpu.VMEM((qd, feats, vocab_here), bf),
            pltpu.VMEM((qd, feats, vocab_here), bf),
            pltpu.VMEM((qd, feats, vocab_here), bf),
            pltpu.VMEM((yd, rows, cols), bf),
            pltpu.VMEM((yd, rows, cols), bf),
            pltpu.VMEM((yd, rows, cols), bf),
            pltpu.VMEM((yd, rows, cols), bf),
            pltpu.VMEM((rows, cols), f32),
            pltpu.VMEM((8, rows), f32),
            pltpu.VMEM((n_fsdp, 8, rows), f32),
            pltpu.VMEM((8, wide), f32),
            pltpu.VMEM((n_dp, 8, wide), f32),
        ]
        + [dma((n,)) for n in (zd, zd, qd, qd, qd, qd, yd, yd, yd, yd, n_fsdp, n_fsdp, n_dp, n_dp)],
        compiler_params=pltpu.CompilerParams(
            collective_id=0, has_side_effects=True, vmem_limit_bytes=60 * 1024 * 1024
        ),
    )(normed, dlogits, head, hidden, gain_row, inv, loss_tile)


def general(hidden, gain, head, targets, lengths, old_logp, rewards, group_slot):
    resp_here, length_max, shard_cols = hidden.shape
    rows = resp_here * length_max
    whole, gain_full = (
        lax.all_gather(hidden, "fsdp", axis=2, tiled=True),
        lax.all_gather(gain, "fsdp", axis=0, tiled=True),
    )
    width = whole.shape[2]
    whole = whole.reshape(rows, width)
    vocab_here = head.shape[0]
    vocab_start = lax.axis_index("fsdp") * vocab_here
    groups_all = resp_here * lax.axis_size("dp") // GROUP
    group = group_slot // GROUP
    member = (group[:, None] == jnp.arange(groups_all, dtype=jnp.int32)[None, :]).astype(
        jnp.float32
    )
    local_sums = jnp.sum(member * rewards[:, None], axis=0)
    local_count = jnp.sum(lengths).astype(jnp.float32)
    group_sums, count = lax.psum((local_sums, local_count), "dp")
    adv_resp = rewards - jnp.sum(member * group_sums[None, :], axis=1) / GROUP
    adv = jnp.repeat(adv_resp, length_max)
    mask = (
        (jnp.arange(length_max, dtype=jnp.int32)[None, :] < lengths[:, None])
        .astype(jnp.float32)
        .reshape(rows)
    )
    gain_f = gain_full.astype(jnp.float32)
    inv = lax.rsqrt(
        jnp.mean(jnp.square(whole.astype(jnp.float32)), axis=1, keepdims=True) + eps_norm
    )
    normed = (whole.astype(jnp.float32) * inv * gain_f).astype(jnp.bfloat16)
    logits = lax.dot_general(
        normed, head, (((1,), (1,)), ((), ())), preferred_element_type=jnp.float32
    )
    top_local = jnp.max(logits, axis=1)
    sum_local = jnp.sum(jnp.exp(logits - top_local[:, None]), axis=1)
    local_targets = targets.reshape(rows) - vocab_start
    hits = jnp.arange(vocab_here, dtype=jnp.int32)[None, :] == local_targets[:, None]
    chosen_local = jnp.sum(jnp.where(hits, logits, 0.0), axis=1)
    stats = lax.all_gather(jnp.stack([top_local, sum_local, chosen_local]), "fsdp", axis=0)
    top = jnp.max(stats[:, 0], axis=0)
    total = jnp.sum(stats[:, 1] * jnp.exp(stats[:, 0] - top[None, :]), axis=0)
    chosen = jnp.sum(stats[:, 2], axis=0)
    lse = top + jnp.log(total)
    logp = chosen - lse
    ratio = jnp.exp(logp - old_logp.reshape(rows))
    first = ratio * adv
    second = jnp.clip(ratio, clip_low, clip_high) * adv
    policy = -jnp.minimum(first, second)
    policy = jnp.where(adv < 0, jnp.minimum(policy, -dual_bound * adv), policy)
    loss_local = jnp.sum(mask * policy)
    active = (first <= second) & jnp.logical_not((adv < 0) & (first < dual_bound * adv))
    slots_all = rows * lax.axis_size("dp")
    grad_logp = slots_all / count * mask * jnp.where(active, -ratio * adv, 0.0)
    probs = jnp.exp(logits - lse[:, None])
    dlogits = (grad_logp[:, None] * (hits.astype(jnp.float32) - probs)).astype(jnp.bfloat16)
    grad_h, grad_head_t, sums = tail(
        normed,
        dlogits,
        head,
        hidden.reshape(rows, shard_cols),
        gain.astype(jnp.float32)[None, :],
        inv,
        jnp.broadcast_to(loss_local, (8, 128)),
    )
    loss = sums[0, shard_cols] / count
    grad_gain = sums[0, :shard_cols]
    grad_hidden = grad_h.reshape(resp_here, length_max, shard_cols)
    return (loss, grad_hidden, grad_gain, grad_head_t)


def solution(mesh):
    in_specs = (
        P("dp", None, "fsdp"),
        P("fsdp"),
        P("fsdp", None),
        P("dp", None),
        P("dp"),
        P("dp", None),
        P("dp"),
        P("dp"),
    )
    out_specs = (P(), P("dp", None, "fsdp"), P("fsdp"), P("dp", "fsdp"))
    return jax.shard_map(body, mesh=mesh, in_specs=in_specs, out_specs=out_specs, check_vma=False)
```

```python
import functools
import jax
import jax.numpy as jnp
from jax import lax
from jax.experimental import pallas as pl
from jax.experimental.pallas import tpu as pltpu
from jax.sharding import PartitionSpec as P

GROUP = 8
LANES = 128


eps_norm = 1e-06
clip_low = 0.8
clip_high = 1.2
dual_bound = 3.0


MESH = pl.DeviceIdType.MESH


def whole_kernel(
    n_dp,
    n_fsdp,
    length_max,
    gain_ref,
    targets_hbm,
    old_hbm,
    lengths_hbm,
    rewards_hbm,
    slots_hbm,
    hidden_ref,
    head_hbm,
    gh_ref,
    gw_ref,
    gg_ref,
    targets,
    old,
    lengths,
    rewards,
    slots,
    target_rows,
    old_rows,
    adv_rows,
    mask_rows,
    head,
    hs,
    hz,
    nm,
    lg,
    inv_s,
    cnt,
    loss_s,
    gain_in,
    meta_out,
    meta_in,
    st_out,
    st_in,
    dls,
    dlz,
    c_out,
    c_in,
    y_out,
    y_in,
    acc,
    d_out,
    d_in,
    x_out,
    x_in,
    z_out,
    z_in,
    fin,
    gsum,
    g_out,
    g_in,
    own_sem,
    head_sem,
    small_sem,
    ysem,
    nsem,
    fsem,
    zsem,
    wsem,
    ssem,
    msem,
    tsem,
    lsem,
    csem,
    rsem,
    dsem,
    xsem,
    hsem,
    gsem,
):
    dp = lax.axis_index("dp")
    fs = lax.axis_index("fsdp")
    zh, zl, x = dp // 4, (dp // 2) % 2, dp % 2
    y, c = fs // 2, fs % 2
    rows, cols = hidden_ref.shape
    voc = head_hbm.shape[0]
    nch = rows // LANES
    half = LANES // 2
    feats = gw_ref.shape[0]
    resp_here = rows // length_max
    groups_all = resp_here * n_dp // GROUP
    f32, bf = jnp.float32, jnp.bfloat16
    pick = (c + 1 - zl) % 2

    def span(i):
        return pl.ds(pl.multiple_of(i * LANES, LANES), LANES)

    def piece(p):
        return pl.ds(pl.multiple_of(p * half, half), half)

    def shard(j):
        return pl.ds(pl.multiple_of((fs ^ j) * cols, LANES), cols)

    def remote(src, dst, sems, at, to):
        return pltpu.make_async_remote_copy(
            src_ref=src,
            dst_ref=dst,
            send_sem=sems.at[(0, *at)],
            recv_sem=sems.at[(1, *at)],
            device_id=to,
            device_id_type=MESH,
        )

    core, across = (dp, fs ^ 1), (dp, fs ^ 2)
    near, side, far = (dp ^ 2, fs), (dp ^ 1, fs), (dp ^ 4, fs)

    def own_copy(i):
        return pltpu.make_async_copy(hidden_ref.at[span(i)], hs.at[0, span(i)], own_sem.at[i])

    head_copy = pltpu.make_async_copy(head_hbm, head, head_sem.at[0])

    def y_copy(i):
        return remote(hs.at[0, span(i)], hs.at[2, span(i)], ysem, (i,), across)

    def n_copy(i):
        return remote(hs.at[0, span(i)], hs.at[1, span(i)], nsem, (i,), core)

    def f_copy(i):
        return remote(hs.at[2, span(i)], hs.at[3, span(i)], fsem, (i,), core)

    def z_copy(k, i):
        part = pl.ds(pl.multiple_of(i * LANES + c * half, half), half)
        return remote(hs.at[2 * k + pick, part], hz.at[k, part], zsem, (k, i), near)

    def w_copy(k, i):
        part = pl.ds(pl.multiple_of(i * LANES + c * half, half), half)
        return remote(hz.at[k, part], hz.at[k, part], wsem, (k, i), core)

    def s_copy(j):
        return remote(gain_ref, gain_in.at[j], ssem, (j,), (dp, fs ^ j))

    def m_copy(k):
        return remote(meta_out, meta_in.at[k], msem, (k,), (dp ^ k, fs))

    def t_copy(j, i):
        return remote(st_out.at[i], st_in.at[j, i], tsem, (j, i), (dp, fs ^ j))

    def l_copy(i):
        return remote(dls.at[i], dlz.at[i], lsem, (i,), near)

    def c_copy(k, i):
        return remote(c_out.at[k, span(i)], c_in.at[k, span(i)], csem, (k, i), core)

    def r_copy(i):
        return remote(y_out.at[span(i)], y_in.at[span(i)], rsem, (i,), across)

    def d_copy(j, i):
        return remote(d_out.at[i], d_in.at[j, i], dsem, (j, i), (dp, fs ^ j))

    def x_copy(k, p):
        return remote(x_out.at[k, piece(p)], x_in.at[k, piece(p)], xsem, (k, p), side)

    def h_copy(p):
        return remote(z_out.at[piece(p)], z_in.at[piece(p)], hsem, (p,), far)

    def g_copy(k):
        return remote(g_out, g_in.at[k], gsem, (k,), (dp ^ k, fs))

    barrier = pltpu.get_barrier_semaphore()
    for k in range(1, n_dp):
        pl.semaphore_signal(barrier, inc=1, device_id=(dp ^ k, fs), device_id_type=MESH)
    for k in range(1, n_fsdp):
        pl.semaphore_signal(barrier, inc=1, device_id=(dp, fs ^ k), device_id_type=MESH)
    loads = [
        pltpu.make_async_copy(src, dst, small_sem.at[n])
        for n, (src, dst) in enumerate(
            [
                (slots_hbm, slots),
                (rewards_hbm, rewards),
                (lengths_hbm, lengths),
                (targets_hbm, targets),
                (old_hbm, old),
            ]
        )
    ]
    for load in loads:
        load.start()
    for i in range(nch):
        own_copy(i).start()
    head_copy.start()
    for load in loads:
        load.wait()

    lane = lax.broadcasted_iota(jnp.int32, (8, LANES), 1)
    tile = jnp.zeros((8, LANES), f32)
    for r in range(resp_here):
        tile += jnp.where(lane == slots[r] // GROUP, rewards[r], 0.0)
        tile += jnp.where(lane == groups_all, lengths[r].astype(f32), 0.0)
    meta_out[...] = tile

    pl.semaphore_wait(barrier, n_dp + n_fsdp - 2)

    for j in range(1, n_fsdp):
        s_copy(j).start()
    for k in range(1, n_dp):
        m_copy(k).start()

    @pl.loop(0, nch)
    def _(i):
        own_copy(i).wait()
        n_copy(i).start()

        @pl.when(i < 2)
        def _():
            y_copy(i).start()

    loss_s[...] = jnp.zeros_like(loss_s)
    gsum[...] = jnp.zeros_like(gsum)
    head_copy.wait()

    @pl.loop(0, nch)
    def _(i):
        n_copy(i).wait_recv()
        z_copy(0, i).start()

    gain_in[0] = gain_ref[...]
    for j in range(1, n_fsdp):
        s_copy(j).wait_recv()
    total = meta_out[...]
    for k in range(1, n_dp):
        m_copy(k).wait_recv()
        total += meta_in[k]

    def entry(g):
        return jnp.sum(jnp.where(lane == g, total, 0.0), axis=1, keepdims=True)[:1]

    for i in range(nch):
        r, first = i * LANES // length_max, i * LANES % length_max
        position = lax.broadcasted_iota(jnp.int32, (1, LANES), 1) + first
        target_rows[i] = targets[r : r + 1, first : first + LANES]
        old_rows[i] = old[r : r + 1, first : first + LANES]
        mask_rows[i] = jnp.where(position < lengths[r], 1.0, 0.0)
        adv = rewards[r] - entry(slots[r] // GROUP) / GROUP
        adv_rows[i] = jnp.broadcast_to(adv, (1, LANES))
    cnt[...] = jnp.broadcast_to(entry(groups_all), cnt.shape)
    slots_all = rows * n_dp

    def hits_of(i):
        at = lax.broadcasted_iota(jnp.int32, (voc, LANES), 0) + fs * voc
        return at == target_rows[i]

    def forward(i):
        y_copy(i).wait_recv()
        f_copy(i).start()
        z_copy(0, i).wait_recv()
        w_copy(0, i).start()
        square = jnp.zeros((LANES, 1), f32)
        for j in range(3):
            h = hs[j, span(i)].astype(f32)
            square += jnp.sum(h * h, axis=1, keepdims=True)
        f_copy(i).wait_recv()
        z_copy(1, i).start()
        h = hs[3, span(i)].astype(f32)
        square += jnp.sum(h * h, axis=1, keepdims=True)
        inv = lax.rsqrt(square / (cols * n_fsdp) + eps_norm)
        inv_s[span(i)] = inv
        for j in range(n_fsdp):
            nm[j] = (hs[j, span(i)].astype(f32) * inv * gain_in[j]).astype(bf)
        lg[i] = jnp.zeros((voc, LANES), f32)

        @pl.loop(0, n_fsdp)
        def _(j):
            lg[i] += lax.dot_general(
                head[:, shard(j)], nm[j], (((1,), (1,)), ((), ())), preferred_element_type=f32
            )

        logits = lg[i]
        top = jnp.max(logits, axis=0, keepdims=True)
        st_out[i, 0:1] = top
        st_out[i, 1:2] = jnp.sum(jnp.exp(logits - top), axis=0, keepdims=True)
        st_out[i, 2:3] = jnp.sum(jnp.where(hits_of(i), logits, 0.0), axis=0, keepdims=True)
        st_out[i, 3:8] = jnp.zeros((5, LANES), f32)
        for j in range(1, n_fsdp):
            t_copy(j, i).start()

        @pl.when(i + 2 < nch)
        def _():
            y_copy(i + 2).start()

    def backward(i):
        for j in range(1, n_fsdp):
            t_copy(j, i).wait_recv()
        stats = [st_out[i]] + [st_in[j, i] for j in range(1, n_fsdp)]
        top = stats[0][0:1]
        for s in stats[1:]:
            top = jnp.maximum(top, s[0:1])
        total = jnp.zeros_like(top)
        chosen = jnp.zeros_like(top)
        for s in stats:
            total += s[1:2] * jnp.exp(s[0:1] - top)
            chosen += s[2:3]
        lse = top + jnp.log(total)
        adv, mask = adv_rows[i], mask_rows[i]
        ratio = jnp.exp(chosen - lse - old_rows[i])
        first = ratio * adv
        second = jnp.clip(ratio, clip_low, clip_high) * adv
        policy = -jnp.minimum(first, second)
        policy = jnp.where(adv < 0, jnp.minimum(policy, -dual_bound * adv), policy)
        loss_s[0:1] += mask * policy
        active = (first <= second) & jnp.logical_not((adv < 0) & (first < dual_bound * adv))
        slope = slots_all / cnt[0:1] * mask * jnp.where(active, -ratio * adv, 0.0)
        grad = slope * (hits_of(i).astype(f32) - jnp.exp(lg[i] - lse))
        inv_row = jnp.transpose(jnp.broadcast_to(inv_s[span(i)], (LANES, LANES)))[:1]
        dls[i] = (grad * inv_row).astype(bf)
        l_copy(i).start()
        left = jnp.transpose(grad).astype(bf)

        def dn(j):
            return jnp.dot(left, head[:, shard(j)], preferred_element_type=f32)

        c_out[1, span(i)] = dn(3).astype(bf)
        c_copy(1, i).start()
        c_out[0, span(i)] = dn(1).astype(bf)
        c_copy(0, i).start()
        z_copy(1, i).wait_recv()
        w_copy(1, i).start()
        acc[span(i)] = dn(2)
        c_copy(1, i).wait_recv()
        y_out[span(i)] = (acc[span(i)] + c_in[1, span(i)].astype(f32)).astype(bf)

        @pl.when(i == nch - 2)
        def _():
            for n in range(nch - 1):
                r_copy(n).start()

        @pl.when(i == nch - 1)
        def _():
            r_copy(i).start()

        acc[span(i)] = dn(0)
        c_copy(0, i).wait_recv()
        acc[span(i)] += c_in[0, span(i)].astype(f32)

    @pl.loop(0, nch + 1)
    def _(i):
        @pl.when(i < nch)
        def _():
            forward(i)

        @pl.when(i > 0)
        def _():
            backward(i - 1)

    def dots(i):
        r_copy(i).wait_recv()
        grad = acc[span(i)] + y_in[span(i)].astype(f32)
        acc[span(i)] = grad
        h = hs[0, span(i)].astype(f32)
        prod = grad * h
        gsum[...] += jnp.sum((prod * inv_s[span(i)]).reshape(LANES // 8, 8, cols), axis=0)
        part = jnp.sum(prod * gain_in[0], axis=1, keepdims=True)
        d_out[i] = jnp.transpose(jnp.broadcast_to(part, (LANES, LANES)))[:8]
        for j in range(1, n_fsdp):
            d_copy(j, i).start()

    def finish(i):
        whole = d_out[i]
        for j in range(1, n_fsdp):
            d_copy(j, i).wait_recv()
            whole += d_in[j, i]
        column = jnp.transpose(jnp.broadcast_to(whole[:1], (LANES, LANES)))[:, :1]
        inv = inv_s[span(i)]
        scale = inv * inv * inv * column / (cols * n_fsdp)
        gh_ref[span(i)] = (
            inv * (acc[span(i)] * gain_in[0])
            - hs[0, span(i)].astype(f32) * scale
        ).astype(bf)

    def dw(p, zb, xb):
        at = pl.ds(pl.multiple_of(xb * feats, LANES), feats)
        left = jnp.concatenate([dls[i, span(p)] for i in range(nch)], axis=1)
        other = jnp.concatenate([dlz[i, span(p)] for i in range(nch)], axis=1)
        return jnp.dot(
            left, hs[fs ^ (2 * zb + zl), :, at], preferred_element_type=f32
        ) + jnp.dot(other, hz[y ^ zb, :, at], preferred_element_type=f32)

    for i in range(nch):
        l_copy(i).wait_recv()
        w_copy(0, i).wait_recv()
        w_copy(1, i).wait_recv()

    @pl.loop(0, nch)
    def _(p):
        x_out[0, span(p)] = dw(p, 1 - zh, 1 - x).astype(bf)
        x_copy(0, 2 * p).start()
        x_copy(0, 2 * p + 1).start()

    @pl.loop(0, nch)
    def _(p):
        x_out[1, span(p)] = dw(p, zh, 1 - x).astype(bf)
        x_copy(1, 2 * p).start()
        x_copy(1, 2 * p + 1).start()
        fin[span(p)] = dw(p, 1 - zh, x)

        @pl.loop(2 * p, 2 * p + 2)
        def _(q):
            x_copy(0, q).wait_recv()
            z_out[piece(q)] = (fin[piece(q)] + x_in[0, piece(q)].astype(f32)).astype(bf)
            h_copy(q).start()

        dots(p)

    nb = cols // LANES
    column_sums = jnp.sum(gsum[...], axis=0, keepdims=True)
    g_out[...] = jnp.zeros_like(g_out)
    for b in range(nb):
        g_out[b : b + 1] = column_sums[:, b * LANES : (b + 1) * LANES]
    g_out[nb : nb + 1] = loss_s[0:1]

    @pl.loop(1, n_dp)
    def _(k):
        g_copy(k).start()

    @pl.loop(0, nch)
    def _(p):
        fin[span(p)] = dw(p, zh, x)
        finish(p)

    @pl.loop(0, nch)
    def _(p):
        x_copy(1, 2 * p).wait_recv()
        x_copy(1, 2 * p + 1).wait_recv()
        fin[span(p)] += x_in[1, span(p)].astype(f32)

    mine = gain_in[fs ^ (2 * zh + zl), :, pl.ds(pl.multiple_of(x * feats, LANES), feats)]
    for p in range(nch):
        h_copy(2 * p).wait_recv()
        h_copy(2 * p + 1).wait_recv()
        gw_ref[:, span(p)] = jnp.transpose((fin[span(p)] + z_in[span(p)].astype(f32)) * mine)

    gg_ref[...] = g_out[...]

    @pl.loop(1, n_dp)
    def _(k):
        g_copy(k).wait_recv()
        gg_ref[...] += g_in[k]

    gg_ref[nb : nb + 1] = jnp.sum(gg_ref[nb : nb + 1], axis=1, keepdims=True) / cnt[0:1]

    @pl.loop(0, nch)
    def _(i):
        y_copy(i).wait_send()
        n_copy(i).wait_send()
        f_copy(i).wait_send()
        l_copy(i).wait_send()
        r_copy(i).wait_send()
        for q in range(2):
            h_copy(2 * i + q).wait_send()
            x_copy(0, 2 * i + q).wait_send()
            x_copy(1, 2 * i + q).wait_send()
        for k in range(2):
            z_copy(k, i).wait_send()
            w_copy(k, i).wait_send()
            c_copy(k, i).wait_send()
        for j in range(1, n_fsdp):
            t_copy(j, i).wait_send()
            d_copy(j, i).wait_send()

    for j in range(1, n_fsdp):
        s_copy(j).wait_send()

    @pl.loop(1, n_dp)
    def _(k):
        m_copy(k).wait_send()
        g_copy(k).wait_send()


def write_kernel(gh_ref, gw_ref, gg_ref, loss_out, gh_out, gg_out, gw_out, sems):
    copies = [
        pltpu.make_async_copy(gh_ref, gh_out, sems.at[0]),
        pltpu.make_async_copy(gw_ref, gw_out, sems.at[1]),
    ]
    for copy in copies:
        copy.start()
    nb = gg_out.shape[0]
    gg_out[...] = gg_ref[:nb]
    loss_out[...] = gg_ref[nb : nb + 1, :1]
    for copy in copies:
        copy.wait()


def write(gh, gw, gg, nb):
    vm = pl.BlockSpec(memory_space=pltpu.VMEM)
    anywhere = pl.BlockSpec(memory_space=pl.ANY)
    return pl.pallas_call(
        write_kernel,
        out_shape=(
            jax.ShapeDtypeStruct((1, 1), jnp.float32),
            jax.ShapeDtypeStruct(gh.shape, gh.dtype),
            jax.ShapeDtypeStruct((nb, LANES), jnp.float32),
            jax.ShapeDtypeStruct(gw.shape, gw.dtype),
        ),
        in_specs=[vm, vm, vm],
        out_specs=(vm, anywhere, vm, anywhere),
        scratch_shapes=[pltpu.SemaphoreType.DMA((2,))],
        compiler_params=pltpu.CompilerParams(vmem_limit_bytes=8 * 1024 * 1024),
    )(gh, gw, gg)


def whole(gain_row, targets, old_logp, lengths, rewards, group_slot, hidden, head):
    n_dp, n_fsdp = lax.axis_size("dp"), lax.axis_size("fsdp")
    resp_here, length_max = targets.shape
    rows, cols = hidden.shape
    voc, width = head.shape
    feats = width // n_dp
    nch = rows // LANES
    tall = (cols // LANES + 8) // 8 * 8
    bf, f32 = jnp.bfloat16, jnp.float32
    vm = pl.BlockSpec(memory_space=pltpu.VMEM)
    anywhere = pl.BlockSpec(memory_space=pl.ANY)
    dma = pltpu.SemaphoreType.DMA
    return pl.pallas_call(
        functools.partial(whole_kernel, n_dp, n_fsdp, length_max),
        out_shape=(
            pltpu.VMEM((rows, cols), bf),
            pltpu.VMEM((feats, voc), f32),
            pltpu.VMEM((tall, LANES), f32),
        ),
        in_specs=[vm] + [anywhere] * 7,
        out_specs=(vm, vm, vm),
        scratch_shapes=[
            pltpu.VMEM((resp_here, length_max), jnp.int32),
            pltpu.VMEM((resp_here, length_max), f32),
            pltpu.SMEM((resp_here,), jnp.int32),
            pltpu.SMEM((resp_here,), f32),
            pltpu.SMEM((resp_here,), jnp.int32),
            pltpu.VMEM((nch, 1, LANES), jnp.int32),
            pltpu.VMEM((nch, 1, LANES), f32),
            pltpu.VMEM((nch, 1, LANES), f32),
            pltpu.VMEM((nch, 1, LANES), f32),
            pltpu.VMEM((voc, width), bf),
            pltpu.VMEM((n_fsdp, rows, cols), bf),
            pltpu.VMEM((2, rows, cols), bf),
            pltpu.VMEM((n_fsdp, LANES, cols), bf),
            pltpu.VMEM((nch, voc, LANES), f32),
            pltpu.VMEM((rows, 1), f32),
            pltpu.VMEM((8, LANES), f32),
            pltpu.VMEM((8, LANES), f32),
            pltpu.VMEM((n_fsdp, 1, cols), f32),
            pltpu.VMEM((8, LANES), f32),
            pltpu.VMEM((n_dp, 8, LANES), f32),
            pltpu.VMEM((nch, 8, LANES), f32),
            pltpu.VMEM((n_fsdp, nch, 8, LANES), f32),
            pltpu.VMEM((nch, voc, LANES), bf),
            pltpu.VMEM((nch, voc, LANES), bf),
            pltpu.VMEM((2, rows, cols), bf),
            pltpu.VMEM((2, rows, cols), bf),
            pltpu.VMEM((rows, cols), bf),
            pltpu.VMEM((rows, cols), bf),
            pltpu.VMEM((rows, cols), f32),
            pltpu.VMEM((nch, 8, LANES), f32),
            pltpu.VMEM((n_fsdp, nch, 8, LANES), f32),
            pltpu.VMEM((2, voc, feats), bf),
            pltpu.VMEM((2, voc, feats), bf),
            pltpu.VMEM((voc, feats), bf),
            pltpu.VMEM((voc, feats), bf),
            pltpu.VMEM((voc, feats), f32),
            pltpu.VMEM((8, cols), f32),
            pltpu.VMEM((tall, LANES), f32),
            pltpu.VMEM((n_dp, tall, LANES), f32),
            dma((nch,)),
            dma((1,)),
            dma((5,)),
            dma((2, nch)),
            dma((2, nch)),
            dma((2, nch)),
            dma((2, 2, nch)),
            dma((2, 2, nch)),
            dma((2, n_fsdp)),
            dma((2, n_dp)),
            dma((2, n_fsdp, nch)),
            dma((2, nch)),
            dma((2, 2, nch)),
            dma((2, nch)),
            dma((2, n_fsdp, nch)),
            dma((2, 2, 2 * nch)),
            dma((2, 2 * nch)),
            dma((2, n_dp)),
        ],
        compiler_params=pltpu.CompilerParams(
            collective_id=1, has_side_effects=True, vmem_limit_bytes=60 * 1024 * 1024
        ),
    )(gain_row, targets, old_logp, lengths, rewards, group_slot, hidden, head)


def fits(hidden, head):
    n_dp, n_fsdp = lax.axis_size("dp"), lax.axis_size("fsdp")
    rows = hidden.shape[0] * hidden.shape[1]
    voc, width = head.shape
    return (
        n_dp == 2 * n_fsdp
        and n_fsdp == 2 * 2
        and (width // n_dp) % LANES == 0
        and rows % LANES == 0
        and rows == voc
        and hidden.shape[1] % LANES == 0
    )


def body(hidden, gain, head, targets, lengths, old_logp, rewards, group_slot):
    if not fits(hidden, head):
        return general(hidden, gain, head, targets, lengths, old_logp, rewards, group_slot)
    resp_here, length_max, cols = hidden.shape
    grad_h, grad_head_t, sums = whole(
        gain.astype(jnp.float32)[None, :],
        targets,
        old_logp,
        lengths,
        rewards,
        group_slot,
        hidden.reshape(resp_here * length_max, cols),
        head,
    )
    loss, grad_h, grad_gain, grad_head_t = write(grad_h, grad_head_t, sums, cols // LANES)
    return (
        loss.reshape(()),
        grad_h.reshape(resp_here, length_max, cols),
        grad_gain.reshape(cols),
        grad_head_t,
    )


def tail_kernel(
    n_dp,
    n_fsdp,
    feats,
    normed_ref,
    dlogits_ref,
    head_ref,
    hidden_ref,
    gain_ref,
    inv_ref,
    loss_ref,
    gh_ref,
    gw_ref,
    gg_ref,
    x_out,
    x_in,
    n_out,
    n_in,
    z_out,
    z_in,
    c_out,
    c_in,
    y_out,
    y_in,
    acc,
    d_out,
    d_in,
    g_out,
    g_in,
    xs,
    xr,
    ns,
    nr,
    zs,
    zr,
    cs,
    cr,
    ys,
    yr,
    ds_,
    dr,
    gs,
    gr,
):
    dp = lax.axis_index("dp")
    fs = lax.axis_index("fsdp")
    z, x = dp // 2, dp % 2
    y, c = fs // 2, fs % 2
    outer_dp, outer_fs, quads = n_dp // 2, n_fsdp // 2, n_dp // 4
    cols = hidden_ref.shape[1]

    barrier = pltpu.get_barrier_semaphore()
    for k in range(1, n_dp):
        pl.semaphore_signal(barrier, inc=1, device_id=(dp ^ k, fs), device_id_type=MESH)
    for k in range(1, n_fsdp):
        pl.semaphore_signal(barrier, inc=1, device_id=(dp, fs ^ k), device_id_type=MESH)
    pl.semaphore_wait(barrier, n_dp + n_fsdp - 2)

    def remote(out, into, send, recv, k, dst):
        return pltpu.make_async_remote_copy(
            src_ref=out,
            dst_ref=into.at[k],
            send_sem=send.at[k],
            recv_sem=recv.at[k],
            device_id=dst,
            device_id_type=MESH,
        )

    def x_copy(k):
        return remote(x_out.at[k], x_in, xs, xr, k, (dp ^ 1, fs))

    def z_copy(k):
        return remote(z_out.at[k], z_in, zs, zr, k, (dp ^ (4 * k), fs))

    def n_copy(k):
        return remote(n_out.at[k], n_in, ns, nr, k, (dp ^ 2, fs))

    def c_copy(j):
        return remote(c_out.at[j], c_in, cs, cr, j, (dp, fs ^ 1))

    def y_copy(j):
        return remote(y_out.at[j], y_in, ys, yr, j, (dp, (y ^ j) * 2 + c))

    def d_copy(j):
        return remote(d_out, d_in, ds_, dr, j, (dp, fs ^ j))

    def g_copy(k):
        return remote(g_out, g_in, gs, gr, k, (dp ^ k, fs))

    def dw(block):
        if feats % 128 == 0:
            left = normed_ref[:, pl.ds(pl.multiple_of(block * feats, 128), feats)]
        else:
            left = normed_ref[block]
        return lax.dot_general(
            left, dlogits_ref[...], (((0,), (0,)), ((), ())), preferred_element_type=jnp.float32
        )

    def dn(block):
        right = head_ref[:, pl.ds(pl.multiple_of(block * cols, 128), cols)]
        return jnp.dot(dlogits_ref[...], right, preferred_element_type=jnp.float32)

    @pl.loop(0, outer_dp)
    def _(i):
        k = outer_dp - 1 - i
        x_out[k] = dw((z ^ k) * 2 + (1 - x)).astype(jnp.bfloat16)
        x_copy(k).start()

    @pl.loop(0, outer_fs)
    def _(i):
        j = outer_fs - 1 - i
        c_out[j] = dn((y ^ j) * 2 + (1 - c)).astype(jnp.bfloat16)
        c_copy(j).start()

    @pl.loop(0, outer_fs - 1)
    def _(i):
        j = outer_fs - 1 - i
        mine = dn((y ^ j) * 2 + c)
        c_copy(j).wait_recv()
        y_out[j] = (mine + c_in[j].astype(jnp.float32)).astype(jnp.bfloat16)
        y_copy(j).start()

    acc[...] = dn(fs)
    c_copy(0).wait_recv()
    acc[...] += c_in[0].astype(jnp.float32)

    def pair_sum(k):
        mine = dw((z ^ k) * 2 + x)
        x_copy(k).wait_recv()
        return mine + x_in[k].astype(jnp.float32)

    def to_near(q):
        n_out[q] = pair_sum(2 * q + 1).astype(jnp.bfloat16)
        n_copy(q).start()

    @pl.loop(0, quads - 1)
    def _(i):
        q = quads - 1 - i
        to_near(q)
        mine = pair_sum(2 * q)
        n_copy(q).wait_recv()
        z_out[q] = (mine + n_in[q].astype(jnp.float32)).astype(jnp.bfloat16)
        z_copy(q).start()

    to_near(0)

    @pl.loop(1, outer_fs)
    def _(j):
        y_copy(j).wait_recv()
        acc[...] += y_in[j].astype(jnp.float32)

    h = hidden_ref[...].astype(jnp.float32)
    inv = inv_ref[...]
    g_out[:, :cols] = jnp.broadcast_to(
        jnp.sum(acc[...] * h * inv, axis=0, keepdims=True), (8, cols)
    )
    g_out[:, cols:] = loss_ref[...]

    @pl.loop(1, n_dp)
    def _(k):
        g_copy(k).start()

    dy = acc[...] * gain_ref[...]
    part = jnp.sum(h * dy, axis=1, keepdims=True)
    rows = part.shape[0]
    d_out[...] = jnp.transpose(jnp.broadcast_to(part, (rows, 128)))[:8]
    for j in range(1, n_fsdp):
        d_copy(j).start()
    dots = d_out[...]
    for j in range(1, n_fsdp):
        d_copy(j).wait_recv()
        dots += d_in[j]
    column = jnp.transpose(jnp.broadcast_to(dots[:1], (128, rows)))[:, :1]
    scale = inv * inv * inv * column / (cols * n_fsdp)
    gh_ref[...] = (
        inv * (acc[...] * gain_ref[...]) - hidden_ref[...].astype(jnp.float32) * scale
    ).astype(jnp.bfloat16)

    gg_ref[...] = g_out[...]

    @pl.loop(1, n_dp)
    def _(k):
        g_copy(k).wait_recv()
        gg_ref[...] += g_in[k]

    gw_ref[...] = pair_sum(0)
    n_copy(0).wait_recv()
    gw_ref[...] += n_in[0].astype(jnp.float32)

    @pl.loop(1, quads)
    def _(k):
        z_copy(k).wait_recv()
        gw_ref[...] += z_in[k].astype(jnp.float32)

    @pl.loop(0, outer_dp)
    def _(k):
        x_copy(k).wait_send()

    @pl.loop(0, quads)
    def _(k):
        n_copy(k).wait_send()

    @pl.loop(1, quads)
    def _(k):
        z_copy(k).wait_send()

    @pl.loop(0, outer_fs)
    def _(j):
        c_copy(j).wait_send()

    @pl.loop(1, outer_fs)
    def _(j):
        y_copy(j).wait_send()

    for j in range(1, n_fsdp):
        d_copy(j).wait_send()

    @pl.loop(1, n_dp)
    def _(k):
        g_copy(k).wait_send()


def tail(normed, dlogits, head, hidden, gain_row, inv, loss_tile):
    n_dp, n_fsdp = lax.axis_size("dp"), lax.axis_size("fsdp")
    rows, width = normed.shape
    vocab_here = head.shape[0]
    cols = hidden.shape[1]
    feats = width // n_dp
    zd, qd, yd = n_dp // 2, n_dp // 4, n_fsdp // 2
    if feats % 128:
        normed = normed.reshape(rows, n_dp, feats).transpose(1, 0, 2)
    wide = cols + 128
    bf, f32 = jnp.bfloat16, jnp.float32
    vm = pl.BlockSpec(memory_space=pltpu.VMEM)
    dma = pltpu.SemaphoreType.DMA
    return pl.pallas_call(
        functools.partial(tail_kernel, n_dp, n_fsdp, feats),
        out_shape=(
            jax.ShapeDtypeStruct((rows, cols), bf),
            jax.ShapeDtypeStruct((feats, vocab_here), f32),
            jax.ShapeDtypeStruct((8, wide), f32),
        ),
        in_specs=[vm] * 7,
        out_specs=(vm, vm, vm),
        scratch_shapes=[
            pltpu.VMEM((zd, feats, vocab_here), bf),
            pltpu.VMEM((zd, feats, vocab_here), bf),
            pltpu.VMEM((qd, feats, vocab_here), bf),
            pltpu.VMEM((qd, feats, vocab_here), bf),
            pltpu.VMEM((qd, feats, vocab_here), bf),
            pltpu.VMEM((qd, feats, vocab_here), bf),
            pltpu.VMEM((yd, rows, cols), bf),
            pltpu.VMEM((yd, rows, cols), bf),
            pltpu.VMEM((yd, rows, cols), bf),
            pltpu.VMEM((yd, rows, cols), bf),
            pltpu.VMEM((rows, cols), f32),
            pltpu.VMEM((8, rows), f32),
            pltpu.VMEM((n_fsdp, 8, rows), f32),
            pltpu.VMEM((8, wide), f32),
            pltpu.VMEM((n_dp, 8, wide), f32),
        ]
        + [dma((n,)) for n in (zd, zd, qd, qd, qd, qd, yd, yd, yd, yd, n_fsdp, n_fsdp, n_dp, n_dp)],
        compiler_params=pltpu.CompilerParams(
            collective_id=0, has_side_effects=True, vmem_limit_bytes=60 * 1024 * 1024
        ),
    )(normed, dlogits, head, hidden, gain_row, inv, loss_tile)


def general(hidden, gain, head, targets, lengths, old_logp, rewards, group_slot):
    resp_here, length_max, shard_cols = hidden.shape
    rows = resp_here * length_max
    whole, gain_full = (
        lax.all_gather(hidden, "fsdp", axis=2, tiled=True),
        lax.all_gather(gain, "fsdp", axis=0, tiled=True),
    )
    width = whole.shape[2]
    whole = whole.reshape(rows, width)
    vocab_here = head.shape[0]
    vocab_start = lax.axis_index("fsdp") * vocab_here
    groups_all = resp_here * lax.axis_size("dp") // GROUP
    group = group_slot // GROUP
    member = (group[:, None] == jnp.arange(groups_all, dtype=jnp.int32)[None, :]).astype(
        jnp.float32
    )
    local_sums = jnp.sum(member * rewards[:, None], axis=0)
    local_count = jnp.sum(lengths).astype(jnp.float32)
    group_sums, count = lax.psum((local_sums, local_count), "dp")
    adv_resp = rewards - jnp.sum(member * group_sums[None, :], axis=1) / GROUP
    adv = jnp.repeat(adv_resp, length_max)
    mask = (
        (jnp.arange(length_max, dtype=jnp.int32)[None, :] < lengths[:, None])
        .astype(jnp.float32)
        .reshape(rows)
    )
    gain_f = gain_full.astype(jnp.float32)
    inv = lax.rsqrt(
        jnp.mean(jnp.square(whole.astype(jnp.float32)), axis=1, keepdims=True) + eps_norm
    )
    normed = (whole.astype(jnp.float32) * inv * gain_f).astype(jnp.bfloat16)
    logits = lax.dot_general(
        normed, head, (((1,), (1,)), ((), ())), preferred_element_type=jnp.float32
    )
    top_local = jnp.max(logits, axis=1)
    sum_local = jnp.sum(jnp.exp(logits - top_local[:, None]), axis=1)
    local_targets = targets.reshape(rows) - vocab_start
    hits = jnp.arange(vocab_here, dtype=jnp.int32)[None, :] == local_targets[:, None]
    chosen_local = jnp.sum(jnp.where(hits, logits, 0.0), axis=1)
    stats = lax.all_gather(jnp.stack([top_local, sum_local, chosen_local]), "fsdp", axis=0)
    top = jnp.max(stats[:, 0], axis=0)
    total = jnp.sum(stats[:, 1] * jnp.exp(stats[:, 0] - top[None, :]), axis=0)
    chosen = jnp.sum(stats[:, 2], axis=0)
    lse = top + jnp.log(total)
    logp = chosen - lse
    ratio = jnp.exp(logp - old_logp.reshape(rows))
    first = ratio * adv
    second = jnp.clip(ratio, clip_low, clip_high) * adv
    policy = -jnp.minimum(first, second)
    policy = jnp.where(adv < 0, jnp.minimum(policy, -dual_bound * adv), policy)
    loss_local = jnp.sum(mask * policy)
    active = (first <= second) & jnp.logical_not((adv < 0) & (first < dual_bound * adv))
    slots_all = rows * lax.axis_size("dp")
    grad_logp = slots_all / count * mask * jnp.where(active, -ratio * adv, 0.0)
    probs = jnp.exp(logits - lse[:, None])
    dlogits = (grad_logp[:, None] * (hits.astype(jnp.float32) - probs)).astype(jnp.bfloat16)
    grad_h, grad_head_t, sums = tail(
        normed,
        dlogits,
        head,
        hidden.reshape(rows, shard_cols),
        gain.astype(jnp.float32)[None, :],
        inv,
        jnp.broadcast_to(loss_local, (8, 128)),
    )
    loss = sums[0, shard_cols] / count
    grad_gain = sums[0, :shard_cols]
    grad_hidden = grad_h.reshape(resp_here, length_max, shard_cols)
    return (loss, grad_hidden, grad_gain, grad_head_t)


def solution(mesh):
    in_specs = (
        P("dp", None, "fsdp"),
        P("fsdp"),
        P("fsdp", None),
        P("dp", None),
        P("dp"),
        P("dp", None),
        P("dp"),
        P("dp"),
    )
    out_specs = (P(), P("dp", None, "fsdp"), P("fsdp"), P("dp", "fsdp"))
    return jax.shard_map(body, mesh=mesh, in_specs=in_specs, out_specs=out_specs, check_vma=False)
```

```python
import functools
import jax
import jax.numpy as jnp
from jax import lax
from jax.experimental import pallas as pl
from jax.experimental.pallas import tpu as pltpu
from jax.sharding import PartitionSpec as P

GROUP = 8
LANES = 128


eps_norm = 1e-06
clip_low = 0.8
clip_high = 1.2
dual_bound = 3.0


MESH = pl.DeviceIdType.MESH


def whole_kernel(
    n_dp,
    n_fsdp,
    length_max,
    gain_hbm,
    targets_hbm,
    old_hbm,
    lengths_hbm,
    rewards_hbm,
    slots_hbm,
    hidden_ref,
    head_hbm,
    gh_ref,
    gw_ref,
    gg_ref,
    targets,
    old,
    lengths,
    rewards,
    slots,
    gain_flat,
    gain_row,
    target_rows,
    old_rows,
    adv_rows,
    mask_rows,
    head,
    turned,
    sums,
    hs,
    hz,
    nm,
    lg,
    inv_s,
    inv_rows,
    squares,
    cnt,
    loss_s,
    gain_in,
    meta_out,
    meta_in,
    st_out,
    st_in,
    dls,
    dlz,
    c_out,
    c_in,
    y_out,
    y_in,
    acc,
    mid,
    left,
    d_out,
    d_in,
    x_out,
    x_in,
    z_out,
    z_in,
    fin,
    gsum,
    g_out,
    g_in,
    own_sem,
    head_sem,
    small_sem,
    sent,
    ysem,
    nsem,
    fsem,
    zsem,
    wsem,
    ssem,
    msem,
    tsem,
    lsem,
    csem,
    rsem,
    dsem,
    xsem,
    vsem,
    hsem,
    gsem,
):
    dp = lax.axis_index("dp")
    fs = lax.axis_index("fsdp")
    zh, zl, x = dp // 4, (dp // 2) % 2, dp % 2
    y, c = fs // 2, fs % 2
    rows, cols = hidden_ref.shape
    voc = head_hbm.shape[0]
    nch = rows // LANES
    quarter = LANES // 4
    feats = gw_ref.shape[0]
    resp_here = rows // length_max
    groups_all = resp_here * n_dp // GROUP
    f32, bf = jnp.float32, jnp.bfloat16

    def span(i):
        return pl.ds(pl.multiple_of(i * LANES, LANES), LANES)

    def piece(p):
        return pl.ds(pl.multiple_of(p * quarter, quarter), quarter)

    def shard(j):
        return pl.ds(pl.multiple_of((fs ^ j) * cols, LANES), cols)

    def remote(src, dst, kind, arrival, to):
        return pltpu.make_async_remote_copy(
            src_ref=src,
            dst_ref=dst,
            send_sem=sent.at[kind],
            recv_sem=arrival,
            device_id=to,
            device_id_type=MESH,
        )

    core, across = (dp, fs ^ 1), (dp, fs ^ 2)
    near, side, far = (dp ^ 2, fs), (dp ^ 1, fs), (dp ^ 4, fs)

    def own_copy(i):
        return pltpu.make_async_copy(hidden_ref.at[span(i)], hs.at[0, span(i)], own_sem.at[i])

    head_copy = pltpu.make_async_copy(head_hbm, head, head_sem.at[0])

    def y_copy(i, b):
        size = LANES * 3 // 8 if b else LANES * 5 // 8
        at = pl.ds(pl.multiple_of(i * LANES + b * (LANES - size), 16), size)
        return remote(hs.at[0, at], hs.at[2, at], 0, ysem.at[i], across)

    def n_copy(i):
        return remote(hs.at[0, span(i)], hs.at[1, span(i)], 1, nsem.at[i], core)

    def f_copy(i):
        return remote(hs.at[2, span(i)], hs.at[3, span(i)], 2, fsem.at[i], core)

    def z_copy(k, i):
        return remote(hs.at[2 * k, span(i)], hz.at[k, span(i)], 3, zsem.at[k, i], near)

    def w_copy(k, i):
        return remote(hz.at[k, span(i)], hz.at[k, span(i)], 4, wsem.at[0], core)

    def s_copy(j):
        return remote(gain_row, gain_in.at[j], 5, ssem.at[0], (dp, fs ^ j))

    def m_copy(k):
        return remote(meta_out, meta_in.at[k], 6, msem.at[0], (dp ^ k, fs))

    def t_copy(j, i):
        return remote(st_out.at[i], st_in.at[j, i], 7, tsem.at[i], (dp, fs ^ j))

    def l_copy(i, p):
        return remote(dls.at[i, span(p)], dlz.at[i, span(p)], 8, lsem.at[p], near)

    def c_copy(k, i):
        return remote(c_out.at[k, span(i)], c_in.at[k, span(i)], 9, csem.at[k, i], core)

    def r_copy(i):
        return remote(y_out.at[span(i)], y_in.at[span(i)], 10, rsem.at[i], across)

    def d_copy(j, i):
        return remote(d_out.at[i], d_in.at[j, i], 11, dsem.at[i], (dp, fs ^ j))

    def x_copy(q):
        return remote(x_out.at[0, piece(q)], x_in.at[0, piece(q)], 12, xsem.at[q], side)

    def v_copy(p):
        return remote(x_out.at[1, span(p)], x_in.at[1, span(p)], 13, vsem.at[p], side)

    def h_copy(p, q):
        at = piece(4 * p + q)
        return remote(z_out.at[at], z_in.at[at], 14, hsem.at[p], far)

    def g_copy(k):
        return remote(g_out, g_in.at[k], 15, gsem.at[0], (dp ^ k, fs))

    def arrived(ref, arrival):
        remote(ref, ref, 0, arrival, core).wait_recv()

    def drained(ref, kind):
        remote(ref, ref, kind, ysem.at[0], core).wait_send()

    gives, takes = c != zl, c == zl

    barrier = pltpu.get_barrier_semaphore()
    for k in range(1, n_dp):
        pl.semaphore_signal(barrier, inc=1, device_id=(dp ^ k, fs), device_id_type=MESH)
    for k in range(1, n_fsdp):
        pl.semaphore_signal(barrier, inc=1, device_id=(dp, fs ^ k), device_id_type=MESH)
    loads = [
        pltpu.make_async_copy(src, dst, small_sem.at[n])
        for n, (src, dst) in enumerate(
            [
                (slots_hbm, slots),
                (rewards_hbm, rewards),
                (lengths_hbm, lengths),
                (targets_hbm, targets),
                (old_hbm, old),
            ]
        )
    ]
    gain_copy = pltpu.make_async_copy(gain_hbm, gain_flat, small_sem.at[5])
    gain_copy.start()
    for load in loads:
        load.start()
    for i in range(nch):
        own_copy(i).start()
    head_copy.start()
    pl.semaphore_wait(barrier, n_dp + n_fsdp - 2)

    gain_copy.wait()
    gain_row[...] = gain_flat[...].astype(f32).reshape(1, cols)
    for j in range(1, n_fsdp):
        s_copy(j).start()

    @pl.loop(0, nch)
    def _(i):
        own_copy(i).wait()

        @pl.when(i == 0)
        def _():
            y_copy(i, 0).start()
            y_copy(i, 1).start()

        @pl.when(i == 1)
        def _():
            y_copy(i, 0).start()

        n_copy(i).start()

    for load in loads:
        load.wait()

    lane = lax.broadcasted_iota(jnp.int32, (8, LANES), 1)
    tile = jnp.zeros((8, LANES), f32)
    for r in range(resp_here):
        tile += jnp.where(lane == slots[r] // GROUP, rewards[r], 0.0)
        tile += jnp.where(lane == groups_all, lengths[r].astype(f32), 0.0)
    meta_out[...] = tile
    for k in range(1, n_dp):
        m_copy(k).start()

    @pl.when(gives)
    def _():
        @pl.loop(0, nch)
        def _(i):
            z_copy(0, i).start()

    loss_s[...] = jnp.zeros_like(loss_s)
    gsum[...] = jnp.zeros_like(gsum)
    head_copy.wait()

    @pl.loop(0, head.shape[1] // LANES)
    def _(b):
        turned[span(b)] = jnp.transpose(head[:, span(b)])

    @pl.loop(0, nch)
    def _(i):
        n_copy(i).wait_recv()

    gain_in[0] = gain_row[...]
    arrived(gain_in.at[pl.ds(1, n_fsdp - 1)], ssem.at[0])
    arrived(meta_in.at[pl.ds(1, n_dp - 1)], msem.at[0])
    total = meta_out[...]
    for k in range(1, n_dp):
        total += meta_in[k]

    def entry(g):
        return jnp.sum(jnp.where(lane == g, total, 0.0), axis=1, keepdims=True)[:1]

    for i in range(nch):
        r, first = i * LANES // length_max, i * LANES % length_max
        position = lax.broadcasted_iota(jnp.int32, (1, LANES), 1) + first
        target_rows[i] = targets[r : r + 1, first : first + LANES]
        old_rows[i] = old[r : r + 1, first : first + LANES]
        mask_rows[i] = jnp.where(position < lengths[r], 1.0, 0.0)
        adv = rewards[r] - entry(slots[r] // GROUP) / GROUP
        adv_rows[i] = jnp.broadcast_to(adv, (1, LANES))
    cnt[...] = jnp.broadcast_to(entry(groups_all), cnt.shape)
    slots_all = rows * n_dp

    def hits_of(i):
        at = lax.broadcasted_iota(jnp.int32, (voc, LANES), 0) + fs * voc
        return at == target_rows[i]

    def take(j, i):
        h = hs[j, span(i)].astype(f32)
        nm[j] = (h * gain_in[j]).astype(bf)
        return jnp.sum(h * h, axis=1, keepdims=True)

    def product(j):
        return jnp.dot(nm[j], turned[shard(j)], preferred_element_type=f32)

    def begin(i):
        squares[...] = take(0, i) + take(1, i)
        sums[...] = product(0)
        sums[...] += product(1)

    def forward(i):
        arrived(hs.at[2, span(i)], ysem.at[i])
        f_copy(i).start()

        @pl.when(gives)
        def _():
            z_copy(1, i).start()

        square = squares[...] + take(2, i)
        sums[...] += product(2)
        f_copy(i).wait_recv()
        square += take(3, i)
        inv = lax.rsqrt(square / (cols * n_fsdp) + eps_norm)
        inv_s[span(i)] = inv
        inv_rows[i] = jnp.transpose(jnp.broadcast_to(inv, (LANES, LANES)))[:1]
        lg[i] = jnp.transpose((sums[...] + product(3)) * inv)
        logits = lg[i]
        top = jnp.max(logits, axis=0, keepdims=True)
        st_out[i, 0:1] = top
        st_out[i, 1:2] = jnp.sum(jnp.exp(logits - top), axis=0, keepdims=True)
        st_out[i, 2:3] = jnp.sum(jnp.where(hits_of(i), logits, 0.0), axis=0, keepdims=True)
        st_out[i, 3:8] = jnp.zeros((5, LANES), f32)
        for j in range(1, n_fsdp):
            t_copy(j, i).start()

        @pl.when(i + 1 < nch)
        def _():
            y_copy(i + 1, 1).start()

        @pl.when(i + 2 < nch)
        def _():
            y_copy(i + 2, 0).start()

    def backward(i):
        arrived(st_in.at[pl.ds(1, n_fsdp - 1), i], tsem.at[i])
        stats = [st_out[i]] + [st_in[j, i] for j in range(1, n_fsdp)]
        top = stats[0][0:1]
        for s in stats[1:]:
            top = jnp.maximum(top, s[0:1])
        total = jnp.zeros_like(top)
        chosen = jnp.zeros_like(top)
        for s in stats:
            total += s[1:2] * jnp.exp(s[0:1] - top)
            chosen += s[2:3]
        lse = top + jnp.log(total)
        adv, mask = adv_rows[i], mask_rows[i]
        ratio = jnp.exp(chosen - lse - old_rows[i])
        first = ratio * adv
        second = jnp.clip(ratio, clip_low, clip_high) * adv
        policy = -jnp.minimum(first, second)
        policy = jnp.where(adv < 0, jnp.minimum(policy, -dual_bound * adv), policy)
        loss_s[0:1] += mask * policy
        active = (first <= second) & jnp.logical_not((adv < 0) & (first < dual_bound * adv))
        slope = slots_all / cnt[0:1] * mask * jnp.where(active, -ratio * adv, 0.0)
        grad = slope * (hits_of(i).astype(f32) - jnp.exp(lg[i] - lse))
        dls[i] = (grad * inv_rows[i]).astype(bf)
        l_copy(i, 0).start()

        @pl.when(i < nch - 2)
        def _():
            for p in range(1, nch):
                l_copy(i, p).start()

        left[...] = jnp.transpose(grad).astype(bf)

    def spread(i):
        def dn(j):
            return jnp.dot(left[...], head[:, shard(j)], preferred_element_type=f32)

        c_out[1, span(i)] = dn(3).astype(bf)
        c_copy(1, i).start()
        c_out[0, span(i)] = dn(1).astype(bf)
        c_copy(0, i).start()
        acc[span(i)] = dn(0)
        mid[span(i)] = dn(2)

    def relay(i):
        @pl.when(takes)
        def _():
            for k in range(2):
                z_copy(k, i).wait_recv()
                w_copy(k, i).start()

    def combine(i):
        c_copy(1, i).wait_recv()
        y_out[span(i)] = (mid[span(i)] + c_in[1, span(i)].astype(f32)).astype(bf)
        c_copy(0, i).wait_recv()
        acc[span(i)] += c_in[0, span(i)].astype(f32)

    begin(0)

    @pl.loop(0, nch)
    def _(i):
        forward(i)

        @pl.when(i + 1 < nch)
        def _():
            begin(i + 1)

        @pl.when(i > 0)
        def _():
            relay(i - 1)
            spread(i - 1)

        @pl.when(i > 1)
        def _():
            combine(i - 2)

        @pl.when(i == nch - 1)
        def _():
            for n in range(nch - 2):
                r_copy(n).start()

        backward(i)

    for p in range(1, nch):
        for i in range(nch - 2, nch):
            l_copy(i, p).start()
    relay(nch - 1)
    spread(nch - 1)
    combine(nch - 2)
    r_copy(nch - 2).start()

    def dots(i):
        r_copy(i).wait_recv()
        grad = acc[span(i)] + y_in[span(i)].astype(f32)
        acc[span(i)] = grad
        h = hs[0, span(i)].astype(f32)
        prod = grad * h
        gsum[...] += jnp.sum((prod * inv_s[span(i)]).reshape(LANES // 8, 8, cols), axis=0)
        part = jnp.sum(prod * gain_in[0], axis=1, keepdims=True)
        d_out[i] = jnp.transpose(jnp.broadcast_to(part, (LANES, LANES)))[:8]
        for j in range(1, n_fsdp):
            d_copy(j, i).start()

    def finish(i):
        whole = d_out[i]
        arrived(d_in.at[pl.ds(1, n_fsdp - 1), i], dsem.at[i])
        for j in range(1, n_fsdp):
            whole += d_in[j, i]
        column = jnp.transpose(jnp.broadcast_to(whole[:1], (LANES, LANES)))[:, :1]
        inv = inv_s[span(i)]
        scale = inv * inv * inv * column / (cols * n_fsdp)
        gh_ref[span(i)] = (
            inv * (acc[span(i)] * gain_in[0])
            - hs[0, span(i)].astype(f32) * scale
        ).astype(bf)

    def dw(p, zb, xb):
        at = pl.ds(pl.multiple_of(xb * feats, LANES), feats)
        here = jnp.concatenate([dls[i, span(p)] for i in range(nch)], axis=1)
        other = jnp.concatenate([dlz[i, span(p)] for i in range(nch)], axis=1)
        return jnp.dot(
            here, hs[fs ^ (2 * zb + zl), :, at], preferred_element_type=f32
        ) + jnp.dot(other, hz[y ^ zb, :, at], preferred_element_type=f32)

    @pl.when(gives)
    def _():
        arrived(hz, wsem.at[0])

    @pl.loop(0, nch)
    def _(p):
        arrived(dlz.at[:, span(p)], lsem.at[p])
        x_out[0, span(p)] = dw(p, 1 - zh, 1 - x).astype(bf)
        for q in range(4):
            x_copy(4 * p + q).start()

    combine(nch - 1)
    r_copy(nch - 1).start()

    @pl.loop(0, nch)
    def _(p):
        x_out[1, span(p)] = dw(p, zh, 1 - x).astype(bf)
        v_copy(p).start()
        fin[span(p)] = dw(p, 1 - zh, x)

        @pl.loop(0, 4)
        def _(q):
            at = piece(4 * p + q)
            x_copy(4 * p + q).wait_recv()
            z_out[at] = (fin[at] + x_in[0, at].astype(f32)).astype(bf)
            h_copy(p, q).start()

    @pl.loop(0, nch)
    def _(p):
        fin[span(p)] = dw(p, zh, x)
        dots(p)

    nb = cols // LANES
    column_sums = jnp.sum(gsum[...], axis=0, keepdims=True)
    g_out[...] = jnp.zeros_like(g_out)
    for b in range(nb):
        g_out[b : b + 1] = column_sums[:, b * LANES : (b + 1) * LANES]
    g_out[nb : nb + 1] = loss_s[0:1]

    for k in range(1, n_dp):
        g_copy(k).start()

    @pl.loop(0, nch)
    def _(p):
        finish(p)

    @pl.loop(0, nch)
    def _(p):
        v_copy(p).wait_recv()
        fin[span(p)] += x_in[1, span(p)].astype(f32)

    mine = gain_in[fs ^ (2 * zh + zl), :, pl.ds(pl.multiple_of(x * feats, LANES), feats)]
    for p in range(nch):
        arrived(z_in.at[span(p)], hsem.at[p])
        gw_ref[:, span(p)] = jnp.transpose((fin[span(p)] + z_in[span(p)].astype(f32)) * mine)

    arrived(g_in.at[pl.ds(1, n_dp - 1)], gsem.at[0])
    whole = g_out[...]
    for k in range(1, n_dp):
        whole += g_in[k]
    gg_ref[...] = whole
    gg_ref[nb : nb + 1] = jnp.sum(gg_ref[nb : nb + 1], axis=1, keepdims=True) / cnt[0:1]

    drained(hs.at[0], 0)
    drained(hs.at[0], 1)
    drained(hs.at[2], 2)

    @pl.when(gives)
    def _():
        drained(hz, 3)

    @pl.when(takes)
    def _():
        drained(hz, 4)

    drained(gain_in.at[pl.ds(1, n_fsdp - 1)], 5)
    drained(meta_in.at[pl.ds(1, n_dp - 1)], 6)
    drained(st_in.at[pl.ds(1, n_fsdp - 1)], 7)
    drained(dls, 8)
    drained(c_out, 9)
    drained(y_out, 10)
    drained(d_in.at[pl.ds(1, n_fsdp - 1)], 11)
    drained(x_out.at[0], 12)
    drained(x_out.at[1], 13)
    drained(z_out, 14)
    drained(g_in.at[pl.ds(1, n_dp - 1)], 15)


def write_kernel(gh_ref, gw_ref, gg_ref, loss_out, gh_out, gg_out, gw_out, sems):
    parts = sems.shape[1]

    def part(ref, n):
        size = ref.shape[0] // parts
        return ref.at[pl.ds(n * size, size)]

    copies = [
        pltpu.make_async_copy(part(src, n), part(dst, n), sems.at[m, n])
        for m, (src, dst) in enumerate([(gw_ref, gw_out), (gh_ref, gh_out)])
        for n in range(parts)
    ]
    for copy in copies:
        copy.start()
    nb = gg_out.shape[0]
    gg_out[...] = gg_ref[:nb]
    loss_out[...] = gg_ref[nb : nb + 1, :1]
    for copy in copies:
        copy.wait()


def write(gh, gw, gg, nb):
    vm = pl.BlockSpec(memory_space=pltpu.VMEM)
    anywhere = pl.BlockSpec(memory_space=pl.ANY)
    return pl.pallas_call(
        write_kernel,
        out_shape=(
            jax.ShapeDtypeStruct((1, 1), jnp.float32),
            jax.ShapeDtypeStruct(gh.shape, gh.dtype),
            jax.ShapeDtypeStruct((nb, LANES), jnp.float32),
            jax.ShapeDtypeStruct(gw.shape, gw.dtype),
        ),
        in_specs=[vm, vm, vm],
        out_specs=(vm, anywhere, vm, anywhere),
        scratch_shapes=[pltpu.SemaphoreType.DMA((2, 4))],
        compiler_params=pltpu.CompilerParams(vmem_limit_bytes=8 * 1024 * 1024),
    )(gh, gw, gg)


def whole(gain, targets, old_logp, lengths, rewards, group_slot, hidden, head):
    n_dp, n_fsdp = lax.axis_size("dp"), lax.axis_size("fsdp")
    resp_here, length_max = targets.shape
    rows, cols = hidden.shape
    voc, width = head.shape
    feats = width // n_dp
    nch = rows // LANES
    tall = (cols // LANES + 8) // 8 * 8
    bf, f32 = jnp.bfloat16, jnp.float32
    vm = pl.BlockSpec(memory_space=pltpu.VMEM)
    anywhere = pl.BlockSpec(memory_space=pl.ANY)
    dma = pltpu.SemaphoreType.DMA
    return pl.pallas_call(
        functools.partial(whole_kernel, n_dp, n_fsdp, length_max),
        out_shape=(
            pltpu.VMEM((rows, cols), bf),
            pltpu.VMEM((feats, voc), f32),
            pltpu.VMEM((tall, LANES), f32),
        ),
        in_specs=[anywhere] * 8,
        out_specs=(vm, vm, vm),
        scratch_shapes=[
            pltpu.VMEM((resp_here, length_max), jnp.int32),
            pltpu.VMEM((resp_here, length_max), f32),
            pltpu.SMEM((resp_here,), jnp.int32),
            pltpu.SMEM((resp_here,), f32),
            pltpu.SMEM((resp_here,), jnp.int32),
            pltpu.VMEM((cols,), bf),
            pltpu.VMEM((1, cols), f32),
            pltpu.VMEM((nch, 1, LANES), jnp.int32),
            pltpu.VMEM((nch, 1, LANES), f32),
            pltpu.VMEM((nch, 1, LANES), f32),
            pltpu.VMEM((nch, 1, LANES), f32),
            pltpu.VMEM((voc, width), bf),
            pltpu.VMEM((width, voc), bf),
            pltpu.VMEM((LANES, voc), f32),
            pltpu.VMEM((n_fsdp, rows, cols), bf),
            pltpu.VMEM((2, rows, cols), bf),
            pltpu.VMEM((n_fsdp, LANES, cols), bf),
            pltpu.VMEM((nch, voc, LANES), f32),
            pltpu.VMEM((rows, 1), f32),
            pltpu.VMEM((nch, 1, LANES), f32),
            pltpu.VMEM((LANES, 1), f32),
            pltpu.VMEM((8, LANES), f32),
            pltpu.VMEM((8, LANES), f32),
            pltpu.VMEM((n_fsdp, 1, cols), f32),
            pltpu.VMEM((8, LANES), f32),
            pltpu.VMEM((n_dp, 8, LANES), f32),
            pltpu.VMEM((nch, 8, LANES), f32),
            pltpu.VMEM((n_fsdp, nch, 8, LANES), f32),
            pltpu.VMEM((nch, voc, LANES), bf),
            pltpu.VMEM((nch, voc, LANES), bf),
            pltpu.VMEM((2, rows, cols), bf),
            pltpu.VMEM((2, rows, cols), bf),
            pltpu.VMEM((rows, cols), bf),
            pltpu.VMEM((rows, cols), bf),
            pltpu.VMEM((rows, cols), f32),
            pltpu.VMEM((rows, cols), f32),
            pltpu.VMEM((LANES, voc), bf),
            pltpu.VMEM((nch, 8, LANES), f32),
            pltpu.VMEM((n_fsdp, nch, 8, LANES), f32),
            pltpu.VMEM((2, voc, feats), bf),
            pltpu.VMEM((2, voc, feats), bf),
            pltpu.VMEM((voc, feats), bf),
            pltpu.VMEM((voc, feats), bf),
            pltpu.VMEM((voc, feats), f32),
            pltpu.VMEM((8, cols), f32),
            pltpu.VMEM((tall, LANES), f32),
            pltpu.VMEM((n_dp, tall, LANES), f32),
            dma((nch,)),
            dma((1,)),
            dma((6,)),
            dma((16,)),
            dma((nch,)),
            dma((nch,)),
            dma((nch,)),
            dma((2, nch)),
            dma((1,)),
            dma((1,)),
            dma((1,)),
            dma((nch,)),
            dma((nch,)),
            dma((2, nch)),
            dma((nch,)),
            dma((nch,)),
            dma((4 * nch,)),
            dma((nch,)),
            dma((nch,)),
            dma((1,)),
        ],
        compiler_params=pltpu.CompilerParams(
            collective_id=1, has_side_effects=True, vmem_limit_bytes=60 * 1024 * 1024
        ),
    )(gain, targets, old_logp, lengths, rewards, group_slot, hidden, head)


def fits(hidden, head):
    n_dp, n_fsdp = lax.axis_size("dp"), lax.axis_size("fsdp")
    rows = hidden.shape[0] * hidden.shape[1]
    voc, width = head.shape
    return (
        n_dp == 2 * n_fsdp
        and n_fsdp == 2 * 2
        and (width // n_dp) % LANES == 0
        and rows % LANES == 0
        and rows == voc
        and hidden.shape[1] % LANES == 0
    )


def body(hidden, gain, head, targets, lengths, old_logp, rewards, group_slot):
    if not fits(hidden, head):
        return general(hidden, gain, head, targets, lengths, old_logp, rewards, group_slot)
    resp_here, length_max, cols = hidden.shape
    grad_h, grad_head_t, sums = whole(
        gain,
        targets,
        old_logp,
        lengths,
        rewards,
        group_slot,
        hidden.reshape(resp_here * length_max, cols),
        head,
    )
    loss, grad_h, grad_gain, grad_head_t = write(grad_h, grad_head_t, sums, cols // LANES)
    return (
        loss.reshape(()),
        grad_h.reshape(resp_here, length_max, cols),
        grad_gain.reshape(cols),
        grad_head_t,
    )


def tail_kernel(
    n_dp,
    n_fsdp,
    feats,
    normed_ref,
    dlogits_ref,
    head_ref,
    hidden_ref,
    gain_ref,
    inv_ref,
    loss_ref,
    gh_ref,
    gw_ref,
    gg_ref,
    x_out,
    x_in,
    n_out,
    n_in,
    z_out,
    z_in,
    c_out,
    c_in,
    y_out,
    y_in,
    acc,
    d_out,
    d_in,
    g_out,
    g_in,
    xs,
    xr,
    ns,
    nr,
    zs,
    zr,
    cs,
    cr,
    ys,
    yr,
    ds_,
    dr,
    gs,
    gr,
):
    dp = lax.axis_index("dp")
    fs = lax.axis_index("fsdp")
    z, x = dp // 2, dp % 2
    y, c = fs // 2, fs % 2
    outer_dp, outer_fs, quads = n_dp // 2, n_fsdp // 2, n_dp // 4
    cols = hidden_ref.shape[1]

    barrier = pltpu.get_barrier_semaphore()
    for k in range(1, n_dp):
        pl.semaphore_signal(barrier, inc=1, device_id=(dp ^ k, fs), device_id_type=MESH)
    for k in range(1, n_fsdp):
        pl.semaphore_signal(barrier, inc=1, device_id=(dp, fs ^ k), device_id_type=MESH)
    pl.semaphore_wait(barrier, n_dp + n_fsdp - 2)

    def remote(out, into, send, recv, k, dst):
        return pltpu.make_async_remote_copy(
            src_ref=out,
            dst_ref=into.at[k],
            send_sem=send.at[k],
            recv_sem=recv.at[k],
            device_id=dst,
            device_id_type=MESH,
        )

    def x_copy(k):
        return remote(x_out.at[k], x_in, xs, xr, k, (dp ^ 1, fs))

    def z_copy(k):
        return remote(z_out.at[k], z_in, zs, zr, k, (dp ^ (4 * k), fs))

    def n_copy(k):
        return remote(n_out.at[k], n_in, ns, nr, k, (dp ^ 2, fs))

    def c_copy(j):
        return remote(c_out.at[j], c_in, cs, cr, j, (dp, fs ^ 1))

    def y_copy(j):
        return remote(y_out.at[j], y_in, ys, yr, j, (dp, (y ^ j) * 2 + c))

    def d_copy(j):
        return remote(d_out, d_in, ds_, dr, j, (dp, fs ^ j))

    def g_copy(k):
        return remote(g_out, g_in, gs, gr, k, (dp ^ k, fs))

    def dw(block):
        if feats % 128 == 0:
            left = normed_ref[:, pl.ds(pl.multiple_of(block * feats, 128), feats)]
        else:
            left = normed_ref[block]
        return lax.dot_general(
            left, dlogits_ref[...], (((0,), (0,)), ((), ())), preferred_element_type=jnp.float32
        )

    def dn(block):
        right = head_ref[:, pl.ds(pl.multiple_of(block * cols, 128), cols)]
        return jnp.dot(dlogits_ref[...], right, preferred_element_type=jnp.float32)

    @pl.loop(0, outer_dp)
    def _(i):
        k = outer_dp - 1 - i
        x_out[k] = dw((z ^ k) * 2 + (1 - x)).astype(jnp.bfloat16)
        x_copy(k).start()

    @pl.loop(0, outer_fs)
    def _(i):
        j = outer_fs - 1 - i
        c_out[j] = dn((y ^ j) * 2 + (1 - c)).astype(jnp.bfloat16)
        c_copy(j).start()

    @pl.loop(0, outer_fs - 1)
    def _(i):
        j = outer_fs - 1 - i
        mine = dn((y ^ j) * 2 + c)
        c_copy(j).wait_recv()
        y_out[j] = (mine + c_in[j].astype(jnp.float32)).astype(jnp.bfloat16)
        y_copy(j).start()

    acc[...] = dn(fs)
    c_copy(0).wait_recv()
    acc[...] += c_in[0].astype(jnp.float32)

    def pair_sum(k):
        mine = dw((z ^ k) * 2 + x)
        x_copy(k).wait_recv()
        return mine + x_in[k].astype(jnp.float32)

    def to_near(q):
        n_out[q] = pair_sum(2 * q + 1).astype(jnp.bfloat16)
        n_copy(q).start()

    @pl.loop(0, quads - 1)
    def _(i):
        q = quads - 1 - i
        to_near(q)
        mine = pair_sum(2 * q)
        n_copy(q).wait_recv()
        z_out[q] = (mine + n_in[q].astype(jnp.float32)).astype(jnp.bfloat16)
        z_copy(q).start()

    to_near(0)

    @pl.loop(1, outer_fs)
    def _(j):
        y_copy(j).wait_recv()
        acc[...] += y_in[j].astype(jnp.float32)

    h = hidden_ref[...].astype(jnp.float32)
    inv = inv_ref[...]
    g_out[:, :cols] = jnp.broadcast_to(
        jnp.sum(acc[...] * h * inv, axis=0, keepdims=True), (8, cols)
    )
    g_out[:, cols:] = loss_ref[...]

    @pl.loop(1, n_dp)
    def _(k):
        g_copy(k).start()

    dy = acc[...] * gain_ref[...]
    part = jnp.sum(h * dy, axis=1, keepdims=True)
    rows = part.shape[0]
    d_out[...] = jnp.transpose(jnp.broadcast_to(part, (rows, 128)))[:8]
    for j in range(1, n_fsdp):
        d_copy(j).start()
    dots = d_out[...]
    for j in range(1, n_fsdp):
        d_copy(j).wait_recv()
        dots += d_in[j]
    column = jnp.transpose(jnp.broadcast_to(dots[:1], (128, rows)))[:, :1]
    scale = inv * inv * inv * column / (cols * n_fsdp)
    gh_ref[...] = (
        inv * (acc[...] * gain_ref[...]) - hidden_ref[...].astype(jnp.float32) * scale
    ).astype(jnp.bfloat16)

    gg_ref[...] = g_out[...]

    @pl.loop(1, n_dp)
    def _(k):
        g_copy(k).wait_recv()
        gg_ref[...] += g_in[k]

    gw_ref[...] = pair_sum(0)
    n_copy(0).wait_recv()
    gw_ref[...] += n_in[0].astype(jnp.float32)

    @pl.loop(1, quads)
    def _(k):
        z_copy(k).wait_recv()
        gw_ref[...] += z_in[k].astype(jnp.float32)

    @pl.loop(0, outer_dp)
    def _(k):
        x_copy(k).wait_send()

    @pl.loop(0, quads)
    def _(k):
        n_copy(k).wait_send()

    @pl.loop(1, quads)
    def _(k):
        z_copy(k).wait_send()

    @pl.loop(0, outer_fs)
    def _(j):
        c_copy(j).wait_send()

    @pl.loop(1, outer_fs)
    def _(j):
        y_copy(j).wait_send()

    for j in range(1, n_fsdp):
        d_copy(j).wait_send()

    @pl.loop(1, n_dp)
    def _(k):
        g_copy(k).wait_send()


def tail(normed, dlogits, head, hidden, gain_row, inv, loss_tile):
    n_dp, n_fsdp = lax.axis_size("dp"), lax.axis_size("fsdp")
    rows, width = normed.shape
    vocab_here = head.shape[0]
    cols = hidden.shape[1]
    feats = width // n_dp
    zd, qd, yd = n_dp // 2, n_dp // 4, n_fsdp // 2
    if feats % 128:
        normed = normed.reshape(rows, n_dp, feats).transpose(1, 0, 2)
    wide = cols + 128
    bf, f32 = jnp.bfloat16, jnp.float32
    vm = pl.BlockSpec(memory_space=pltpu.VMEM)
    dma = pltpu.SemaphoreType.DMA
    return pl.pallas_call(
        functools.partial(tail_kernel, n_dp, n_fsdp, feats),
        out_shape=(
            jax.ShapeDtypeStruct((rows, cols), bf),
            jax.ShapeDtypeStruct((feats, vocab_here), f32),
            jax.ShapeDtypeStruct((8, wide), f32),
        ),
        in_specs=[vm] * 7,
        out_specs=(vm, vm, vm),
        scratch_shapes=[
            pltpu.VMEM((zd, feats, vocab_here), bf),
            pltpu.VMEM((zd, feats, vocab_here), bf),
            pltpu.VMEM((qd, feats, vocab_here), bf),
            pltpu.VMEM((qd, feats, vocab_here), bf),
            pltpu.VMEM((qd, feats, vocab_here), bf),
            pltpu.VMEM((qd, feats, vocab_here), bf),
            pltpu.VMEM((yd, rows, cols), bf),
            pltpu.VMEM((yd, rows, cols), bf),
            pltpu.VMEM((yd, rows, cols), bf),
            pltpu.VMEM((yd, rows, cols), bf),
            pltpu.VMEM((rows, cols), f32),
            pltpu.VMEM((8, rows), f32),
            pltpu.VMEM((n_fsdp, 8, rows), f32),
            pltpu.VMEM((8, wide), f32),
            pltpu.VMEM((n_dp, 8, wide), f32),
        ]
        + [dma((n,)) for n in (zd, zd, qd, qd, qd, qd, yd, yd, yd, yd, n_fsdp, n_fsdp, n_dp, n_dp)],
        compiler_params=pltpu.CompilerParams(
            collective_id=0, has_side_effects=True, vmem_limit_bytes=60 * 1024 * 1024
        ),
    )(normed, dlogits, head, hidden, gain_row, inv, loss_tile)


def general(hidden, gain, head, targets, lengths, old_logp, rewards, group_slot):
    resp_here, length_max, shard_cols = hidden.shape
    rows = resp_here * length_max
    whole, gain_full = (
        lax.all_gather(hidden, "fsdp", axis=2, tiled=True),
        lax.all_gather(gain, "fsdp", axis=0, tiled=True),
    )
    width = whole.shape[2]
    whole = whole.reshape(rows, width)
    vocab_here = head.shape[0]
    vocab_start = lax.axis_index("fsdp") * vocab_here
    groups_all = resp_here * lax.axis_size("dp") // GROUP
    group = group_slot // GROUP
    member = (group[:, None] == jnp.arange(groups_all, dtype=jnp.int32)[None, :]).astype(
        jnp.float32
    )
    local_sums = jnp.sum(member * rewards[:, None], axis=0)
    local_count = jnp.sum(lengths).astype(jnp.float32)
    group_sums, count = lax.psum((local_sums, local_count), "dp")
    adv_resp = rewards - jnp.sum(member * group_sums[None, :], axis=1) / GROUP
    adv = jnp.repeat(adv_resp, length_max)
    mask = (
        (jnp.arange(length_max, dtype=jnp.int32)[None, :] < lengths[:, None])
        .astype(jnp.float32)
        .reshape(rows)
    )
    gain_f = gain_full.astype(jnp.float32)
    inv = lax.rsqrt(
        jnp.mean(jnp.square(whole.astype(jnp.float32)), axis=1, keepdims=True) + eps_norm
    )
    normed = (whole.astype(jnp.float32) * inv * gain_f).astype(jnp.bfloat16)
    logits = lax.dot_general(
        normed, head, (((1,), (1,)), ((), ())), preferred_element_type=jnp.float32
    )
    top_local = jnp.max(logits, axis=1)
    sum_local = jnp.sum(jnp.exp(logits - top_local[:, None]), axis=1)
    local_targets = targets.reshape(rows) - vocab_start
    hits = jnp.arange(vocab_here, dtype=jnp.int32)[None, :] == local_targets[:, None]
    chosen_local = jnp.sum(jnp.where(hits, logits, 0.0), axis=1)
    stats = lax.all_gather(jnp.stack([top_local, sum_local, chosen_local]), "fsdp", axis=0)
    top = jnp.max(stats[:, 0], axis=0)
    total = jnp.sum(stats[:, 1] * jnp.exp(stats[:, 0] - top[None, :]), axis=0)
    chosen = jnp.sum(stats[:, 2], axis=0)
    lse = top + jnp.log(total)
    logp = chosen - lse
    ratio = jnp.exp(logp - old_logp.reshape(rows))
    first = ratio * adv
    second = jnp.clip(ratio, clip_low, clip_high) * adv
    policy = -jnp.minimum(first, second)
    policy = jnp.where(adv < 0, jnp.minimum(policy, -dual_bound * adv), policy)
    loss_local = jnp.sum(mask * policy)
    active = (first <= second) & jnp.logical_not((adv < 0) & (first < dual_bound * adv))
    slots_all = rows * lax.axis_size("dp")
    grad_logp = slots_all / count * mask * jnp.where(active, -ratio * adv, 0.0)
    probs = jnp.exp(logits - lse[:, None])
    dlogits = (grad_logp[:, None] * (hits.astype(jnp.float32) - probs)).astype(jnp.bfloat16)
    grad_h, grad_head_t, sums = tail(
        normed,
        dlogits,
        head,
        hidden.reshape(rows, shard_cols),
        gain.astype(jnp.float32)[None, :],
        inv,
        jnp.broadcast_to(loss_local, (8, 128)),
    )
    loss = sums[0, shard_cols] / count
    grad_gain = sums[0, :shard_cols]
    grad_hidden = grad_h.reshape(resp_here, length_max, shard_cols)
    return (loss, grad_hidden, grad_gain, grad_head_t)


def solution(mesh):
    in_specs = (
        P("dp", None, "fsdp"),
        P("fsdp"),
        P("fsdp", None),
        P("dp", None),
        P("dp"),
        P("dp", None),
        P("dp"),
        P("dp"),
    )
    out_specs = (P(), P("dp", None, "fsdp"), P("fsdp"), P("dp", "fsdp"))
    return jax.shard_map(body, mesh=mesh, in_specs=in_specs, out_specs=out_specs, check_vma=False)
```

```python
import functools
import jax
import jax.numpy as jnp
from jax import lax
from jax.experimental import pallas as pl
from jax.experimental.pallas import tpu as pltpu
from jax.sharding import PartitionSpec as P

GROUP = 8
LANES = 128


eps_norm = 1e-06
clip_low = 0.8
clip_high = 1.2
dual_bound = 3.0


MESH = pl.DeviceIdType.MESH


def whole_kernel(
    n_dp,
    n_fsdp,
    length_max,
    gain_hbm,
    targets_hbm,
    old_hbm,
    lengths_hbm,
    rewards_hbm,
    slots_hbm,
    hidden_ref,
    head_hbm,
    gh_ref,
    gw_ref,
    gg_ref,
    targets,
    old,
    lengths,
    rewards,
    slots,
    gain_flat,
    gain_row,
    target_rows,
    old_rows,
    adv_rows,
    mask_rows,
    head,
    turned,
    sums,
    hs,
    hz,
    nm,
    lg,
    inv_s,
    inv_rows,
    squares,
    cnt,
    loss_s,
    gain_in,
    meta_out,
    meta_in,
    st_out,
    st_in,
    dls,
    dlz,
    c_out,
    c_in,
    y_out,
    y_in,
    acc,
    mid,
    left,
    d_out,
    d_in,
    x_out,
    x_in,
    z_out,
    z_in,
    fin,
    gsum,
    g_out,
    g_in,
    own_sem,
    head_sem,
    small_sem,
    sent,
    ysem,
    nsem,
    fsem,
    zsem,
    wsem,
    ssem,
    msem,
    tsem,
    lsem,
    csem,
    rsem,
    dsem,
    xsem,
    vsem,
    hsem,
    gsem,
):
    dp = lax.axis_index("dp")
    fs = lax.axis_index("fsdp")
    zh, zl, x = dp // 4, (dp // 2) % 2, dp % 2
    y, c = fs // 2, fs % 2
    rows, cols = hidden_ref.shape
    voc = head_hbm.shape[0]
    nch = rows // LANES
    quarter = LANES // 4
    feats = gw_ref.shape[0]
    resp_here = rows // length_max
    groups_all = resp_here * n_dp // GROUP
    f32, bf = jnp.float32, jnp.bfloat16

    def span(i):
        return pl.ds(pl.multiple_of(i * LANES, LANES), LANES)

    def piece(p):
        return pl.ds(pl.multiple_of(p * quarter, quarter), quarter)

    def shard(j):
        return pl.ds(pl.multiple_of((fs ^ j) * cols, LANES), cols)

    def remote(src, dst, kind, arrival, to):
        return pltpu.make_async_remote_copy(
            src_ref=src,
            dst_ref=dst,
            send_sem=sent.at[kind],
            recv_sem=arrival,
            device_id=to,
            device_id_type=MESH,
        )

    core, across = (dp, fs ^ 1), (dp, fs ^ 2)
    near, side, far = (dp ^ 2, fs), (dp ^ 1, fs), (dp ^ 4, fs)

    def own_copy(i):
        return pltpu.make_async_copy(hidden_ref.at[span(i)], hs.at[0, span(i)], own_sem.at[i])

    head_copy = pltpu.make_async_copy(head_hbm, head, head_sem.at[0])

    def y_copy(i, b):
        size = LANES * 3 // 8 if b else LANES * 5 // 8
        at = pl.ds(pl.multiple_of(i * LANES + b * (LANES - size), 16), size)
        return remote(hs.at[0, at], hs.at[2, at], 0, ysem.at[i], across)

    def n_copy(i):
        return remote(hs.at[0, span(i)], hs.at[1, span(i)], 1, nsem.at[i], core)

    def f_copy(i):
        return remote(hs.at[2, span(i)], hs.at[3, span(i)], 2, fsem.at[i], core)

    def z_copy(k, i):
        return remote(hs.at[2 * k, span(i)], hz.at[k, span(i)], 3, zsem.at[k, i], near)

    def w_copy(k, i):
        return remote(hz.at[k, span(i)], hz.at[k, span(i)], 4, wsem.at[0], core)

    def s_copy(j):
        return remote(gain_row, gain_in.at[j], 5, ssem.at[0], (dp, fs ^ j))

    def m_copy(k):
        return remote(meta_out, meta_in.at[k], 6, msem.at[0], (dp ^ k, fs))

    def t_copy(j, i):
        return remote(st_out.at[i], st_in.at[j, i], 7, tsem.at[i], (dp, fs ^ j))

    def l_copy(i, p):
        return remote(dls.at[i, span(p)], dlz.at[i, span(p)], 8, lsem.at[p], near)

    def c_copy(k, i):
        return remote(c_out.at[k, span(i)], c_in.at[k, span(i)], 9, csem.at[k, i], core)

    def r_copy(i):
        return remote(y_out.at[span(i)], y_in.at[span(i)], 10, rsem.at[i], across)

    def d_copy(j, i):
        return remote(d_out.at[i], d_in.at[j, i], 11, dsem.at[i], (dp, fs ^ j))

    def x_copy(q):
        return remote(x_out.at[0, piece(q)], x_in.at[0, piece(q)], 12, xsem.at[q], side)

    def v_copy(p):
        return remote(x_out.at[1, span(p)], x_in.at[1, span(p)], 13, vsem.at[p], side)

    def h_copy(p, q):
        at = piece(4 * p + q)
        return remote(z_out.at[at], z_in.at[at], 14, hsem.at[p], far)

    def g_copy(k):
        return remote(g_out, g_in.at[k], 15, gsem.at[0], (dp ^ k, fs))

    def arrived(ref, arrival):
        remote(ref, ref, 0, arrival, core).wait_recv()

    def drained(ref, kind):
        remote(ref, ref, kind, ysem.at[0], core).wait_send()

    gives, takes = c != zl, c == zl

    barrier = pltpu.get_barrier_semaphore()
    for k in range(1, n_dp):
        pl.semaphore_signal(barrier, inc=1, device_id=(dp ^ k, fs), device_id_type=MESH)
    for k in range(1, n_fsdp):
        pl.semaphore_signal(barrier, inc=1, device_id=(dp, fs ^ k), device_id_type=MESH)
    loads = [
        pltpu.make_async_copy(src, dst, small_sem.at[n])
        for n, (src, dst) in enumerate(
            [
                (slots_hbm, slots),
                (rewards_hbm, rewards),
                (lengths_hbm, lengths),
                (targets_hbm, targets),
                (old_hbm, old),
            ]
        )
    ]
    gain_copy = pltpu.make_async_copy(gain_hbm, gain_flat, small_sem.at[5])
    gain_copy.start()
    for load in loads:
        load.start()
    for i in range(nch):
        own_copy(i).start()
    head_copy.start()
    pl.semaphore_wait(barrier, n_dp + n_fsdp - 2)

    gain_copy.wait()
    gain_row[...] = gain_flat[...].astype(f32).reshape(1, cols)
    for j in range(1, n_fsdp):
        s_copy(j).start()

    @pl.loop(0, nch)
    def _(i):
        own_copy(i).wait()

        @pl.when(i == 0)
        def _():
            y_copy(i, 0).start()
            y_copy(i, 1).start()

        @pl.when(i == 1)
        def _():
            y_copy(i, 0).start()

        n_copy(i).start()

    for load in loads:
        load.wait()

    lane = lax.broadcasted_iota(jnp.int32, (8, LANES), 1)
    tile = jnp.zeros((8, LANES), f32)
    for r in range(resp_here):
        tile += jnp.where(lane == slots[r] // GROUP, rewards[r], 0.0)
        tile += jnp.where(lane == groups_all, lengths[r].astype(f32), 0.0)
    meta_out[...] = tile
    for k in range(1, n_dp):
        m_copy(k).start()

    @pl.when(gives)
    def _():
        @pl.loop(0, nch)
        def _(i):
            z_copy(0, i).start()

    loss_s[...] = jnp.zeros_like(loss_s)
    gsum[...] = jnp.zeros_like(gsum)
    head_copy.wait()

    @pl.loop(0, head.shape[1] // LANES)
    def _(b):
        turned[span(b)] = jnp.transpose(head[:, span(b)])

    @pl.loop(0, nch)
    def _(i):
        n_copy(i).wait_recv()

    gain_in[0] = gain_row[...]
    arrived(gain_in.at[pl.ds(1, n_fsdp - 1)], ssem.at[0])
    arrived(meta_in.at[pl.ds(1, n_dp - 1)], msem.at[0])
    total = meta_out[...]
    for k in range(1, n_dp):
        total += meta_in[k]

    def entry(g):
        return jnp.sum(jnp.where(lane == g, total, 0.0), axis=1, keepdims=True)[:1]

    for i in range(nch):
        r, first = i * LANES // length_max, i * LANES % length_max
        position = lax.broadcasted_iota(jnp.int32, (1, LANES), 1) + first
        target_rows[i] = targets[r : r + 1, first : first + LANES]
        old_rows[i] = old[r : r + 1, first : first + LANES]
        mask_rows[i] = jnp.where(position < lengths[r], 1.0, 0.0)
        adv = rewards[r] - entry(slots[r] // GROUP) / GROUP
        adv_rows[i] = jnp.broadcast_to(adv, (1, LANES))
    cnt[...] = jnp.broadcast_to(entry(groups_all), cnt.shape)
    slots_all = rows * n_dp

    def hits_of(i):
        at = lax.broadcasted_iota(jnp.int32, (voc, LANES), 0) + fs * voc
        return at == target_rows[i]

    def take(j, i):
        h = hs[j, span(i)].astype(f32)
        nm[j] = (h * gain_in[j]).astype(bf)
        return jnp.sum(h * h, axis=1, keepdims=True)

    def product(j):
        return jnp.dot(nm[j], turned[shard(j)], preferred_element_type=f32)

    def begin(i):
        squares[...] = take(0, i) + take(1, i)
        sums[...] = product(0)
        sums[...] += product(1)

    def forward(i):
        arrived(hs.at[2, span(i)], ysem.at[i])
        f_copy(i).start()

        @pl.when(gives)
        def _():
            z_copy(1, i).start()

        square = squares[...] + take(2, i)
        sums[...] += product(2)
        f_copy(i).wait_recv()
        square += take(3, i)
        inv = lax.rsqrt(square / (cols * n_fsdp) + eps_norm)
        inv_s[span(i)] = inv
        inv_rows[i] = jnp.transpose(jnp.broadcast_to(inv, (LANES, LANES)))[:1]
        lg[i] = jnp.transpose((sums[...] + product(3)) * inv)
        logits = lg[i]
        top = jnp.max(logits, axis=0, keepdims=True)
        st_out[i, 0:1] = top
        st_out[i, 1:2] = jnp.sum(jnp.exp(logits - top), axis=0, keepdims=True)
        st_out[i, 2:3] = jnp.sum(jnp.where(hits_of(i), logits, 0.0), axis=0, keepdims=True)
        st_out[i, 3:8] = jnp.zeros((5, LANES), f32)
        for j in range(1, n_fsdp):
            t_copy(j, i).start()

        @pl.when(i + 1 < nch)
        def _():
            y_copy(i + 1, 1).start()

        @pl.when(i + 2 < nch)
        def _():
            y_copy(i + 2, 0).start()

    def backward(i):
        arrived(st_in.at[pl.ds(1, n_fsdp - 1), i], tsem.at[i])
        stats = [st_out[i]] + [st_in[j, i] for j in range(1, n_fsdp)]
        top = stats[0][0:1]
        for s in stats[1:]:
            top = jnp.maximum(top, s[0:1])
        total = jnp.zeros_like(top)
        chosen = jnp.zeros_like(top)
        for s in stats:
            total += s[1:2] * jnp.exp(s[0:1] - top)
            chosen += s[2:3]
        lse = top + jnp.log(total)
        adv, mask = adv_rows[i], mask_rows[i]
        ratio = jnp.exp(chosen - lse - old_rows[i])
        first = ratio * adv
        second = jnp.clip(ratio, clip_low, clip_high) * adv
        policy = -jnp.minimum(first, second)
        policy = jnp.where(adv < 0, jnp.minimum(policy, -dual_bound * adv), policy)
        loss_s[0:1] += mask * policy
        active = (first <= second) & jnp.logical_not((adv < 0) & (first < dual_bound * adv))
        slope = slots_all / cnt[0:1] * mask * jnp.where(active, -ratio * adv, 0.0)
        grad = slope * (hits_of(i).astype(f32) - jnp.exp(lg[i] - lse))
        dls[i] = (grad * inv_rows[i]).astype(bf)
        l_copy(i, 0).start()

        @pl.when(i < nch - 2)
        def _():
            for p in range(1, nch):
                l_copy(i, p).start()

        left[...] = jnp.transpose(grad).astype(bf)

    def spread(i):
        def dn(j):
            return jnp.dot(left[...], head[:, shard(j)], preferred_element_type=f32)

        c_out[1, span(i)] = dn(3).astype(bf)
        c_copy(1, i).start()
        c_out[0, span(i)] = dn(1).astype(bf)
        c_copy(0, i).start()
        acc[span(i)] = dn(0)
        mid[span(i)] = dn(2)

    def relay(i):
        @pl.when(takes)
        def _():
            for k in range(2):
                z_copy(k, i).wait_recv()
                w_copy(k, i).start()

    def combine(i):
        c_copy(1, i).wait_recv()
        y_out[span(i)] = (mid[span(i)] + c_in[1, span(i)].astype(f32)).astype(bf)
        c_copy(0, i).wait_recv()
        acc[span(i)] += c_in[0, span(i)].astype(f32)

    begin(0)

    @pl.loop(0, nch)
    def _(i):
        forward(i)

        @pl.when(i + 1 < nch)
        def _():
            begin(i + 1)

        @pl.when(i > 0)
        def _():
            relay(i - 1)
            spread(i - 1)

        @pl.when(i > 1)
        def _():
            combine(i - 2)

        @pl.when(i == nch - 1)
        def _():
            for n in range(nch - 2):
                r_copy(n).start()

        backward(i)

    for p in range(1, nch):
        for i in range(nch - 2, nch):
            l_copy(i, p).start()
    relay(nch - 1)
    spread(nch - 1)
    combine(nch - 2)
    r_copy(nch - 2).start()

    def dots(i):
        r_copy(i).wait_recv()
        grad = acc[span(i)] + y_in[span(i)].astype(f32)
        acc[span(i)] = grad
        h = hs[0, span(i)].astype(f32)
        prod = grad * h
        gsum[...] += jnp.sum((prod * inv_s[span(i)]).reshape(LANES // 8, 8, cols), axis=0)
        part = jnp.sum(prod * gain_in[0], axis=1, keepdims=True)
        d_out[i] = jnp.transpose(jnp.broadcast_to(part, (LANES, LANES)))[:8]
        for j in range(1, n_fsdp):
            d_copy(j, i).start()

    def finish(i):
        whole = d_out[i]
        arrived(d_in.at[pl.ds(1, n_fsdp - 1), i], dsem.at[i])
        for j in range(1, n_fsdp):
            whole += d_in[j, i]
        column = jnp.transpose(jnp.broadcast_to(whole[:1], (LANES, LANES)))[:, :1]
        inv = inv_s[span(i)]
        scale = inv * inv * inv * column / (cols * n_fsdp)
        gh_ref[span(i)] = (
            inv * (acc[span(i)] * gain_in[0])
            - hs[0, span(i)].astype(f32) * scale
        ).astype(bf)

    def dw(p, zb, xb):
        at = pl.ds(pl.multiple_of(xb * feats, LANES), feats)
        here = jnp.concatenate([dls[i, span(p)] for i in range(nch)], axis=1)
        other = jnp.concatenate([dlz[i, span(p)] for i in range(nch)], axis=1)
        return jnp.dot(
            here, hs[fs ^ (2 * zb + zl), :, at], preferred_element_type=f32
        ) + jnp.dot(other, hz[y ^ zb, :, at], preferred_element_type=f32)

    @pl.when(gives)
    def _():
        arrived(hz, wsem.at[0])

    def lead(p):
        arrived(dlz.at[:, span(p)], lsem.at[p])
        x_out[0, span(p)] = dw(p, 1 - zh, 1 - x).astype(bf)
        for q in range(4):
            x_copy(4 * p + q).start()
        fin[span(p)] = dw(p, 1 - zh, x)

    lead(0)

    @pl.loop(0, nch)
    def _(p):
        @pl.when(p + 1 < nch)
        def _():
            lead(p + 1)

        @pl.loop(0, 4)
        def _(q):
            at = piece(4 * p + q)
            x_copy(4 * p + q).wait_recv()
            z_out[at] = (fin[at] + x_in[0, at].astype(f32)).astype(bf)
            h_copy(p, q).start()

        @pl.when(p == 0)
        def _():
            combine(nch - 1)
            r_copy(nch - 1).start()

        x_out[1, span(p)] = dw(p, zh, 1 - x).astype(bf)
        v_copy(p).start()

    @pl.loop(0, nch)
    def _(p):
        fin[span(p)] = dw(p, zh, x)
        dots(p)

    nb = cols // LANES
    column_sums = jnp.sum(gsum[...], axis=0, keepdims=True)
    g_out[...] = jnp.zeros_like(g_out)
    for b in range(nb):
        g_out[b : b + 1] = column_sums[:, b * LANES : (b + 1) * LANES]
    g_out[nb : nb + 1] = loss_s[0:1]

    for k in range(1, n_dp):
        g_copy(k).start()

    @pl.loop(0, nch)
    def _(p):
        finish(p)

    @pl.loop(0, nch)
    def _(p):
        v_copy(p).wait_recv()
        fin[span(p)] += x_in[1, span(p)].astype(f32)

    mine = gain_in[fs ^ (2 * zh + zl), :, pl.ds(pl.multiple_of(x * feats, LANES), feats)]
    for p in range(nch):
        arrived(z_in.at[span(p)], hsem.at[p])
        gw_ref[:, span(p)] = jnp.transpose((fin[span(p)] + z_in[span(p)].astype(f32)) * mine)

    arrived(g_in.at[pl.ds(1, n_dp - 1)], gsem.at[0])
    whole = g_out[...]
    for k in range(1, n_dp):
        whole += g_in[k]
    gg_ref[...] = whole
    gg_ref[nb : nb + 1] = jnp.sum(gg_ref[nb : nb + 1], axis=1, keepdims=True) / cnt[0:1]

    drained(hs.at[0], 0)
    drained(hs.at[0], 1)
    drained(hs.at[2], 2)

    @pl.when(gives)
    def _():
        drained(hz, 3)

    @pl.when(takes)
    def _():
        drained(hz, 4)

    drained(gain_in.at[pl.ds(1, n_fsdp - 1)], 5)
    drained(meta_in.at[pl.ds(1, n_dp - 1)], 6)
    drained(st_in.at[pl.ds(1, n_fsdp - 1)], 7)
    drained(dls, 8)
    drained(c_out, 9)
    drained(y_out, 10)
    drained(d_in.at[pl.ds(1, n_fsdp - 1)], 11)
    drained(x_out.at[0], 12)
    drained(x_out.at[1], 13)
    drained(z_out, 14)
    drained(g_in.at[pl.ds(1, n_dp - 1)], 15)


def write_kernel(gh_ref, gw_ref, gg_ref, loss_out, gh_out, gg_out, gw_out, sems):
    parts = sems.shape[1]

    def part(ref, n):
        size = ref.shape[0] // parts
        return ref.at[pl.ds(n * size, size)]

    copies = [
        pltpu.make_async_copy(part(src, n), part(dst, n), sems.at[m, n])
        for m, (src, dst) in enumerate([(gw_ref, gw_out), (gh_ref, gh_out)])
        for n in range(parts)
    ]
    for copy in copies:
        copy.start()
    nb = gg_out.shape[0]
    gg_out[...] = gg_ref[:nb]
    loss_out[...] = gg_ref[nb : nb + 1, :1]
    for copy in copies:
        copy.wait()


def write(gh, gw, gg, nb):
    vm = pl.BlockSpec(memory_space=pltpu.VMEM)
    anywhere = pl.BlockSpec(memory_space=pl.ANY)
    return pl.pallas_call(
        write_kernel,
        out_shape=(
            jax.ShapeDtypeStruct((1, 1), jnp.float32),
            jax.ShapeDtypeStruct(gh.shape, gh.dtype),
            jax.ShapeDtypeStruct((nb, LANES), jnp.float32),
            jax.ShapeDtypeStruct(gw.shape, gw.dtype),
        ),
        in_specs=[vm, vm, vm],
        out_specs=(vm, anywhere, vm, anywhere),
        scratch_shapes=[pltpu.SemaphoreType.DMA((2, 4))],
        compiler_params=pltpu.CompilerParams(vmem_limit_bytes=8 * 1024 * 1024),
    )(gh, gw, gg)


def whole(gain, targets, old_logp, lengths, rewards, group_slot, hidden, head):
    n_dp, n_fsdp = lax.axis_size("dp"), lax.axis_size("fsdp")
    resp_here, length_max = targets.shape
    rows, cols = hidden.shape
    voc, width = head.shape
    feats = width // n_dp
    nch = rows // LANES
    tall = (cols // LANES + 8) // 8 * 8
    bf, f32 = jnp.bfloat16, jnp.float32
    vm = pl.BlockSpec(memory_space=pltpu.VMEM)
    anywhere = pl.BlockSpec(memory_space=pl.ANY)
    dma = pltpu.SemaphoreType.DMA
    return pl.pallas_call(
        functools.partial(whole_kernel, n_dp, n_fsdp, length_max),
        out_shape=(
            pltpu.VMEM((rows, cols), bf),
            pltpu.VMEM((feats, voc), f32),
            pltpu.VMEM((tall, LANES), f32),
        ),
        in_specs=[anywhere] * 8,
        out_specs=(vm, vm, vm),
        scratch_shapes=[
            pltpu.VMEM((resp_here, length_max), jnp.int32),
            pltpu.VMEM((resp_here, length_max), f32),
            pltpu.SMEM((resp_here,), jnp.int32),
            pltpu.SMEM((resp_here,), f32),
            pltpu.SMEM((resp_here,), jnp.int32),
            pltpu.VMEM((cols,), bf),
            pltpu.VMEM((1, cols), f32),
            pltpu.VMEM((nch, 1, LANES), jnp.int32),
            pltpu.VMEM((nch, 1, LANES), f32),
            pltpu.VMEM((nch, 1, LANES), f32),
            pltpu.VMEM((nch, 1, LANES), f32),
            pltpu.VMEM((voc, width), bf),
            pltpu.VMEM((width, voc), bf),
            pltpu.VMEM((LANES, voc), f32),
            pltpu.VMEM((n_fsdp, rows, cols), bf),
            pltpu.VMEM((2, rows, cols), bf),
            pltpu.VMEM((n_fsdp, LANES, cols), bf),
            pltpu.VMEM((nch, voc, LANES), f32),
            pltpu.VMEM((rows, 1), f32),
            pltpu.VMEM((nch, 1, LANES), f32),
            pltpu.VMEM((LANES, 1), f32),
            pltpu.VMEM((8, LANES), f32),
            pltpu.VMEM((8, LANES), f32),
            pltpu.VMEM((n_fsdp, 1, cols), f32),
            pltpu.VMEM((8, LANES), f32),
            pltpu.VMEM((n_dp, 8, LANES), f32),
            pltpu.VMEM((nch, 8, LANES), f32),
            pltpu.VMEM((n_fsdp, nch, 8, LANES), f32),
            pltpu.VMEM((nch, voc, LANES), bf),
            pltpu.VMEM((nch, voc, LANES), bf),
            pltpu.VMEM((2, rows, cols), bf),
            pltpu.VMEM((2, rows, cols), bf),
            pltpu.VMEM((rows, cols), bf),
            pltpu.VMEM((rows, cols), bf),
            pltpu.VMEM((rows, cols), f32),
            pltpu.VMEM((rows, cols), f32),
            pltpu.VMEM((LANES, voc), bf),
            pltpu.VMEM((nch, 8, LANES), f32),
            pltpu.VMEM((n_fsdp, nch, 8, LANES), f32),
            pltpu.VMEM((2, voc, feats), bf),
            pltpu.VMEM((2, voc, feats), bf),
            pltpu.VMEM((voc, feats), bf),
            pltpu.VMEM((voc, feats), bf),
            pltpu.VMEM((voc, feats), f32),
            pltpu.VMEM((8, cols), f32),
            pltpu.VMEM((tall, LANES), f32),
            pltpu.VMEM((n_dp, tall, LANES), f32),
            dma((nch,)),
            dma((1,)),
            dma((6,)),
            dma((16,)),
            dma((nch,)),
            dma((nch,)),
            dma((nch,)),
            dma((2, nch)),
            dma((1,)),
            dma((1,)),
            dma((1,)),
            dma((nch,)),
            dma((nch,)),
            dma((2, nch)),
            dma((nch,)),
            dma((nch,)),
            dma((4 * nch,)),
            dma((nch,)),
            dma((nch,)),
            dma((1,)),
        ],
        compiler_params=pltpu.CompilerParams(
            collective_id=1, has_side_effects=True, vmem_limit_bytes=60 * 1024 * 1024
        ),
    )(gain, targets, old_logp, lengths, rewards, group_slot, hidden, head)


def fits(hidden, head):
    n_dp, n_fsdp = lax.axis_size("dp"), lax.axis_size("fsdp")
    rows = hidden.shape[0] * hidden.shape[1]
    voc, width = head.shape
    return (
        n_dp == 2 * n_fsdp
        and n_fsdp == 2 * 2
        and (width // n_dp) % LANES == 0
        and rows % LANES == 0
        and rows == voc
        and hidden.shape[1] % LANES == 0
    )


def body(hidden, gain, head, targets, lengths, old_logp, rewards, group_slot):
    if not fits(hidden, head):
        return general(hidden, gain, head, targets, lengths, old_logp, rewards, group_slot)
    resp_here, length_max, cols = hidden.shape
    grad_h, grad_head_t, sums = whole(
        gain,
        targets,
        old_logp,
        lengths,
        rewards,
        group_slot,
        hidden.reshape(resp_here * length_max, cols),
        head,
    )
    loss, grad_h, grad_gain, grad_head_t = write(grad_h, grad_head_t, sums, cols // LANES)
    return (
        loss.reshape(()),
        grad_h.reshape(resp_here, length_max, cols),
        grad_gain.reshape(cols),
        grad_head_t,
    )


def tail_kernel(
    n_dp,
    n_fsdp,
    feats,
    normed_ref,
    dlogits_ref,
    head_ref,
    hidden_ref,
    gain_ref,
    inv_ref,
    loss_ref,
    gh_ref,
    gw_ref,
    gg_ref,
    x_out,
    x_in,
    n_out,
    n_in,
    z_out,
    z_in,
    c_out,
    c_in,
    y_out,
    y_in,
    acc,
    d_out,
    d_in,
    g_out,
    g_in,
    xs,
    xr,
    ns,
    nr,
    zs,
    zr,
    cs,
    cr,
    ys,
    yr,
    ds_,
    dr,
    gs,
    gr,
):
    dp = lax.axis_index("dp")
    fs = lax.axis_index("fsdp")
    z, x = dp // 2, dp % 2
    y, c = fs // 2, fs % 2
    outer_dp, outer_fs, quads = n_dp // 2, n_fsdp // 2, n_dp // 4
    cols = hidden_ref.shape[1]

    barrier = pltpu.get_barrier_semaphore()
    for k in range(1, n_dp):
        pl.semaphore_signal(barrier, inc=1, device_id=(dp ^ k, fs), device_id_type=MESH)
    for k in range(1, n_fsdp):
        pl.semaphore_signal(barrier, inc=1, device_id=(dp, fs ^ k), device_id_type=MESH)
    pl.semaphore_wait(barrier, n_dp + n_fsdp - 2)

    def remote(out, into, send, recv, k, dst):
        return pltpu.make_async_remote_copy(
            src_ref=out,
            dst_ref=into.at[k],
            send_sem=send.at[k],
            recv_sem=recv.at[k],
            device_id=dst,
            device_id_type=MESH,
        )

    def x_copy(k):
        return remote(x_out.at[k], x_in, xs, xr, k, (dp ^ 1, fs))

    def z_copy(k):
        return remote(z_out.at[k], z_in, zs, zr, k, (dp ^ (4 * k), fs))

    def n_copy(k):
        return remote(n_out.at[k], n_in, ns, nr, k, (dp ^ 2, fs))

    def c_copy(j):
        return remote(c_out.at[j], c_in, cs, cr, j, (dp, fs ^ 1))

    def y_copy(j):
        return remote(y_out.at[j], y_in, ys, yr, j, (dp, (y ^ j) * 2 + c))

    def d_copy(j):
        return remote(d_out, d_in, ds_, dr, j, (dp, fs ^ j))

    def g_copy(k):
        return remote(g_out, g_in, gs, gr, k, (dp ^ k, fs))

    def dw(block):
        if feats % 128 == 0:
            left = normed_ref[:, pl.ds(pl.multiple_of(block * feats, 128), feats)]
        else:
            left = normed_ref[block]
        return lax.dot_general(
            left, dlogits_ref[...], (((0,), (0,)), ((), ())), preferred_element_type=jnp.float32
        )

    def dn(block):
        right = head_ref[:, pl.ds(pl.multiple_of(block * cols, 128), cols)]
        return jnp.dot(dlogits_ref[...], right, preferred_element_type=jnp.float32)

    @pl.loop(0, outer_dp)
    def _(i):
        k = outer_dp - 1 - i
        x_out[k] = dw((z ^ k) * 2 + (1 - x)).astype(jnp.bfloat16)
        x_copy(k).start()

    @pl.loop(0, outer_fs)
    def _(i):
        j = outer_fs - 1 - i
        c_out[j] = dn((y ^ j) * 2 + (1 - c)).astype(jnp.bfloat16)
        c_copy(j).start()

    @pl.loop(0, outer_fs - 1)
    def _(i):
        j = outer_fs - 1 - i
        mine = dn((y ^ j) * 2 + c)
        c_copy(j).wait_recv()
        y_out[j] = (mine + c_in[j].astype(jnp.float32)).astype(jnp.bfloat16)
        y_copy(j).start()

    acc[...] = dn(fs)
    c_copy(0).wait_recv()
    acc[...] += c_in[0].astype(jnp.float32)

    def pair_sum(k):
        mine = dw((z ^ k) * 2 + x)
        x_copy(k).wait_recv()
        return mine + x_in[k].astype(jnp.float32)

    def to_near(q):
        n_out[q] = pair_sum(2 * q + 1).astype(jnp.bfloat16)
        n_copy(q).start()

    @pl.loop(0, quads - 1)
    def _(i):
        q = quads - 1 - i
        to_near(q)
        mine = pair_sum(2 * q)
        n_copy(q).wait_recv()
        z_out[q] = (mine + n_in[q].astype(jnp.float32)).astype(jnp.bfloat16)
        z_copy(q).start()

    to_near(0)

    @pl.loop(1, outer_fs)
    def _(j):
        y_copy(j).wait_recv()
        acc[...] += y_in[j].astype(jnp.float32)

    h = hidden_ref[...].astype(jnp.float32)
    inv = inv_ref[...]
    g_out[:, :cols] = jnp.broadcast_to(
        jnp.sum(acc[...] * h * inv, axis=0, keepdims=True), (8, cols)
    )
    g_out[:, cols:] = loss_ref[...]

    @pl.loop(1, n_dp)
    def _(k):
        g_copy(k).start()

    dy = acc[...] * gain_ref[...]
    part = jnp.sum(h * dy, axis=1, keepdims=True)
    rows = part.shape[0]
    d_out[...] = jnp.transpose(jnp.broadcast_to(part, (rows, 128)))[:8]
    for j in range(1, n_fsdp):
        d_copy(j).start()
    dots = d_out[...]
    for j in range(1, n_fsdp):
        d_copy(j).wait_recv()
        dots += d_in[j]
    column = jnp.transpose(jnp.broadcast_to(dots[:1], (128, rows)))[:, :1]
    scale = inv * inv * inv * column / (cols * n_fsdp)
    gh_ref[...] = (
        inv * (acc[...] * gain_ref[...]) - hidden_ref[...].astype(jnp.float32) * scale
    ).astype(jnp.bfloat16)

    gg_ref[...] = g_out[...]

    @pl.loop(1, n_dp)
    def _(k):
        g_copy(k).wait_recv()
        gg_ref[...] += g_in[k]

    gw_ref[...] = pair_sum(0)
    n_copy(0).wait_recv()
    gw_ref[...] += n_in[0].astype(jnp.float32)

    @pl.loop(1, quads)
    def _(k):
        z_copy(k).wait_recv()
        gw_ref[...] += z_in[k].astype(jnp.float32)

    @pl.loop(0, outer_dp)
    def _(k):
        x_copy(k).wait_send()

    @pl.loop(0, quads)
    def _(k):
        n_copy(k).wait_send()

    @pl.loop(1, quads)
    def _(k):
        z_copy(k).wait_send()

    @pl.loop(0, outer_fs)
    def _(j):
        c_copy(j).wait_send()

    @pl.loop(1, outer_fs)
    def _(j):
        y_copy(j).wait_send()

    for j in range(1, n_fsdp):
        d_copy(j).wait_send()

    @pl.loop(1, n_dp)
    def _(k):
        g_copy(k).wait_send()


def tail(normed, dlogits, head, hidden, gain_row, inv, loss_tile):
    n_dp, n_fsdp = lax.axis_size("dp"), lax.axis_size("fsdp")
    rows, width = normed.shape
    vocab_here = head.shape[0]
    cols = hidden.shape[1]
    feats = width // n_dp
    zd, qd, yd = n_dp // 2, n_dp // 4, n_fsdp // 2
    if feats % 128:
        normed = normed.reshape(rows, n_dp, feats).transpose(1, 0, 2)
    wide = cols + 128
    bf, f32 = jnp.bfloat16, jnp.float32
    vm = pl.BlockSpec(memory_space=pltpu.VMEM)
    dma = pltpu.SemaphoreType.DMA
    return pl.pallas_call(
        functools.partial(tail_kernel, n_dp, n_fsdp, feats),
        out_shape=(
            jax.ShapeDtypeStruct((rows, cols), bf),
            jax.ShapeDtypeStruct((feats, vocab_here), f32),
            jax.ShapeDtypeStruct((8, wide), f32),
        ),
        in_specs=[vm] * 7,
        out_specs=(vm, vm, vm),
        scratch_shapes=[
            pltpu.VMEM((zd, feats, vocab_here), bf),
            pltpu.VMEM((zd, feats, vocab_here), bf),
            pltpu.VMEM((qd, feats, vocab_here), bf),
            pltpu.VMEM((qd, feats, vocab_here), bf),
            pltpu.VMEM((qd, feats, vocab_here), bf),
            pltpu.VMEM((qd, feats, vocab_here), bf),
            pltpu.VMEM((yd, rows, cols), bf),
            pltpu.VMEM((yd, rows, cols), bf),
            pltpu.VMEM((yd, rows, cols), bf),
            pltpu.VMEM((yd, rows, cols), bf),
            pltpu.VMEM((rows, cols), f32),
            pltpu.VMEM((8, rows), f32),
            pltpu.VMEM((n_fsdp, 8, rows), f32),
            pltpu.VMEM((8, wide), f32),
            pltpu.VMEM((n_dp, 8, wide), f32),
        ]
        + [dma((n,)) for n in (zd, zd, qd, qd, qd, qd, yd, yd, yd, yd, n_fsdp, n_fsdp, n_dp, n_dp)],
        compiler_params=pltpu.CompilerParams(
            collective_id=0, has_side_effects=True, vmem_limit_bytes=60 * 1024 * 1024
        ),
    )(normed, dlogits, head, hidden, gain_row, inv, loss_tile)


def general(hidden, gain, head, targets, lengths, old_logp, rewards, group_slot):
    resp_here, length_max, shard_cols = hidden.shape
    rows = resp_here * length_max
    whole, gain_full = (
        lax.all_gather(hidden, "fsdp", axis=2, tiled=True),
        lax.all_gather(gain, "fsdp", axis=0, tiled=True),
    )
    width = whole.shape[2]
    whole = whole.reshape(rows, width)
    vocab_here = head.shape[0]
    vocab_start = lax.axis_index("fsdp") * vocab_here
    groups_all = resp_here * lax.axis_size("dp") // GROUP
    group = group_slot // GROUP
    member = (group[:, None] == jnp.arange(groups_all, dtype=jnp.int32)[None, :]).astype(
        jnp.float32
    )
    local_sums = jnp.sum(member * rewards[:, None], axis=0)
    local_count = jnp.sum(lengths).astype(jnp.float32)
    group_sums, count = lax.psum((local_sums, local_count), "dp")
    adv_resp = rewards - jnp.sum(member * group_sums[None, :], axis=1) / GROUP
    adv = jnp.repeat(adv_resp, length_max)
    mask = (
        (jnp.arange(length_max, dtype=jnp.int32)[None, :] < lengths[:, None])
        .astype(jnp.float32)
        .reshape(rows)
    )
    gain_f = gain_full.astype(jnp.float32)
    inv = lax.rsqrt(
        jnp.mean(jnp.square(whole.astype(jnp.float32)), axis=1, keepdims=True) + eps_norm
    )
    normed = (whole.astype(jnp.float32) * inv * gain_f).astype(jnp.bfloat16)
    logits = lax.dot_general(
        normed, head, (((1,), (1,)), ((), ())), preferred_element_type=jnp.float32
    )
    top_local = jnp.max(logits, axis=1)
    sum_local = jnp.sum(jnp.exp(logits - top_local[:, None]), axis=1)
    local_targets = targets.reshape(rows) - vocab_start
    hits = jnp.arange(vocab_here, dtype=jnp.int32)[None, :] == local_targets[:, None]
    chosen_local = jnp.sum(jnp.where(hits, logits, 0.0), axis=1)
    stats = lax.all_gather(jnp.stack([top_local, sum_local, chosen_local]), "fsdp", axis=0)
    top = jnp.max(stats[:, 0], axis=0)
    total = jnp.sum(stats[:, 1] * jnp.exp(stats[:, 0] - top[None, :]), axis=0)
    chosen = jnp.sum(stats[:, 2], axis=0)
    lse = top + jnp.log(total)
    logp = chosen - lse
    ratio = jnp.exp(logp - old_logp.reshape(rows))
    first = ratio * adv
    second = jnp.clip(ratio, clip_low, clip_high) * adv
    policy = -jnp.minimum(first, second)
    policy = jnp.where(adv < 0, jnp.minimum(policy, -dual_bound * adv), policy)
    loss_local = jnp.sum(mask * policy)
    active = (first <= second) & jnp.logical_not((adv < 0) & (first < dual_bound * adv))
    slots_all = rows * lax.axis_size("dp")
    grad_logp = slots_all / count * mask * jnp.where(active, -ratio * adv, 0.0)
    probs = jnp.exp(logits - lse[:, None])
    dlogits = (grad_logp[:, None] * (hits.astype(jnp.float32) - probs)).astype(jnp.bfloat16)
    grad_h, grad_head_t, sums = tail(
        normed,
        dlogits,
        head,
        hidden.reshape(rows, shard_cols),
        gain.astype(jnp.float32)[None, :],
        inv,
        jnp.broadcast_to(loss_local, (8, 128)),
    )
    loss = sums[0, shard_cols] / count
    grad_gain = sums[0, :shard_cols]
    grad_hidden = grad_h.reshape(resp_here, length_max, shard_cols)
    return (loss, grad_hidden, grad_gain, grad_head_t)


def solution(mesh):
    in_specs = (
        P("dp", None, "fsdp"),
        P("fsdp"),
        P("fsdp", None),
        P("dp", None),
        P("dp"),
        P("dp", None),
        P("dp"),
        P("dp"),
    )
    out_specs = (P(), P("dp", None, "fsdp"), P("fsdp"), P("dp", "fsdp"))
    return jax.shard_map(body, mesh=mesh, in_specs=in_specs, out_specs=out_specs, check_vma=False)
```

```python
import functools
import jax
import jax.numpy as jnp
from jax import lax
from jax.experimental import pallas as pl
from jax.experimental.pallas import tpu as pltpu
from jax.sharding import PartitionSpec as P

GROUP = 8
LANES = 128


eps_norm = 1e-06
clip_low = 0.8
clip_high = 1.2
dual_bound = 3.0


MESH = pl.DeviceIdType.MESH


def whole_kernel(
    n_dp,
    n_fsdp,
    length_max,
    gain_hbm,
    targets_hbm,
    old_hbm,
    lengths_hbm,
    rewards_hbm,
    slots_hbm,
    hidden_ref,
    head_hbm,
    gh_ref,
    gw_ref,
    gg_ref,
    targets,
    old,
    lengths,
    rewards,
    slots,
    gain_flat,
    gain_row,
    target_rows,
    old_rows,
    adv_rows,
    mask_rows,
    head,
    turned,
    sums,
    hs,
    hz,
    nm,
    lg,
    inv_s,
    inv_rows,
    squares,
    cnt,
    loss_s,
    gain_in,
    meta_out,
    meta_in,
    st_out,
    st_in,
    dls,
    dlz,
    c_out,
    c_in,
    y_out,
    y_in,
    acc,
    mid,
    left,
    d_out,
    d_in,
    x_out,
    x_in,
    z_out,
    z_in,
    fin,
    gsum,
    g_out,
    g_in,
    own_sem,
    head_sem,
    small_sem,
    sent,
    ysem,
    nsem,
    fsem,
    zsem,
    wsem,
    ssem,
    msem,
    tsem,
    lsem,
    csem,
    rsem,
    dsem,
    xsem,
    vsem,
    hsem,
    gsem,
):
    dp = lax.axis_index("dp")
    fs = lax.axis_index("fsdp")
    zh, zl, x = dp // 4, (dp // 2) % 2, dp % 2
    y, c = fs // 2, fs % 2
    rows, cols = hidden_ref.shape
    voc = head_hbm.shape[0]
    nch = rows // LANES
    quarter = LANES // 4
    feats = gw_ref.shape[0]
    resp_here = rows // length_max
    groups_all = resp_here * n_dp // GROUP
    f32, bf = jnp.float32, jnp.bfloat16

    def span(i):
        return pl.ds(pl.multiple_of(i * LANES, LANES), LANES)

    def piece(p):
        return pl.ds(pl.multiple_of(p * quarter, quarter), quarter)

    def shard(j):
        return pl.ds(pl.multiple_of((fs ^ j) * cols, LANES), cols)

    def remote(src, dst, kind, arrival, to):
        return pltpu.make_async_remote_copy(
            src_ref=src,
            dst_ref=dst,
            send_sem=sent.at[kind],
            recv_sem=arrival,
            device_id=to,
            device_id_type=MESH,
        )

    core, across = (dp, fs ^ 1), (dp, fs ^ 2)
    near, side, far = (dp ^ 2, fs), (dp ^ 1, fs), (dp ^ 4, fs)

    def own_copy(i):
        return pltpu.make_async_copy(hidden_ref.at[span(i)], hs.at[0, span(i)], own_sem.at[i])

    head_copy = pltpu.make_async_copy(head_hbm, head, head_sem.at[0])

    def cut(i, b):
        size = LANES * 3 // 8 if b else LANES * 5 // 8
        return pl.ds(pl.multiple_of(i * LANES + b * (LANES - size), 16), size)

    def y_copy(i, b):
        at = cut(i, b)
        return remote(hs.at[0, at], hs.at[2, at], 0, ysem.at[b, i], across)

    def n_copy(i):
        return remote(hs.at[0, span(i)], hs.at[1, span(i)], 1, nsem.at[i], core)

    def f_copy(i, b):
        at = cut(i, b)
        return remote(hs.at[2, at], hs.at[3, at], 2, fsem.at[i], core)

    def z_copy(k, i):
        return remote(hs.at[2 * k, span(i)], hz.at[k, span(i)], 3, zsem.at[k, i], near)

    def w_copy(k, i):
        return remote(hz.at[k, span(i)], hz.at[k, span(i)], 4, wsem.at[0], core)

    def s_copy(j):
        return remote(gain_row, gain_in.at[j], 5, ssem.at[0], (dp, fs ^ j))

    def m_copy(k):
        return remote(meta_out, meta_in.at[k], 6, msem.at[0], (dp ^ k, fs))

    def t_copy(j, i):
        return remote(st_out.at[i], st_in.at[j, i], 7, tsem.at[i], (dp, fs ^ j))

    def l_copy(i, p):
        return remote(dls.at[i, span(p)], dlz.at[i, span(p)], 8, lsem.at[p], near)

    def c_copy(k, i):
        return remote(c_out.at[k, span(i)], c_in.at[k, span(i)], 9, csem.at[k, i], core)

    def r_copy(i, b):
        at = pl.ds(pl.multiple_of(i * LANES + b * 2 * quarter, 2 * quarter), 2 * quarter)
        return remote(y_out.at[at], y_in.at[at], 10, rsem.at[i], across)

    def d_copy(j, i):
        return remote(d_out.at[i], d_in.at[j, i], 11, dsem.at[i], (dp, fs ^ j))

    def x_copy(q):
        return remote(x_out.at[0, piece(q)], x_in.at[0, piece(q)], 12, xsem.at[q], side)

    def e_copy():
        return remote(x_out.at[0, piece(0)], x_in.at[0, piece(0)], 12, xsem.at[0], far)

    def v_copy(p):
        return remote(x_out.at[1, span(p)], x_in.at[1, span(p)], 13, vsem.at[p], side)

    def h_copy(p, q):
        at = piece(4 * p + q)
        return remote(z_out.at[at], z_in.at[at], 14, hsem.at[p], far)

    def g_copy(k):
        return remote(g_out, g_in.at[k], 15, gsem.at[0], (dp ^ k, fs))

    def arrived(ref, arrival):
        remote(ref, ref, 0, arrival, core).wait_recv()

    def drained(ref, kind):
        remote(ref, ref, kind, wsem.at[0], core).wait_send()

    gives, takes = c != zl, c == zl

    barrier = pltpu.get_barrier_semaphore()
    for k in range(1, n_dp):
        pl.semaphore_signal(barrier, inc=1, device_id=(dp ^ k, fs), device_id_type=MESH)
    for k in range(1, n_fsdp):
        pl.semaphore_signal(barrier, inc=1, device_id=(dp, fs ^ k), device_id_type=MESH)
    loads = [
        pltpu.make_async_copy(src, dst, small_sem.at[n])
        for n, (src, dst) in enumerate(
            [
                (slots_hbm, slots),
                (rewards_hbm, rewards),
                (lengths_hbm, lengths),
                (targets_hbm, targets),
                (old_hbm, old),
            ]
        )
    ]
    gain_copy = pltpu.make_async_copy(gain_hbm, gain_flat, small_sem.at[5])
    gain_copy.start()
    for load in loads:
        load.start()
    for i in range(nch):
        own_copy(i).start()
    head_copy.start()
    pl.semaphore_wait(barrier, n_dp + n_fsdp - 2)

    gain_copy.wait()
    gain_row[...] = gain_flat[...].astype(f32).reshape(1, cols)
    for j in range(1, n_fsdp):
        s_copy(j).start()

    @pl.loop(0, nch)
    def _(i):
        own_copy(i).wait()

        @pl.when(i == 0)
        def _():
            y_copy(i, 0).start()
            y_copy(i, 1).start()

        @pl.when(i == 1)
        def _():
            y_copy(i, 0).start()

        n_copy(i).start()

    for load in loads:
        load.wait()

    lane = lax.broadcasted_iota(jnp.int32, (8, LANES), 1)
    tile = jnp.zeros((8, LANES), f32)
    for r in range(resp_here):
        tile += jnp.where(lane == slots[r] // GROUP, rewards[r], 0.0)
        tile += jnp.where(lane == groups_all, lengths[r].astype(f32), 0.0)
    meta_out[...] = tile
    for k in range(1, n_dp):
        m_copy(k).start()

    @pl.when(gives)
    def _():
        @pl.loop(0, nch)
        def _(i):
            z_copy(0, i).start()

    loss_s[...] = jnp.zeros_like(loss_s)
    gsum[...] = jnp.zeros_like(gsum)
    head_copy.wait()

    @pl.loop(0, head.shape[1] // LANES)
    def _(b):
        turned[span(b)] = jnp.transpose(head[:, span(b)])

    @pl.loop(0, nch)
    def _(i):
        n_copy(i).wait_recv()

    gain_in[0] = gain_row[...]
    arrived(gain_in.at[pl.ds(1, n_fsdp - 1)], ssem.at[0])
    arrived(meta_in.at[pl.ds(1, n_dp - 1)], msem.at[0])
    total = meta_out[...]
    for k in range(1, n_dp):
        total += meta_in[k]

    def entry(g):
        return jnp.sum(jnp.where(lane == g, total, 0.0), axis=1, keepdims=True)[:1]

    for i in range(nch):
        r, first = i * LANES // length_max, i * LANES % length_max
        position = lax.broadcasted_iota(jnp.int32, (1, LANES), 1) + first
        target_rows[i] = targets[r : r + 1, first : first + LANES]
        old_rows[i] = old[r : r + 1, first : first + LANES]
        mask_rows[i] = jnp.where(position < lengths[r], 1.0, 0.0)
        adv = rewards[r] - entry(slots[r] // GROUP) / GROUP
        adv_rows[i] = jnp.broadcast_to(adv, (1, LANES))
    cnt[...] = jnp.broadcast_to(entry(groups_all), cnt.shape)
    slots_all = rows * n_dp

    def hits_of(i):
        at = lax.broadcasted_iota(jnp.int32, (voc, LANES), 0) + fs * voc
        return at == target_rows[i]

    def take(j, i):
        h = hs[j, span(i)].astype(f32)
        nm[j] = (h * gain_in[j]).astype(bf)
        return jnp.sum(h * h, axis=1, keepdims=True)

    def product(j):
        return jnp.dot(nm[j], turned[shard(j)], preferred_element_type=f32)

    def begin(i):
        squares[...] = take(0, i) + take(1, i)
        sums[...] = product(0)
        sums[...] += product(1)

    def forward(i):
        for b in range(2):
            y_copy(i, b).wait_recv()
            f_copy(i, b).start()

        @pl.when(gives)
        def _():
            z_copy(1, i).start()

        square = squares[...] + take(2, i)
        sums[...] += product(2)
        arrived(hs.at[3, span(i)], fsem.at[i])
        square += take(3, i)
        inv = lax.rsqrt(square / (cols * n_fsdp) + eps_norm)
        inv_s[span(i)] = inv
        inv_rows[i] = jnp.transpose(jnp.broadcast_to(inv, (LANES, LANES)))[:1]
        lg[i] = jnp.transpose((sums[...] + product(3)) * inv)
        logits = lg[i]
        top = jnp.max(logits, axis=0, keepdims=True)
        st_out[i, 0:1] = top
        st_out[i, 1:2] = jnp.sum(jnp.exp(logits - top), axis=0, keepdims=True)
        st_out[i, 2:3] = jnp.sum(jnp.where(hits_of(i), logits, 0.0), axis=0, keepdims=True)
        st_out[i, 3:8] = jnp.zeros((5, LANES), f32)
        for j in range(1, n_fsdp):
            t_copy(j, i).start()

        @pl.when(i + 1 < nch)
        def _():
            y_copy(i + 1, 1).start()

        @pl.when(i + 2 < nch)
        def _():
            y_copy(i + 2, 0).start()

    def backward(i):
        arrived(st_in.at[pl.ds(1, n_fsdp - 1), i], tsem.at[i])
        stats = [st_out[i]] + [st_in[j, i] for j in range(1, n_fsdp)]
        top = stats[0][0:1]
        for s in stats[1:]:
            top = jnp.maximum(top, s[0:1])
        total = jnp.zeros_like(top)
        chosen = jnp.zeros_like(top)
        for s in stats:
            total += s[1:2] * jnp.exp(s[0:1] - top)
            chosen += s[2:3]
        lse = top + jnp.log(total)
        adv, mask = adv_rows[i], mask_rows[i]
        ratio = jnp.exp(chosen - lse - old_rows[i])
        first = ratio * adv
        second = jnp.clip(ratio, clip_low, clip_high) * adv
        policy = -jnp.minimum(first, second)
        policy = jnp.where(adv < 0, jnp.minimum(policy, -dual_bound * adv), policy)
        loss_s[0:1] += mask * policy
        active = (first <= second) & jnp.logical_not((adv < 0) & (first < dual_bound * adv))
        slope = slots_all / cnt[0:1] * mask * jnp.where(active, -ratio * adv, 0.0)
        grad = slope * (hits_of(i).astype(f32) - jnp.exp(lg[i] - lse))
        dls[i] = (grad * inv_rows[i]).astype(bf)
        l_copy(i, 0).start()

        @pl.when(i < nch - 2)
        def _():
            for p in range(1, nch):
                l_copy(i, p).start()

        left[...] = jnp.transpose(grad).astype(bf)

    def spread(i):
        def dn(j):
            return jnp.dot(left[...], head[:, shard(j)], preferred_element_type=f32)

        c_out[1, span(i)] = dn(3).astype(bf)
        c_copy(1, i).start()
        c_out[0, span(i)] = dn(1).astype(bf)
        c_copy(0, i).start()
        acc[span(i)] = dn(0)
        mid[span(i)] = dn(2)

    def relay(i):
        @pl.when(takes)
        def _():
            for k in range(2):
                z_copy(k, i).wait_recv()
                w_copy(k, i).start()

    def combine(i):
        c_copy(1, i).wait_recv()
        y_out[span(i)] = (mid[span(i)] + c_in[1, span(i)].astype(f32)).astype(bf)
        c_copy(0, i).wait_recv()
        acc[span(i)] += c_in[0, span(i)].astype(f32)

    begin(0)

    @pl.loop(0, nch)
    def _(i):
        forward(i)

        @pl.when(i + 1 < nch)
        def _():
            begin(i + 1)

        @pl.when(i > 0)
        def _():
            relay(i - 1)
            spread(i - 1)

        @pl.when(i > 1)
        def _():
            combine(i - 2)

        @pl.when(i == nch - 2)
        def _():
            r_copy(0, 0).start()

        @pl.when(i == nch - 1)
        def _():
            r_copy(0, 1).start()
            for n in range(1, nch - 2):
                r_copy(n, 0).start()
                r_copy(n, 1).start()

        backward(i)

    for p in range(1, nch):
        for i in range(nch - 2, nch):
            l_copy(i, p).start()
    relay(nch - 1)
    spread(nch - 1)
    combine(nch - 2)
    r_copy(nch - 2, 0).start()
    r_copy(nch - 2, 1).start()

    def dots(i):
        arrived(y_in.at[span(i)], rsem.at[i])
        grad = acc[span(i)] + y_in[span(i)].astype(f32)
        acc[span(i)] = grad
        h = hs[0, span(i)].astype(f32)
        prod = grad * h
        gsum[...] += jnp.sum((prod * inv_s[span(i)]).reshape(LANES // 8, 8, cols), axis=0)
        part = jnp.sum(prod * gain_in[0], axis=1, keepdims=True)
        d_out[i] = jnp.transpose(jnp.broadcast_to(part, (LANES, LANES)))[:8]
        for j in range(1, n_fsdp):
            d_copy(j, i).start()

    def finish(i):
        whole = d_out[i]
        arrived(d_in.at[pl.ds(1, n_fsdp - 1), i], dsem.at[i])
        for j in range(1, n_fsdp):
            whole += d_in[j, i]
        column = jnp.transpose(jnp.broadcast_to(whole[:1], (LANES, LANES)))[:, :1]
        inv = inv_s[span(i)]
        scale = inv * inv * inv * column / (cols * n_fsdp)
        gh_ref[span(i)] = (
            inv * (acc[span(i)] * gain_in[0])
            - hs[0, span(i)].astype(f32) * scale
        ).astype(bf)

    def dw(p, zb, xb):
        at = pl.ds(pl.multiple_of(xb * feats, LANES), feats)
        here = jnp.concatenate([dls[i, span(p)] for i in range(nch)], axis=1)
        other = jnp.concatenate([dlz[i, span(p)] for i in range(nch)], axis=1)
        return jnp.dot(
            here, hs[fs ^ (2 * zb + zl), :, at], preferred_element_type=f32
        ) + jnp.dot(other, hz[y ^ zb, :, at], preferred_element_type=f32)

    @pl.when(gives)
    def _():
        arrived(hz, wsem.at[0])

    def lead(p, direct):
        arrived(dlz.at[:, span(p)], lsem.at[p])
        x_out[0, span(p)] = dw(p, 1 - zh, 1 - x).astype(bf)
        if direct:
            e_copy().start()
        for q in range(direct, 4):
            x_copy(4 * p + q).start()
        fin[span(p)] = dw(p, 1 - zh, x)
        if direct:
            z_out[piece(0)] = fin[piece(0)].astype(bf)
            h_copy(0, 0).start()

    def follow(p, direct):
        @pl.loop(direct, 4)
        def _(q):
            at = piece(4 * p + q)
            x_copy(4 * p + q).wait_recv()
            z_out[at] = (fin[at] + x_in[0, at].astype(f32)).astype(bf)

            @pl.when((p < nch - 1) | (q < 2))
            def _():
                h_copy(p, q).start()

    def back(p):
        x_out[1, span(p)] = dw(p, zh, 1 - x).astype(bf)
        v_copy(p).start()

    lead(0, 1)
    lead(1, 0)
    follow(0, 1)
    combine(nch - 1)
    r_copy(nch - 1, 0).start()
    r_copy(nch - 1, 1).start()
    lead(2, 0)
    mid[span(0), :feats] = dw(0, zh, 1 - x)
    e_copy().wait_recv()
    mid[piece(0), :feats] += x_in[0, piece(0)].astype(f32)
    x_out[1, span(0)] = mid[span(0), :feats].astype(bf)
    v_copy(0).start()

    @pl.loop(1, nch)
    def _(p):
        @pl.when((p > 1) & (p + 1 < nch))
        def _():
            lead(p + 1, 0)

        @pl.when(p > 1)
        def _():
            back(p - 1)

        dots(p - 1)
        follow(p, 0)

    back(nch - 1)

    dots(nch - 1)

    nb = cols // LANES
    column_sums = jnp.sum(gsum[...], axis=0, keepdims=True)
    g_out[...] = jnp.zeros_like(g_out)
    for b in range(nb):
        g_out[b : b + 1] = column_sums[:, b * LANES : (b + 1) * LANES]
    g_out[nb : nb + 1] = loss_s[0:1]

    for k in range(1, n_dp):
        g_copy(k).start()
    for q in range(2, 4):
        h_copy(nch - 1, q).start()

    @pl.loop(0, nch)
    def _(p):
        fin[span(p)] = dw(p, zh, x)


    @pl.loop(0, nch)
    def _(p):
        finish(p)

    @pl.loop(0, nch)
    def _(p):
        v_copy(p).wait_recv()
        fin[span(p)] += x_in[1, span(p)].astype(f32)

    mine = gain_in[fs ^ (2 * zh + zl), :, pl.ds(pl.multiple_of(x * feats, LANES), feats)]
    for p in range(nch):
        arrived(z_in.at[span(p)], hsem.at[p])
        gw_ref[:, span(p)] = jnp.transpose((fin[span(p)] + z_in[span(p)].astype(f32)) * mine)

    arrived(g_in.at[pl.ds(1, n_dp - 1)], gsem.at[0])
    whole = g_out[...]
    for k in range(1, n_dp):
        whole += g_in[k]
    gg_ref[...] = whole
    gg_ref[nb : nb + 1] = jnp.sum(gg_ref[nb : nb + 1], axis=1, keepdims=True) / cnt[0:1]

    drained(hs.at[0], 0)
    drained(hs.at[0], 1)
    drained(hs.at[2], 2)

    @pl.when(gives)
    def _():
        drained(hz, 3)

    @pl.when(takes)
    def _():
        drained(hz, 4)

    drained(gain_in.at[pl.ds(1, n_fsdp - 1)], 5)
    drained(meta_in.at[pl.ds(1, n_dp - 1)], 6)
    drained(st_in.at[pl.ds(1, n_fsdp - 1)], 7)
    drained(dls, 8)
    drained(c_out, 9)
    drained(y_out, 10)
    drained(d_in.at[pl.ds(1, n_fsdp - 1)], 11)
    drained(x_out.at[0], 12)
    drained(x_out.at[1], 13)
    drained(z_out, 14)
    drained(g_in.at[pl.ds(1, n_dp - 1)], 15)


def write_kernel(gh_ref, gw_ref, gg_ref, loss_out, gh_out, gg_out, gw_out, sems):
    parts = sems.shape[1]

    def part(ref, n):
        size = ref.shape[0] // parts
        return ref.at[pl.ds(n * size, size)]

    copies = [
        pltpu.make_async_copy(part(src, n), part(dst, n), sems.at[m, n])
        for m, (src, dst) in enumerate([(gw_ref, gw_out), (gh_ref, gh_out)])
        for n in range(parts)
    ]
    for copy in copies:
        copy.start()
    nb = gg_out.shape[0]
    gg_out[...] = gg_ref[:nb]
    loss_out[...] = gg_ref[nb : nb + 1, :1]
    for copy in copies:
        copy.wait()


def write(gh, gw, gg, nb):
    vm = pl.BlockSpec(memory_space=pltpu.VMEM)
    anywhere = pl.BlockSpec(memory_space=pl.ANY)
    return pl.pallas_call(
        write_kernel,
        out_shape=(
            jax.ShapeDtypeStruct((1, 1), jnp.float32),
            jax.ShapeDtypeStruct(gh.shape, gh.dtype),
            jax.ShapeDtypeStruct((nb, LANES), jnp.float32),
            jax.ShapeDtypeStruct(gw.shape, gw.dtype),
        ),
        in_specs=[vm, vm, vm],
        out_specs=(vm, anywhere, vm, anywhere),
        scratch_shapes=[pltpu.SemaphoreType.DMA((2, 4))],
        compiler_params=pltpu.CompilerParams(vmem_limit_bytes=8 * 1024 * 1024),
    )(gh, gw, gg)


def whole(gain, targets, old_logp, lengths, rewards, group_slot, hidden, head):
    n_dp, n_fsdp = lax.axis_size("dp"), lax.axis_size("fsdp")
    resp_here, length_max = targets.shape
    rows, cols = hidden.shape
    voc, width = head.shape
    feats = width // n_dp
    nch = rows // LANES
    tall = (cols // LANES + 8) // 8 * 8
    bf, f32 = jnp.bfloat16, jnp.float32
    vm = pl.BlockSpec(memory_space=pltpu.VMEM)
    anywhere = pl.BlockSpec(memory_space=pl.ANY)
    dma = pltpu.SemaphoreType.DMA
    return pl.pallas_call(
        functools.partial(whole_kernel, n_dp, n_fsdp, length_max),
        out_shape=(
            pltpu.VMEM((rows, cols), bf),
            pltpu.VMEM((feats, voc), f32),
            pltpu.VMEM((tall, LANES), f32),
        ),
        in_specs=[anywhere] * 8,
        out_specs=(vm, vm, vm),
        scratch_shapes=[
            pltpu.VMEM((resp_here, length_max), jnp.int32),
            pltpu.VMEM((resp_here, length_max), f32),
            pltpu.SMEM((resp_here,), jnp.int32),
            pltpu.SMEM((resp_here,), f32),
            pltpu.SMEM((resp_here,), jnp.int32),
            pltpu.VMEM((cols,), bf),
            pltpu.VMEM((1, cols), f32),
            pltpu.VMEM((nch, 1, LANES), jnp.int32),
            pltpu.VMEM((nch, 1, LANES), f32),
            pltpu.VMEM((nch, 1, LANES), f32),
            pltpu.VMEM((nch, 1, LANES), f32),
            pltpu.VMEM((voc, width), bf),
            pltpu.VMEM((width, voc), bf),
            pltpu.VMEM((LANES, voc), f32),
            pltpu.VMEM((n_fsdp, rows, cols), bf),
            pltpu.VMEM((2, rows, cols), bf),
            pltpu.VMEM((n_fsdp, LANES, cols), bf),
            pltpu.VMEM((nch, voc, LANES), f32),
            pltpu.VMEM((rows, 1), f32),
            pltpu.VMEM((nch, 1, LANES), f32),
            pltpu.VMEM((LANES, 1), f32),
            pltpu.VMEM((8, LANES), f32),
            pltpu.VMEM((8, LANES), f32),
            pltpu.VMEM((n_fsdp, 1, cols), f32),
            pltpu.VMEM((8, LANES), f32),
            pltpu.VMEM((n_dp, 8, LANES), f32),
            pltpu.VMEM((nch, 8, LANES), f32),
            pltpu.VMEM((n_fsdp, nch, 8, LANES), f32),
            pltpu.VMEM((nch, voc, LANES), bf),
            pltpu.VMEM((nch, voc, LANES), bf),
            pltpu.VMEM((2, rows, cols), bf),
            pltpu.VMEM((2, rows, cols), bf),
            pltpu.VMEM((rows, cols), bf),
            pltpu.VMEM((rows, cols), bf),
            pltpu.VMEM((rows, cols), f32),
            pltpu.VMEM((rows, cols), f32),
            pltpu.VMEM((LANES, voc), bf),
            pltpu.VMEM((nch, 8, LANES), f32),
            pltpu.VMEM((n_fsdp, nch, 8, LANES), f32),
            pltpu.VMEM((2, voc, feats), bf),
            pltpu.VMEM((2, voc, feats), bf),
            pltpu.VMEM((voc, feats), bf),
            pltpu.VMEM((voc, feats), bf),
            pltpu.VMEM((voc, feats), f32),
            pltpu.VMEM((8, cols), f32),
            pltpu.VMEM((tall, LANES), f32),
            pltpu.VMEM((n_dp, tall, LANES), f32),
            dma((nch,)),
            dma((1,)),
            dma((6,)),
            dma((16,)),
            dma((2, nch)),
            dma((nch,)),
            dma((nch,)),
            dma((2, nch)),
            dma((1,)),
            dma((1,)),
            dma((1,)),
            dma((nch,)),
            dma((nch,)),
            dma((2, nch)),
            dma((nch,)),
            dma((nch,)),
            dma((4 * nch,)),
            dma((nch,)),
            dma((nch,)),
            dma((1,)),
        ],
        compiler_params=pltpu.CompilerParams(
            collective_id=1, has_side_effects=True, vmem_limit_bytes=60 * 1024 * 1024
        ),
    )(gain, targets, old_logp, lengths, rewards, group_slot, hidden, head)


def fits(hidden, head):
    n_dp, n_fsdp = lax.axis_size("dp"), lax.axis_size("fsdp")
    rows = hidden.shape[0] * hidden.shape[1]
    voc, width = head.shape
    return (
        n_dp == 2 * n_fsdp
        and n_fsdp == 2 * 2
        and (width // n_dp) % LANES == 0
        and rows % LANES == 0
        and rows == voc
        and rows > 2 * LANES
        and hidden.shape[1] % LANES == 0
    )


def body(hidden, gain, head, targets, lengths, old_logp, rewards, group_slot):
    if not fits(hidden, head):
        return general(hidden, gain, head, targets, lengths, old_logp, rewards, group_slot)
    resp_here, length_max, cols = hidden.shape
    grad_h, grad_head_t, sums = whole(
        gain,
        targets,
        old_logp,
        lengths,
        rewards,
        group_slot,
        hidden.reshape(resp_here * length_max, cols),
        head,
    )
    loss, grad_h, grad_gain, grad_head_t = write(grad_h, grad_head_t, sums, cols // LANES)
    return (
        loss.reshape(()),
        grad_h.reshape(resp_here, length_max, cols),
        grad_gain.reshape(cols),
        grad_head_t,
    )


def tail_kernel(
    n_dp,
    n_fsdp,
    feats,
    normed_ref,
    dlogits_ref,
    head_ref,
    hidden_ref,
    gain_ref,
    inv_ref,
    loss_ref,
    gh_ref,
    gw_ref,
    gg_ref,
    x_out,
    x_in,
    n_out,
    n_in,
    z_out,
    z_in,
    c_out,
    c_in,
    y_out,
    y_in,
    acc,
    d_out,
    d_in,
    g_out,
    g_in,
    xs,
    xr,
    ns,
    nr,
    zs,
    zr,
    cs,
    cr,
    ys,
    yr,
    ds_,
    dr,
    gs,
    gr,
):
    dp = lax.axis_index("dp")
    fs = lax.axis_index("fsdp")
    z, x = dp // 2, dp % 2
    y, c = fs // 2, fs % 2
    outer_dp, outer_fs, quads = n_dp // 2, n_fsdp // 2, n_dp // 4
    cols = hidden_ref.shape[1]

    barrier = pltpu.get_barrier_semaphore()
    for k in range(1, n_dp):
        pl.semaphore_signal(barrier, inc=1, device_id=(dp ^ k, fs), device_id_type=MESH)
    for k in range(1, n_fsdp):
        pl.semaphore_signal(barrier, inc=1, device_id=(dp, fs ^ k), device_id_type=MESH)
    pl.semaphore_wait(barrier, n_dp + n_fsdp - 2)

    def remote(out, into, send, recv, k, dst):
        return pltpu.make_async_remote_copy(
            src_ref=out,
            dst_ref=into.at[k],
            send_sem=send.at[k],
            recv_sem=recv.at[k],
            device_id=dst,
            device_id_type=MESH,
        )

    def x_copy(k):
        return remote(x_out.at[k], x_in, xs, xr, k, (dp ^ 1, fs))

    def z_copy(k):
        return remote(z_out.at[k], z_in, zs, zr, k, (dp ^ (4 * k), fs))

    def n_copy(k):
        return remote(n_out.at[k], n_in, ns, nr, k, (dp ^ 2, fs))

    def c_copy(j):
        return remote(c_out.at[j], c_in, cs, cr, j, (dp, fs ^ 1))

    def y_copy(j):
        return remote(y_out.at[j], y_in, ys, yr, j, (dp, (y ^ j) * 2 + c))

    def d_copy(j):
        return remote(d_out, d_in, ds_, dr, j, (dp, fs ^ j))

    def g_copy(k):
        return remote(g_out, g_in, gs, gr, k, (dp ^ k, fs))

    def dw(block):
        if feats % 128 == 0:
            left = normed_ref[:, pl.ds(pl.multiple_of(block * feats, 128), feats)]
        else:
            left = normed_ref[block]
        return lax.dot_general(
            left, dlogits_ref[...], (((0,), (0,)), ((), ())), preferred_element_type=jnp.float32
        )

    def dn(block):
        right = head_ref[:, pl.ds(pl.multiple_of(block * cols, 128), cols)]
        return jnp.dot(dlogits_ref[...], right, preferred_element_type=jnp.float32)

    @pl.loop(0, outer_dp)
    def _(i):
        k = outer_dp - 1 - i
        x_out[k] = dw((z ^ k) * 2 + (1 - x)).astype(jnp.bfloat16)
        x_copy(k).start()

    @pl.loop(0, outer_fs)
    def _(i):
        j = outer_fs - 1 - i
        c_out[j] = dn((y ^ j) * 2 + (1 - c)).astype(jnp.bfloat16)
        c_copy(j).start()

    @pl.loop(0, outer_fs - 1)
    def _(i):
        j = outer_fs - 1 - i
        mine = dn((y ^ j) * 2 + c)
        c_copy(j).wait_recv()
        y_out[j] = (mine + c_in[j].astype(jnp.float32)).astype(jnp.bfloat16)
        y_copy(j).start()

    acc[...] = dn(fs)
    c_copy(0).wait_recv()
    acc[...] += c_in[0].astype(jnp.float32)

    def pair_sum(k):
        mine = dw((z ^ k) * 2 + x)
        x_copy(k).wait_recv()
        return mine + x_in[k].astype(jnp.float32)

    def to_near(q):
        n_out[q] = pair_sum(2 * q + 1).astype(jnp.bfloat16)
        n_copy(q).start()

    @pl.loop(0, quads - 1)
    def _(i):
        q = quads - 1 - i
        to_near(q)
        mine = pair_sum(2 * q)
        n_copy(q).wait_recv()
        z_out[q] = (mine + n_in[q].astype(jnp.float32)).astype(jnp.bfloat16)
        z_copy(q).start()

    to_near(0)

    @pl.loop(1, outer_fs)
    def _(j):
        y_copy(j).wait_recv()
        acc[...] += y_in[j].astype(jnp.float32)

    h = hidden_ref[...].astype(jnp.float32)
    inv = inv_ref[...]
    g_out[:, :cols] = jnp.broadcast_to(
        jnp.sum(acc[...] * h * inv, axis=0, keepdims=True), (8, cols)
    )
    g_out[:, cols:] = loss_ref[...]

    @pl.loop(1, n_dp)
    def _(k):
        g_copy(k).start()

    dy = acc[...] * gain_ref[...]
    part = jnp.sum(h * dy, axis=1, keepdims=True)
    rows = part.shape[0]
    d_out[...] = jnp.transpose(jnp.broadcast_to(part, (rows, 128)))[:8]
    for j in range(1, n_fsdp):
        d_copy(j).start()
    dots = d_out[...]
    for j in range(1, n_fsdp):
        d_copy(j).wait_recv()
        dots += d_in[j]
    column = jnp.transpose(jnp.broadcast_to(dots[:1], (128, rows)))[:, :1]
    scale = inv * inv * inv * column / (cols * n_fsdp)
    gh_ref[...] = (
        inv * (acc[...] * gain_ref[...]) - hidden_ref[...].astype(jnp.float32) * scale
    ).astype(jnp.bfloat16)

    gg_ref[...] = g_out[...]

    @pl.loop(1, n_dp)
    def _(k):
        g_copy(k).wait_recv()
        gg_ref[...] += g_in[k]

    gw_ref[...] = pair_sum(0)
    n_copy(0).wait_recv()
    gw_ref[...] += n_in[0].astype(jnp.float32)

    @pl.loop(1, quads)
    def _(k):
        z_copy(k).wait_recv()
        gw_ref[...] += z_in[k].astype(jnp.float32)

    @pl.loop(0, outer_dp)
    def _(k):
        x_copy(k).wait_send()

    @pl.loop(0, quads)
    def _(k):
        n_copy(k).wait_send()

    @pl.loop(1, quads)
    def _(k):
        z_copy(k).wait_send()

    @pl.loop(0, outer_fs)
    def _(j):
        c_copy(j).wait_send()

    @pl.loop(1, outer_fs)
    def _(j):
        y_copy(j).wait_send()

    for j in range(1, n_fsdp):
        d_copy(j).wait_send()

    @pl.loop(1, n_dp)
    def _(k):
        g_copy(k).wait_send()


def tail(normed, dlogits, head, hidden, gain_row, inv, loss_tile):
    n_dp, n_fsdp = lax.axis_size("dp"), lax.axis_size("fsdp")
    rows, width = normed.shape
    vocab_here = head.shape[0]
    cols = hidden.shape[1]
    feats = width // n_dp
    zd, qd, yd = n_dp // 2, n_dp // 4, n_fsdp // 2
    if feats % 128:
        normed = normed.reshape(rows, n_dp, feats).transpose(1, 0, 2)
    wide = cols + 128
    bf, f32 = jnp.bfloat16, jnp.float32
    vm = pl.BlockSpec(memory_space=pltpu.VMEM)
    dma = pltpu.SemaphoreType.DMA
    return pl.pallas_call(
        functools.partial(tail_kernel, n_dp, n_fsdp, feats),
        out_shape=(
            jax.ShapeDtypeStruct((rows, cols), bf),
            jax.ShapeDtypeStruct((feats, vocab_here), f32),
            jax.ShapeDtypeStruct((8, wide), f32),
        ),
        in_specs=[vm] * 7,
        out_specs=(vm, vm, vm),
        scratch_shapes=[
            pltpu.VMEM((zd, feats, vocab_here), bf),
            pltpu.VMEM((zd, feats, vocab_here), bf),
            pltpu.VMEM((qd, feats, vocab_here), bf),
            pltpu.VMEM((qd, feats, vocab_here), bf),
            pltpu.VMEM((qd, feats, vocab_here), bf),
            pltpu.VMEM((qd, feats, vocab_here), bf),
            pltpu.VMEM((yd, rows, cols), bf),
            pltpu.VMEM((yd, rows, cols), bf),
            pltpu.VMEM((yd, rows, cols), bf),
            pltpu.VMEM((yd, rows, cols), bf),
            pltpu.VMEM((rows, cols), f32),
            pltpu.VMEM((8, rows), f32),
            pltpu.VMEM((n_fsdp, 8, rows), f32),
            pltpu.VMEM((8, wide), f32),
            pltpu.VMEM((n_dp, 8, wide), f32),
        ]
        + [dma((n,)) for n in (zd, zd, qd, qd, qd, qd, yd, yd, yd, yd, n_fsdp, n_fsdp, n_dp, n_dp)],
        compiler_params=pltpu.CompilerParams(
            collective_id=0, has_side_effects=True, vmem_limit_bytes=60 * 1024 * 1024
        ),
    )(normed, dlogits, head, hidden, gain_row, inv, loss_tile)


def general(hidden, gain, head, targets, lengths, old_logp, rewards, group_slot):
    resp_here, length_max, shard_cols = hidden.shape
    rows = resp_here * length_max
    whole, gain_full = (
        lax.all_gather(hidden, "fsdp", axis=2, tiled=True),
        lax.all_gather(gain, "fsdp", axis=0, tiled=True),
    )
    width = whole.shape[2]
    whole = whole.reshape(rows, width)
    vocab_here = head.shape[0]
    vocab_start = lax.axis_index("fsdp") * vocab_here
    groups_all = resp_here * lax.axis_size("dp") // GROUP
    group = group_slot // GROUP
    member = (group[:, None] == jnp.arange(groups_all, dtype=jnp.int32)[None, :]).astype(
        jnp.float32
    )
    local_sums = jnp.sum(member * rewards[:, None], axis=0)
    local_count = jnp.sum(lengths).astype(jnp.float32)
    group_sums, count = lax.psum((local_sums, local_count), "dp")
    adv_resp = rewards - jnp.sum(member * group_sums[None, :], axis=1) / GROUP
    adv = jnp.repeat(adv_resp, length_max)
    mask = (
        (jnp.arange(length_max, dtype=jnp.int32)[None, :] < lengths[:, None])
        .astype(jnp.float32)
        .reshape(rows)
    )
    gain_f = gain_full.astype(jnp.float32)
    inv = lax.rsqrt(
        jnp.mean(jnp.square(whole.astype(jnp.float32)), axis=1, keepdims=True) + eps_norm
    )
    normed = (whole.astype(jnp.float32) * inv * gain_f).astype(jnp.bfloat16)
    logits = lax.dot_general(
        normed, head, (((1,), (1,)), ((), ())), preferred_element_type=jnp.float32
    )
    top_local = jnp.max(logits, axis=1)
    sum_local = jnp.sum(jnp.exp(logits - top_local[:, None]), axis=1)
    local_targets = targets.reshape(rows) - vocab_start
    hits = jnp.arange(vocab_here, dtype=jnp.int32)[None, :] == local_targets[:, None]
    chosen_local = jnp.sum(jnp.where(hits, logits, 0.0), axis=1)
    stats = lax.all_gather(jnp.stack([top_local, sum_local, chosen_local]), "fsdp", axis=0)
    top = jnp.max(stats[:, 0], axis=0)
    total = jnp.sum(stats[:, 1] * jnp.exp(stats[:, 0] - top[None, :]), axis=0)
    chosen = jnp.sum(stats[:, 2], axis=0)
    lse = top + jnp.log(total)
    logp = chosen - lse
    ratio = jnp.exp(logp - old_logp.reshape(rows))
    first = ratio * adv
    second = jnp.clip(ratio, clip_low, clip_high) * adv
    policy = -jnp.minimum(first, second)
    policy = jnp.where(adv < 0, jnp.minimum(policy, -dual_bound * adv), policy)
    loss_local = jnp.sum(mask * policy)
    active = (first <= second) & jnp.logical_not((adv < 0) & (first < dual_bound * adv))
    slots_all = rows * lax.axis_size("dp")
    grad_logp = slots_all / count * mask * jnp.where(active, -ratio * adv, 0.0)
    probs = jnp.exp(logits - lse[:, None])
    dlogits = (grad_logp[:, None] * (hits.astype(jnp.float32) - probs)).astype(jnp.bfloat16)
    grad_h, grad_head_t, sums = tail(
        normed,
        dlogits,
        head,
        hidden.reshape(rows, shard_cols),
        gain.astype(jnp.float32)[None, :],
        inv,
        jnp.broadcast_to(loss_local, (8, 128)),
    )
    loss = sums[0, shard_cols] / count
    grad_gain = sums[0, :shard_cols]
    grad_hidden = grad_h.reshape(resp_here, length_max, shard_cols)
    return (loss, grad_hidden, grad_gain, grad_head_t)


def solution(mesh):
    in_specs = (
        P("dp", None, "fsdp"),
        P("fsdp"),
        P("fsdp", None),
        P("dp", None),
        P("dp"),
        P("dp", None),
        P("dp"),
        P("dp"),
    )
    out_specs = (P(), P("dp", None, "fsdp"), P("fsdp"), P("dp", "fsdp"))
    return jax.shard_map(body, mesh=mesh, in_specs=in_specs, out_specs=out_specs, check_vma=False)
```
